128 devices in a mesh: grp: 8 (over y, core), rep: 16 (over z, x).
Axes of the slice: x: 4, y: 4, z: 4, core: 2. Of those that a mesh axis runs over, the one named last changes fastest.
Arguments:
- coefficients: bfloat16 [16384, 2048], P(('grp', 'rep')), may hold values from -100 to 100
- truncation: int32 [16], replicated, may hold values from 16 to 64
- neighbours: int32 [50, 16384], P(None, ('grp', 'rep')), may hold values from 0 to 16383, as said below
- initial: float32 [32, 16384], P(None, ('grp', 'rep')), may hold values from -6 to 6
Outputs:
- alignment: float32 [2, 50, 16384], P(None, None, ('grp', 'rep'))
- vectors: float32 [32, 16384], P(None, ('grp', 'rep'))
The draws below stay inside these ranges and needn't reach their ends.
Inputs may be any that keep to these rules, and one draw needn't show every extreme that they name: `neighbours`: every neighbour of a particle is another particle of the same block of 2048 particles that holds it (the particles of one group of 16 devices along rep). For each device, the neighbour slots of its 128 particles that name particles of one other device number at most 64; every device has, in every draw, one other device that its slots name exactly 64 times.
All inputs are finite; a program needn't handle non-finite values.
Results may differ from the reference program's by a relative error of at most 0.0003.
Values may be sent and summed in bfloat16 or wider, within the bound.
No kernel may reach another device: no remote copies, remote signals or barrier semaphores. Data moves between devices by JAX's collectives and lax.ppermute only.
A program may use at most 128 MiB of HBM per device.

```python
import math
import jax
import jax.numpy as jnp
from jax import lax

ANG = 64
RAD = 16
ANGLES = 256
NB = 50
VEC = 16
ITERS = 3
P_DEV = 128
CAP = 64
CW = 2048
NPART = 16384
N_REP = 16


def draw_coefficients(key, part):
    scale_key, noise_key = jax.random.split(key, 2)
    row_scale = jnp.exp(jax.random.uniform(scale_key, (NPART, 1), jnp.float32, 0.0, math.log(10.0)))
    noise = jnp.clip(jax.random.normal(noise_key, (NPART, CW), jnp.float32), -6.0, 6.0)
    return (row_scale * noise).astype(jnp.bfloat16)


def draw_neighbours(key, part):
    devices = NPART // P_DEV
    slots = NB * P_DEV
    peers = N_REP - 1
    count_key, complete_random_key, order_key, near_key, far_key = jax.random.split(key, 5)
    counts = jax.random.randint(count_key, (devices, peers), CAP // 4, CAP // 2 + 1)
    chosen = jax.random.randint(complete_random_key, (devices, 1), 0, peers)
    counts = jnp.where(jnp.arange(peers, dtype=jnp.int32)[None, :] == chosen, CAP, counts).astype(jnp.int32)
    bounds = jnp.cumsum(counts, axis=1).astype(jnp.int32)
    order_keys = jax.random.split(order_key, devices)
    ranks = jax.vmap(lambda single: jax.random.permutation(single, slots))(order_keys).astype(jnp.int32)
    offsets = jax.vmap(lambda edges, values: jnp.searchsorted(edges, values, side='right'))(bounds, ranks).astype(jnp.int32)
    remote = offsets < peers
    device_ids = jnp.arange(devices, dtype=jnp.int32)[:, None]
    own_rep = device_ids % N_REP
    group_start = device_ids // N_REP * (N_REP * P_DEV)
    peer_rep = (own_rep + 1 + offsets) % N_REP
    particle = jnp.arange(slots, dtype=jnp.int32)[None, :] % P_DEV
    near = (particle + jax.random.randint(near_key, (devices, slots), 1, P_DEV)) % P_DEV
    far = jax.random.randint(far_key, (devices, slots), 0, P_DEV)
    owner_rep = jnp.where(remote, peer_rep, own_rep)
    within = jnp.where(remote, far, near)
    global_ids = group_start + owner_rep * P_DEV + within
    return global_ids.reshape(devices, NB, P_DEV).transpose(1, 0, 2).reshape(NB, NPART).astype(jnp.int32)


def set_ends(drawn, rng, low, top_value):
    longest = drawn.shape.index(max(drawn.shape))
    spots = []
    for shift in (0, 1):
        where = [jax.random.randint(jax.random.fold_in(rng, axis), (), 0, length) for axis, length in enumerate(drawn.shape)]
        where[longest] = (where[longest] + shift) % drawn.shape[longest]
        spots.append(tuple(where))
    return drawn.at[spots[0]].set(low).at[spots[1]].set(top_value)


def shard_levels(stream_key, dims, pieces, low, largest):
    loudness = 1.0
    for dim, parts in pieces:
        steps = jax.random.uniform(jax.random.fold_in(jax.random.fold_in(stream_key, 6), dim), (parts,), jnp.float32, low / len(pieces), largest / len(pieces))
        loudness = loudness * jnp.repeat(jnp.exp(steps), dims[dim] // parts).reshape((-1,) + (1,) * (len(dims) - 1 - dim))
    return loudness


def bell_draw(rng, dims, deviation, most, cuts=(), kind=jnp.bfloat16):
    entries = jax.random.normal(rng, dims, jnp.float32) * deviation
    if len(cuts) > 0:
        entries = shard_levels(rng, dims, cuts, -0.22, 0.18) * entries
    return jnp.clip(entries, min=-most, max=most).astype(kind)


def setup_inputs(seed: int = 0) -> dict:
    seeds = jax.random.split(jax.random.key(seed), 5)
    coefficients = draw_coefficients(jax.random.fold_in(seeds[4], 71), 0)
    truncation = set_ends(jax.random.randint(seeds[1], (RAD,), ANG // 4, ANG + 1), jax.random.fold_in(seeds[1], 1), ANG // 4, ANG).astype(jnp.int32)
    neighbours = draw_neighbours(jax.random.fold_in(seeds[4], 71), 0)
    initial = bell_draw(seeds[3], (2 * VEC, NPART), 1.0, 6.0, ((1, 128),), jnp.float32)
    return {"coefficients": coefficients, "truncation": truncation, "neighbours": neighbours, "initial": initial}


epsilon = 1e-06

def rotation_angle_grid(angular, samples):
    frequency = jnp.arange(angular, dtype=jnp.float32)
    sample_angle = jnp.arange(samples, dtype=jnp.float32) * (2.0 * math.pi / samples)
    phases = frequency[:, None] * sample_angle[None, :]
    transform = jnp.concatenate([jnp.cos(phases), -jnp.sin(phases)], axis=0)
    return (transform, jnp.cos(sample_angle), jnp.sin(sample_angle))

def kept_mask(truncation):
    levels = jnp.arange(ANG, dtype=jnp.int32)
    return (levels[None, :] < truncation[:, None]).astype(jnp.float32)

def pair_moments(own_rows, other_rows, weights, transform, cosine_row, sine_row):
    row_count = own_rows.shape[0]
    local_complete = own_rows.astype(jnp.float32).reshape(row_count, 2, RAD, ANG) * weights
    partner_complete = other_rows.astype(jnp.float32).reshape(NB, row_count, 2, RAD, ANG)
    maximum_frequency = lax.Precision.HIGHEST
    real_fourier_coeffs = jnp.einsum('fwh,rfwh->rfh', local_complete[:, 0], partner_complete[:, :, 0], precision=maximum_frequency)
    real_fourier_coeffs = real_fourier_coeffs + jnp.einsum('fwh,rfwh->rfh', local_complete[:, 1], partner_complete[:, :, 1], precision=maximum_frequency)
    imaginary_fourier_coeffs = jnp.einsum('fwh,rfwh->rfh', local_complete[:, 1], partner_complete[:, :, 0], precision=maximum_frequency)
    imaginary_fourier_coeffs = imaginary_fourier_coeffs - jnp.einsum('fwh,rfwh->rfh', local_complete[:, 0], partner_complete[:, :, 1], precision=maximum_frequency)
    spectrum = jnp.concatenate([real_fourier_coeffs, imaginary_fourier_coeffs], axis=2)
    correlation = jnp.einsum('nbk,km->nbm', spectrum, transform, precision=maximum_frequency)
    squared = correlation * correlation
    energy = jnp.mean(squared, axis=2)
    moment_real = jnp.mean(squared * cosine_row, axis=2)
    moment_imaginary = jnp.mean(squared * sine_row, axis=2)
    return (energy, moment_real, moment_imaginary)

def lower_inverse(lower):
    matrix_order = lower.shape[0]
    identity = jnp.eye(matrix_order, dtype=lower.dtype)
    inverse_rows = []
    for target in range(matrix_order):
        running = identity[target]
        for source in range(target):
            running = running - lower[target, source] * inverse_rows[source]
        inverse_rows.append(running / lower[target, target])
    return jnp.stack(inverse_rows)

def reference(coefficients, truncation, neighbours, initial):
    maximum_frequency = lax.Precision.HIGHEST
    weights = kept_mask(truncation)
    transform, cosine_row, sine_row = rotation_angle_grid(ANG, ANGLES)
    particle_total = coefficients.shape[0]
    block_width = math.gcd(particle_total, 128)
    blocks = particle_total // block_width
    own_blocks = coefficients.reshape(blocks, block_width, coefficients.shape[1])
    index_blocks = neighbours.reshape(NB, blocks, block_width).transpose(1, 0, 2)

    def one_block(operands):
        own_rows, indices = operands
        other_rows = jnp.take(coefficients, indices.reshape(-1), axis=0)
        return pair_moments(own_rows, other_rows, weights, transform, cosine_row, sine_row)
    energy, moment_real, moment_imaginary = lax.map(one_block, (own_blocks, index_blocks))
    energy = energy.transpose(1, 0, 2).reshape(NB, particle_total)
    moment_real = moment_real.transpose(1, 0, 2).reshape(NB, particle_total)
    moment_imaginary = moment_imaginary.transpose(1, 0, 2).reshape(NB, particle_total)
    alignment = jnp.stack([moment_real / (energy + epsilon), moment_imaginary / (energy + epsilon)])
    degree = epsilon + jnp.sum(energy, axis=0)
    current = initial
    vector_count = initial.shape[0] // 2
    for iteration in range(ITERS):
        picked = jnp.take(current, neighbours.reshape(-1), axis=1).reshape(current.shape[0], NB, particle_total)
        real_part = picked[:vector_count]
        imag_part = picked[vector_count:]
        image_real = jnp.sum(moment_real * real_part - moment_imaginary * imag_part, axis=1) / degree
        image_imag = jnp.sum(moment_real * imag_part + moment_imaginary * real_part, axis=1) / degree
        gram_matrix = (jnp.dot(image_real, image_real.T, precision=maximum_frequency) + jnp.dot(image_imag, image_imag.T, precision=maximum_frequency)) / particle_total
        inverse = lower_inverse(jnp.linalg.cholesky(gram_matrix))
        current = jnp.concatenate([jnp.dot(inverse, image_real, precision=maximum_frequency), jnp.dot(inverse, image_imag, precision=maximum_frequency)], axis=0)
    return (alignment, current)
```

```python
import functools

import jax
import jax.numpy as jnp
from jax import lax
from jax.experimental import pallas as pl
from jax.experimental.pallas import tpu as pltpu
from jax.sharding import Mesh
from jax.sharding import PartitionSpec as P

ANG = 64
RAD = 16
NB = 50
NBP = 56
VEC = 16
PD = 128
CAP = 64
CW = 2048
XW = CW + 128
PEERS = 16
PAIRS = PEERS // 2
GRP = ("grp_0", "grp_1")
REP = ("rep_0", "rep_1")
GRP_REP = ("grp_0", "grp_1", "rep_0", "rep_1")
EPS = 1e-06
F32 = jnp.float32
BF16 = jnp.bfloat16
HIGHEST = lax.Precision.HIGHEST

NT = (((1,), (1,)), ((), ()))
TN = (((0,), (0,)), ((), ()))


def iota(shape, dim):
    return lax.broadcasted_iota(jnp.int32, shape, dim)


def one_hot(cond):
    return jnp.where(cond, 1.0, 0.0).astype(BF16)


def three_parts(x):
    high = x.astype(BF16)
    rest = x - high.astype(F32)
    mid = rest.astype(BF16)
    low = (rest - mid.astype(F32)).astype(BF16)
    return jnp.concatenate([high, mid, low], axis=0)


def exact_select(x, selector, dims=(((1,), (0,)), ((), ()))):
    rows = x.shape[0]
    parts = lax.dot_general(three_parts(x), selector, dims, preferred_element_type=F32)
    return parts[:rows] + (parts[rows : 2 * rows] + parts[2 * rows :])


def kept_rows(trunc_ref, rows, lanes):
    row = iota((rows, lanes), 0) % RAD
    kept = jnp.zeros((rows, lanes), jnp.int32)
    for q in range(RAD):
        kept = jnp.where(row == q, trunc_ref[q], kept)
    return kept


def slot_kernel(where_ref, nb_ref, code_ref, lists_ref, req_ref, nbp_ref, a_ref, b_ref):
    nbp_ref[...] = jnp.full((NBP, PD), -1, jnp.int32)
    nbp_ref[:NB, :] = nb_ref[...] - where_ref[0]
    local = nbp_ref[...]
    me = where_ref[1]
    owner = local >> 7
    within = local & (PD - 1)
    remote = (owner != me) & (local >= 0)
    owner = jnp.where(remote, owner, -1)
    masks = [one_hot(owner == p) for p in range(PEERS)]
    before = one_hot(iota((NBP, NBP), 0) > iota((NBP, NBP), 1))
    in_column = jnp.dot(before, jnp.concatenate(masks, axis=1), preferred_element_type=F32)
    totals = jnp.concatenate(
        [jnp.sum(m.astype(F32), axis=0, keepdims=True) for m in masks], axis=0
    )
    left = one_hot(iota((PD, PD), 0) < iota((PD, PD), 1))
    columns = jnp.dot(totals.astype(BF16), left, preferred_element_type=F32)
    rank = jnp.zeros((NBP, PD), F32)
    for p in range(PEERS):
        here = in_column[:, p * PD : (p + 1) * PD] + columns[p : p + 1, :]
        rank = jnp.where(owner == p, here, rank)
    rank = rank.astype(jnp.int32)
    code = jnp.where(remote, owner * CAP + rank, -1)
    code_ref[...] = code
    pair = code >> 7
    lane = jnp.where(remote, code & (PD - 1), -1)
    particle = iota((1, PD), 1).astype(F32) + 1.0
    rows8 = iota((PAIRS, PD), 0)
    rows128 = iota((PD, PD), 0)
    for n in range(NB):
        mine = rows8 == pair[n : n + 1, :]
        names = within[n : n + 1, :].astype(F32)
        both = jnp.concatenate(
            [jnp.where(mine, names, 0.0), jnp.where(mine, particle, 0.0)], axis=0
        )
        a_ref[:, n * PD : (n + 1) * PD] = both.astype(BF16)
        b_ref[:, n * PD : (n + 1) * PD] = one_hot(rows128 == lane[n : n + 1, :])
    lists = lax.dot_general(a_ref[...], b_ref[...], NT, preferred_element_type=F32)
    lists_ref[...] = lists
    turned = pltpu.roll(lists[:PAIRS], CAP, 1)
    for p in range(PEERS):
        row = (turned if p % 2 else lists)[p // 2 : p // 2 + 1, :]
        req_ref[p] = jnp.broadcast_to(row, (8, PD))


def wanted_row(rx_ref, r):
    even = rx_ref[2 * r][:1, :]
    odd = pltpu.roll(rx_ref[2 * r + 1], CAP, 1)[:1, :]
    return jnp.where(iota((1, PD), 1) < CAP, even, odd).astype(jnp.int32)


def pick_kernel(rx_ref, coef_ref, init_ref, out_ref, x_ref):
    r = pl.program_id(0)

    @pl.when(r == 0)
    def _():
        x_ref[:, :CW] = coef_ref[...]
        parts = three_parts(init_ref[...]).astype(F32)
        parts = jnp.concatenate([parts, jnp.zeros((32, PD), F32)], axis=0)
        x_ref[:, CW:] = parts.T.astype(BF16)

    row = jnp.broadcast_to(wanted_row(rx_ref, r), (PD, PD)).astype(F32).T
    pick = one_hot(row.astype(jnp.int32) == iota((PD, PD), 1))
    rows = jnp.dot(pick, x_ref[...], preferred_element_type=F32)
    out_ref[...] = rows.astype(BF16).reshape(2, CAP, XW)


def own_kernel(trunc_ref, coef_ref, e_ref, re_ref, im_ref, xt_ref, s_ref):
    for c in range(CW // PD):
        block = coef_ref[:, c * PD : (c + 1) * PD].astype(F32)
        xt_ref[c * PD : (c + 1) * PD, :] = block.T
    kept = kept_rows(trunc_ref, 2 * RAD, PD)

    def per_frequency(k, carry):
        rows = xt_ref[pl.ds(k, 2 * RAD, stride=ANG), :]
        masked = jnp.where(kept > k, rows, 0.0)
        turned = jnp.concatenate([masked[RAD:], -masked[:RAD]], axis=0)
        right = jnp.concatenate([masked, turned], axis=1).astype(BF16)
        s_ref[k] = lax.dot_general(
            rows.astype(BF16), right, TN, preferred_element_type=F32
        )
        return carry

    lax.fori_loop(0, ANG, per_frequency, 0, unroll=4)

    def per_rows(b, carry):
        sub = pl.ds(b * 8, 8)
        last_re = s_ref[0, sub, :PD]
        energy = last_re * last_re
        re = s_ref[1, sub, :PD]
        im = s_ref[1, sub, PD:]
        half = re * re + im * im
        first_re = last_re * re
        first_im = last_re * im
        m_re = jnp.zeros_like(re)
        m_im = jnp.zeros_like(re)
        for k in range(2, ANG):
            next_re = s_ref[k, sub, :PD]
            next_im = s_ref[k, sub, PD:]
            half = half + (next_re * next_re + next_im * next_im)
            m_re = m_re + (re * next_re + im * next_im)
            m_im = m_im + (im * next_re - re * next_im)
            re, im = next_re, next_im
        e_ref[sub, :] = energy + 0.5 * half
        re_ref[sub, :] = first_re + 0.5 * m_re
        im_ref[sub, :] = 0.5 * m_im - first_im
        return carry

    lax.fori_loop(0, PD // 8, per_rows, 0)


def far_kernel(trunc_ref, lists_ref, coef_ref, recv_ref, table_ref, cur_ref, own_ref):
    r = pl.program_id(0)

    @pl.when(r == 0)
    def _():
        lane = iota((1, PD), 1)
        for c in range(CW // PD):
            q = (2 * c) % RAD
            kept = jnp.where(lane < ANG, trunc_ref[q], trunc_ref[q + 1])
            block = coef_ref[:, c * PD : (c + 1) * PD].astype(F32)
            own_ref[:, c * PD : (c + 1) * PD] = jnp.where(
                (lane & (ANG - 1)) < kept, block, 0.0
            ).astype(BF16)

    particle = lists_ref[pl.ds(PAIRS + r, 1), :]
    row = jnp.broadcast_to(particle, (PD, PD)).T.astype(jnp.int32)
    pick = one_hot(row == iota((PD, PD), 1) + 1)
    other = recv_ref[...].reshape(PD, XW)
    sum_re = jnp.zeros((PD, PD), F32)
    sum_im = jnp.zeros((PD, PD), F32)
    half = CW // 2
    for c in range(half // PD):
        lo = slice(c * PD, (c + 1) * PD)
        hi = slice(half + c * PD, half + (c + 1) * PD)
        a_re = jnp.dot(pick, own_ref[:, lo], preferred_element_type=F32)
        a_im = jnp.dot(pick, own_ref[:, hi], preferred_element_type=F32)
        b_re = other[:, lo].astype(F32)
        b_im = other[:, hi].astype(F32)
        sum_re = sum_re + (a_re * b_re + a_im * b_im)
        sum_im = sum_im + (a_im * b_re - a_re * b_im)
    s_re = sum_re.T
    s_im = sum_im.T
    s_re = s_re[:ANG] + s_re[ANG:]
    s_im = s_im[:ANG] + s_im[ANG:]
    power = s_re * s_re + s_im * s_im
    freq = iota((ANG, PD), 0)
    next_re = pltpu.roll(s_re, ANG - 1, 0)
    next_im = pltpu.roll(s_im, ANG - 1, 0)
    zero_re = s_re[:1]
    energy = zero_re * zero_re + 0.5 * jnp.sum(
        jnp.where(freq == 0, 0.0, power), axis=0, keepdims=True
    )
    inner = (freq > 0) & (freq < ANG - 1)
    m_re = zero_re * s_re[1:2] + 0.5 * jnp.sum(
        jnp.where(inner, s_re * next_re + s_im * next_im, 0.0), axis=0, keepdims=True
    )
    m_im = 0.5 * jnp.sum(
        jnp.where(inner, s_im * next_re - s_re * next_im, 0.0), axis=0, keepdims=True
    ) - zero_re * s_im[1:2]
    table_ref[0] = jnp.concatenate(
        [energy, m_re, m_im, jnp.zeros((5, PD), F32)], axis=0
    )
    parts = other[:, CW:].astype(F32).T
    cur_ref[0] = parts[:32] + (parts[32:64] + parts[64:96])


def near_image(cur, w_re, w_im):
    weights = jnp.concatenate([w_re, w_im], axis=1)
    both = jnp.dot(cur, weights, precision=HIGHEST, preferred_element_type=F32)
    re = both[:VEC, :PD] - both[VEC:, PD:]
    im = both[VEC:, :PD] + both[:VEC, PD:]
    return jnp.concatenate([re, im], axis=0)


def far_image(slots, table_ref, lists_ref):
    values = []
    picks = []
    for r in range(PAIRS):
        m_re = table_ref[r, 1:2, :]
        m_im = table_ref[r, 2:3, :]
        c_re, c_im = slots[r][:VEC], slots[r][VEC:]
        values.append(
            jnp.concatenate([m_re * c_re - m_im * c_im, m_re * c_im + m_im * c_re], axis=0)
        )
        particle = lists_ref[PAIRS + r : PAIRS + r + 1, :].astype(jnp.int32)
        picks.append(one_hot(iota((PD, PD), 0) + 1 == particle))
    return exact_select(
        jnp.concatenate(values, axis=1), jnp.concatenate(picks, axis=1), NT
    )


def send_columns(cur, rx_ref, out_ref):
    picks = [one_hot(iota((PD, PD), 0) == wanted_row(rx_ref, r)) for r in range(PAIRS)]
    columns = exact_select(cur, jnp.concatenate(picks, axis=1))
    first = iota((VEC, PD), 1) < CAP
    for r in range(PAIRS):
        re = columns[:VEC, r * PD : (r + 1) * PD]
        im = columns[VEC:, r * PD : (r + 1) * PD]
        out_ref[2 * r] = jnp.where(first, re, pltpu.roll(im, CAP, 1))
        out_ref[2 * r + 1] = jnp.where(first, pltpu.roll(re, CAP, 1), im)


def received_columns(recv_ref):
    first = iota((VEC, PD), 1) < CAP
    slots = []
    for r in range(PAIRS):
        even = recv_ref[2 * r]
        odd = recv_ref[2 * r + 1]
        re = jnp.where(first, even, pltpu.roll(odd, CAP, 1))
        im = jnp.where(first, pltpu.roll(even, CAP, 1), odd)
        slots.append(jnp.concatenate([re, im], axis=0))
    return slots


def first_kernel(
    where_ref, nb_ref, code_ref, lists_ref, table_ref, e_ref, re_ref, im_ref,
    slots_ref, init_ref, rx_ref,
    align_ref, weights_ref, degree_ref, cur_ref, send_ref, near_ref,
):
    local = nb_ref[...] - where_ref[0]
    near = (local >> 7) == where_ref[1]
    near_ref[...] = jnp.where(near, local & (PD - 1), -1)
    rows = iota((PD, PD), 0)
    counts = jnp.zeros((PD, PD), F32)
    energy = []
    m_re = []
    m_im = []
    for n in range(NB):
        mine = rows == near_ref[n : n + 1, :]
        counts = counts + jnp.where(mine, 1.0, 0.0)
        energy.append(jnp.sum(jnp.where(mine, e_ref[...], 0.0), axis=0, keepdims=True))
        m_re.append(jnp.sum(jnp.where(mine, re_ref[...], 0.0), axis=0, keepdims=True))
        m_im.append(jnp.sum(jnp.where(mine, im_ref[...], 0.0), axis=0, keepdims=True))
    pad = [jnp.zeros((NBP - NB, PD), F32)]
    values = [jnp.concatenate(v + pad, axis=0) for v in (energy, m_re, m_im)]
    code = code_ref[...]
    pair = code >> 7
    lane = code & (PD - 1)
    for r in range(PAIRS):
        mine = pair == r
        for v in range(3):
            row = jnp.broadcast_to(table_ref[r, v : v + 1, :], (NBP, PD))
            found = jnp.take_along_axis(row, lane, axis=1, mode="promise_in_bounds")
            values[v] = jnp.where(mine, found, values[v])
    below = values[0] + EPS
    align_ref[0] = (values[1] / below)[:NB]
    align_ref[1] = (values[2] / below)[:NB]
    degree = EPS + jnp.sum(values[0], axis=0, keepdims=True)
    degree_ref[...] = jnp.broadcast_to(degree, (8, PD))
    w_re = counts * re_ref[...]
    w_im = counts * im_ref[...]
    weights_ref[0] = w_re
    weights_ref[1] = w_im
    slots = [slots_ref[r] for r in range(PAIRS)]
    image = near_image(init_ref[...], w_re, w_im) + far_image(slots, table_ref, lists_ref)
    image = image / degree
    cur_ref[...] = image
    send_columns(image, rx_ref, send_ref)


def next_image(recv_ref, cur_ref, weights_ref, degree_ref, table_ref, lists_ref):
    slots = received_columns(recv_ref)
    image = near_image(cur_ref[...], weights_ref[0], weights_ref[1])
    image = image + far_image(slots, table_ref, lists_ref)
    return image / degree_ref[:1, :]


def middle_kernel(
    recv_ref, cur_ref, weights_ref, degree_ref, table_ref, lists_ref, rx_ref,
    out_ref, send_ref,
):
    image = next_image(recv_ref, cur_ref, weights_ref, degree_ref, table_ref, lists_ref)
    out_ref[...] = image
    send_columns(image, rx_ref, send_ref)


def last_kernel(
    total, recv_ref, cur_ref, weights_ref, degree_ref, table_ref, lists_ref,
    out_ref, gram_ref,
):
    image = next_image(recv_ref, cur_ref, weights_ref, degree_ref, table_ref, lists_ref)
    out_ref[...] = image
    gram = lax.dot_general(
        image[:VEC], image[:VEC], NT, precision=HIGHEST, preferred_element_type=F32
    ) + lax.dot_general(
        image[VEC:], image[VEC:], NT, precision=HIGHEST, preferred_element_type=F32
    )
    gram = gram * (1.0 / total)
    wide = jnp.concatenate([gram] * 8, axis=1)
    mine = iota((VEC, PD), 1) // VEC == iota((VEC, PD), 0) % 8
    wide = jnp.where(mine, wide, 0.0)
    packed = jnp.concatenate(
        [
            jnp.sum(wide[:8], axis=0, keepdims=True),
            jnp.sum(wide[8:], axis=0, keepdims=True),
        ],
        axis=0,
    )
    gram_ref[...] = jnp.broadcast_to(packed[None], gram_ref.shape)


def finish_kernel(grams_ref, cur_ref, out_ref):
    packed = jnp.sum(grams_ref[...], axis=0)
    row = iota((VEC, PD), 0)
    lane = iota((VEC, PD), 1)
    wide = jnp.where(row < 8, packed[0:1, :], packed[1:2, :])
    wide = jnp.where(lane // VEC == row % 8, wide, 0.0)
    for shift in (64, 32, 16):
        wide = wide + pltpu.roll(wide, shift, 1)
    gram = wide
    re = cur_ref[:VEC, :]
    im = cur_ref[VEC:, :]
    for c in range(VEC):
        pivot = gram[c : c + 1, c : c + 1]
        scale = lax.rsqrt(pivot)
        scale = scale * (1.5 - 0.5 * pivot * scale * scale)
        column = gram[:, c : c + 1] * scale
        column = jnp.where(row[:, :1] > c, column, 0.0)
        top_gram = gram[c : c + 1, :] * scale
        top_re = re[c : c + 1, :] * scale
        top_im = im[c : c + 1, :] * scale
        here = row == c
        gram = gram - column * top_gram
        re = jnp.where(here, top_re, re - column * top_re)
        im = jnp.where(here, top_im, im - column * top_im)
    out_ref[:VEC, :] = re
    out_ref[VEC:, :] = im


def struct(shape, dtype=F32):
    return jax.ShapeDtypeStruct(shape, dtype)


SMEM = pl.BlockSpec(memory_space=pltpu.SMEM)
VMEM = pl.BlockSpec(memory_space=pltpu.VMEM)


def shards(coefficients, truncation, neighbours, initial):
    groups = lax.axis_size(GRP)
    replicas = lax.axis_size(REP)
    devices = groups * replicas
    place = jnp.stack(
        [lax.axis_index(GRP) * (replicas * PD), lax.axis_index(REP)]
    ).astype(jnp.int32)
    code, lists, requests = pl.pallas_call(
        slot_kernel,
        out_shape=(
            struct((NBP, PD), jnp.int32),
            struct((2 * PAIRS, PD)),
            struct((PEERS, 8, PD)),
        ),
        in_specs=[SMEM, VMEM],
        scratch_shapes=[
            pltpu.VMEM((NBP, PD), jnp.int32),
            pltpu.VMEM((2 * PAIRS, NB * PD), BF16),
            pltpu.VMEM((PD, NB * PD), BF16),
        ],
        name="slots",
    )(place, neighbours)
    asked = lax.all_to_all(requests, REP, 0, 0, tiled=True)
    e_own, re_own, im_own = pl.pallas_call(
        own_kernel,
        out_shape=(struct((PD, PD)),) * 3,
        in_specs=[SMEM, VMEM],
        scratch_shapes=[
            pltpu.VMEM((CW, PD), F32),
            pltpu.VMEM((ANG, PD, 2 * PD), F32),
        ],
        cost_estimate=pl.CostEstimate(
            flops=20_000_000_000, bytes_accessed=1_000_000, transcendentals=0
        ),
        name="own",
    )(truncation, coefficients)
    whole = lambda *shape: pl.BlockSpec(shape, lambda r: (0,) * len(shape))
    sent = pl.pallas_call(
        pick_kernel,
        grid=(PAIRS,),
        out_shape=struct((PEERS, CAP, XW), BF16),
        in_specs=[whole(PEERS, 8, PD), whole(PD, CW), whole(32, PD)],
        out_specs=pl.BlockSpec((2, CAP, XW), lambda r: (r, 0, 0)),
        scratch_shapes=[pltpu.VMEM((PD, XW), BF16)],
        name="pick",
    )(asked, coefficients, initial)
    received = lax.all_to_all(sent, REP, 0, 0, tiled=True)
    table, slots = pl.pallas_call(
        far_kernel,
        grid=(PAIRS,),
        out_shape=(struct((PAIRS, 8, PD)), struct((PAIRS, 32, PD))),
        in_specs=[
            SMEM,
            whole(2 * PAIRS, PD),
            whole(PD, CW),
            pl.BlockSpec((2, CAP, XW), lambda r: (r, 0, 0)),
        ],
        out_specs=(
            pl.BlockSpec((1, 8, PD), lambda r: (r, 0, 0)),
            pl.BlockSpec((1, 32, PD), lambda r: (r, 0, 0)),
        ),
        scratch_shapes=[pltpu.VMEM((PD, CW), BF16)],
        name="far",
    )(truncation, lists, coefficients, received)
    alignment, weights, degree, current, columns = pl.pallas_call(
        first_kernel,
        out_shape=(
            struct((2, NB, PD)),
            struct((2, PD, PD)),
            struct((8, PD)),
            struct((32, PD)),
            struct((PEERS, VEC, PD)),
        ),
        in_specs=[SMEM] + [VMEM] * 10,
        scratch_shapes=[pltpu.VMEM((NB, PD), jnp.int32)],
        name="first",
    )(
        place, neighbours, code, lists, table, e_own, re_own, im_own,
        slots, initial, asked,
    )
    columns = lax.all_to_all(columns, REP, 0, 0, tiled=True)
    current, columns = pl.pallas_call(
        middle_kernel,
        out_shape=(struct((32, PD)), struct((PEERS, VEC, PD))),
        name="middle",
    )(columns, current, weights, degree, table, lists, asked)
    columns = lax.all_to_all(columns, REP, 0, 0, tiled=True)
    current, gram = pl.pallas_call(
        functools.partial(last_kernel, float(PD * devices)),
        out_shape=(struct((32, PD)), struct((devices, 2, PD))),
        name="last",
    )(columns, current, weights, degree, table, lists)
    grams = lax.all_to_all(gram, GRP_REP, 0, 0, tiled=True)
    vectors = pl.pallas_call(
        finish_kernel, out_shape=struct((32, PD)), name="finish"
    )(grams, current)
    return (alignment, vectors)


def solution(mesh):
    split = Mesh(mesh.devices.reshape(4, 2, 4, 4), GRP_REP)
    in_specs = (P(GRP_REP, None), P(), P(None, GRP_REP), P(None, GRP_REP))
    out_specs = (P(None, None, GRP_REP), P(None, GRP_REP))
    return jax.shard_map(
        shards, mesh=split, in_specs=in_specs, out_specs=out_specs, check_vma=False
    )
```

```python
import functools

import jax
import jax.numpy as jnp
from jax import lax
from jax.experimental import pallas as pl
from jax.experimental.pallas import tpu as pltpu
from jax.sharding import Mesh
from jax.sharding import PartitionSpec as P

ANG = 64
RAD = 16
NB = 50
NBP = 56
VEC = 16
PD = 128
CAP = 64
CW = 2048
FULL = RAD * ANG
LEAST = 256
STEP = 64
HEAD = 2 * VEC
PEERS = 16
PAIRS = PEERS // 2
GRP = ("grp_0", "grp_1")
REP = ("rep_0", "rep_1")
GRP_REP = ("grp_0", "grp_1", "rep_0", "rep_1")
EPS = 1e-06
F32 = jnp.float32
BF16 = jnp.bfloat16
HIGHEST = lax.Precision.HIGHEST

NT = (((1,), (1,)), ((), ()))
TN = (((0,), (0,)), ((), ()))


def iota(shape, dim):
    return lax.broadcasted_iota(jnp.int32, shape, dim)


def one_hot(cond):
    return jnp.where(cond, 1.0, 0.0).astype(BF16)


def three_parts(x):
    high = x.astype(BF16)
    rest = x - high.astype(F32)
    mid = rest.astype(BF16)
    low = (rest - mid.astype(F32)).astype(BF16)
    return jnp.concatenate([high, mid, low], axis=0)


def two_parts(x):
    high = x.astype(BF16)
    rest = (x - high.astype(F32)).astype(BF16)
    return jnp.concatenate([high, rest], axis=0)


def exact_select(x, selector, dims=(((1,), (0,)), ((), ()))):
    rows = x.shape[0]
    parts = lax.dot_general(three_parts(x), selector, dims, preferred_element_type=F32)
    return parts[:rows] + (parts[rows : 2 * rows] + parts[2 * rows :])


def kept_rows(trunc_ref, rows, lanes):
    row = iota((rows, lanes), 0) % RAD
    kept = jnp.zeros((rows, lanes), jnp.int32)
    for q in range(RAD):
        kept = jnp.where(row == q, trunc_ref[q], kept)
    return kept


def slot_kernel(
    where_ref, nb_ref, code_ref, lists_ref, names_ref, req_ref, nbp_ref, a_ref, b_ref
):
    nbp_ref[...] = jnp.full((NBP, PD), -1, jnp.int32)
    nbp_ref[:NB, :] = nb_ref[...] - where_ref[0]
    local = nbp_ref[...]
    me = where_ref[1]
    owner = local >> 7
    within = local & (PD - 1)
    remote = (owner != me) & (local >= 0)
    owner = jnp.where(remote, owner, -1)
    masks = [one_hot(owner == p) for p in range(PEERS)]
    before = one_hot(iota((NBP, NBP), 0) > iota((NBP, NBP), 1))
    in_column = jnp.dot(before, jnp.concatenate(masks, axis=1), preferred_element_type=F32)
    totals = jnp.concatenate(
        [jnp.sum(m.astype(F32), axis=0, keepdims=True) for m in masks], axis=0
    )
    left = one_hot(iota((PD, PD), 0) < iota((PD, PD), 1))
    columns = jnp.dot(totals.astype(BF16), left, preferred_element_type=F32)
    rank = jnp.zeros((NBP, PD), F32)
    for p in range(PEERS):
        here = in_column[:, p * PD : (p + 1) * PD] + columns[p : p + 1, :]
        rank = jnp.where(owner == p, here, rank)
    rank = rank.astype(jnp.int32)
    code = jnp.where(remote, owner * CAP + rank, -1)
    code_ref[...] = code
    pair = code >> 7
    lane = jnp.where(remote, code & (PD - 1), -1)
    particle = iota((1, PD), 1).astype(F32) + 1.0
    rows8 = iota((PAIRS, PD), 0)
    rows128 = iota((PD, PD), 0)
    for n in range(NB):
        mine = rows8 == pair[n : n + 1, :]
        names = within[n : n + 1, :].astype(F32)
        both = jnp.concatenate(
            [jnp.where(mine, names, 0.0), jnp.where(mine, particle, 0.0)], axis=0
        )
        a_ref[:, n * PD : (n + 1) * PD] = both.astype(BF16)
        b_ref[:, n * PD : (n + 1) * PD] = one_hot(rows128 == lane[n : n + 1, :])
    lists = lax.dot_general(a_ref[...], b_ref[...], NT, preferred_element_type=F32)
    lists_ref[...] = lists[PAIRS:]
    turned = pltpu.roll(lists, CAP, 1)
    first = iota((2 * PAIRS, PD), 1) < CAP
    both = (jnp.where(first, lists, turned), jnp.where(first, turned, lists))
    for p in range(PEERS):
        rows = both[p % 2]
        r = p // 2
        req_ref[p] = jnp.broadcast_to(rows[r : r + 1, :], (8, PD))
        names_ref[p : p + 1, :] = rows[PAIRS + r : PAIRS + r + 1, :]


def wanted_row(rx_ref, r):
    even = rx_ref[2 * r][:1, :]
    odd = rx_ref[2 * r + 1][:1, :]
    return jnp.where(iota((1, PD), 1) < CAP, even, odd).astype(jnp.int32)


def pack_kernel(trunc_ref, coef_ref, init_ref, out_ref, f_ref, re_ref, im_ref):
    init = init_ref[...]
    parts = two_parts(jnp.concatenate([init[:VEC], init[VEC:]], axis=1))
    out_ref[:HEAD, :] = parts
    blocks = CW // PD
    for c in range(blocks):
        block = coef_ref[:, c * PD : (c + 1) * PD].astype(F32)
        f_ref[c * PD : (c + 1) * PD, :] = block.T
    offset = 0
    for q in range(RAD):
        here = pl.ds(offset, ANG)
        re_ref[here, :] = f_ref[q * ANG : (q + 1) * ANG, :]
        im_ref[here, :] = f_ref[(RAD + q) * ANG : (RAD + q + 1) * ANG, :]
        offset = offset + trunc_ref[q]
    for b in range(FULL // PD):
        rows = slice(b * PD, (b + 1) * PD)
        kept = iota((PD, PD), 0) + b * PD < offset
        out_ref[HEAD + b * PD : HEAD + (b + 1) * PD, :PD] = jnp.where(
            kept, re_ref[rows, :], 0.0
        ).astype(BF16)
        out_ref[HEAD + b * PD : HEAD + (b + 1) * PD, PD:] = jnp.where(
            kept, im_ref[rows, :], 0.0
        ).astype(BF16)


def pick_kernel(size, rx_ref, pack_ref, out_ref):
    r = pl.program_id(0)
    rows = iota((PD, PD), 0)
    first = iota((PD, PD), 1) < CAP
    sides = []
    for p in range(2):
        picked = rows == rx_ref[2 * r + p][:1, :].astype(jnp.int32)
        top = one_hot(picked & first)
        bottom = one_hot(picked & jnp.logical_not(first))
        sides.append(jnp.concatenate([top, bottom], axis=0))
    side = jnp.concatenate(sides, axis=1)
    chosen = jnp.dot(pack_ref[:size, :], side, preferred_element_type=F32).astype(BF16)
    out_ref[0] = chosen[:, :PD]
    out_ref[1] = chosen[:, PD:]


def own_kernel(trunc_ref, coef_ref, e_ref, re_ref, im_ref, xt_ref, s_ref):
    for c in range(CW // PD):
        block = coef_ref[:, c * PD : (c + 1) * PD].astype(F32)
        xt_ref[c * PD : (c + 1) * PD, :] = block.T
    kept = kept_rows(trunc_ref, 2 * RAD, PD)

    def per_frequency(k, carry):
        rows = xt_ref[pl.ds(k, 2 * RAD, stride=ANG), :]
        masked = jnp.where(kept > k, rows, 0.0)
        turned = jnp.concatenate([masked[RAD:], -masked[:RAD]], axis=0)
        right = jnp.concatenate([masked, turned], axis=1).astype(BF16)
        s_ref[k] = lax.dot_general(
            rows.astype(BF16), right, TN, preferred_element_type=F32
        )
        return carry

    lax.fori_loop(0, ANG, per_frequency, 0, unroll=4)

    def per_rows(b, carry):
        sub = pl.ds(b * 8, 8)
        last_re = s_ref[0, sub, :PD]
        energy = last_re * last_re
        re = s_ref[1, sub, :PD]
        im = s_ref[1, sub, PD:]
        half = re * re + im * im
        first_re = last_re * re
        first_im = last_re * im
        m_re = jnp.zeros_like(re)
        m_im = jnp.zeros_like(re)
        for k in range(2, ANG):
            next_re = s_ref[k, sub, :PD]
            next_im = s_ref[k, sub, PD:]
            half = half + (next_re * next_re + next_im * next_im)
            m_re = m_re + (re * next_re + im * next_im)
            m_im = m_im + (im * next_re - re * next_im)
            re, im = next_re, next_im
        e_ref[sub, :] = energy + 0.5 * half
        re_ref[sub, :] = first_re + 0.5 * m_re
        im_ref[sub, :] = 0.5 * m_im - first_im
        return carry

    lax.fori_loop(0, PD // 8, per_rows, 0)


def far_kernel(
    size, trunc_ref, names_ref, pack_ref, recv_ref, table_ref, cur_ref,
    same_ref, cross_ref, other_ref,
):
    r = pl.program_id(0)
    kept = size - HEAD

    @pl.when(r == 0)
    def _():
        same_ref[kept:, :] = jnp.zeros((ANG, PD), F32)
        cross_ref[kept:, :] = jnp.zeros((ANG, PD), F32)
        other_ref[kept:, :] = jnp.zeros((ANG, PD), F32)

    first = iota((PD, PD), 1) < CAP
    freq = iota((ANG, PD), 0)
    halves = []
    for p in range(2):
        named = iota((PD, PD), 0) + 1 == names_ref[pl.ds(2 * r + p, 1), :].astype(jnp.int32)
        low = one_hot(named & first)
        high = one_hot(named & jnp.logical_not(first))
        side = jnp.concatenate(
            [
                jnp.concatenate([low, high], axis=1),
                jnp.concatenate([high, low], axis=1),
            ],
            axis=0,
        )
        mine = jnp.dot(pack_ref[HEAD:size, :], side, preferred_element_type=F32)
        same_ref[:kept, :] = mine[:, :PD]
        cross_ref[:kept, :] = mine[:, PD:]
        other_ref[:kept, :] = recv_ref[p, HEAD:, :].astype(F32)
        sum_re = jnp.zeros((ANG, PD), F32)
        sum_im = jnp.zeros((ANG, PD), F32)
        offset = 0
        for q in range(RAD):
            here = pl.ds(offset, ANG)
            other = jnp.where(freq < trunc_ref[q], other_ref[here, :], 0.0)
            sum_re = sum_re + same_ref[here, :] * other
            sum_im = sum_im + cross_ref[here, :] * other
            offset = offset + trunc_ref[q]
        halves.append((sum_re, sum_im))
        parts = recv_ref[p, :HEAD, :].astype(F32)
        cur_ref[p] = parts[:VEC] + parts[VEC:]
    first = first[:ANG]
    s_re = jnp.where(first, halves[0][0], halves[1][0])
    s_re = s_re + pltpu.roll(jnp.where(first, halves[1][0], halves[0][0]), CAP, 1)
    s_im = pltpu.roll(jnp.where(first, halves[1][1], halves[0][1]), CAP, 1)
    s_im = jnp.where(first, halves[0][1] - s_im, s_im - halves[1][1])
    power = s_re * s_re + s_im * s_im
    next_re = pltpu.roll(s_re, ANG - 1, 0)
    next_im = pltpu.roll(s_im, ANG - 1, 0)
    zero_re = s_re[:1]
    energy = zero_re * zero_re + 0.5 * jnp.sum(
        jnp.where(freq == 0, 0.0, power), axis=0, keepdims=True
    )
    inner = (freq > 0) & (freq < ANG - 1)
    m_re = zero_re * s_re[1:2] + 0.5 * jnp.sum(
        jnp.where(inner, s_re * next_re + s_im * next_im, 0.0), axis=0, keepdims=True
    )
    m_im = 0.5 * jnp.sum(
        jnp.where(inner, s_im * next_re - s_re * next_im, 0.0), axis=0, keepdims=True
    ) - zero_re * s_im[1:2]
    table_ref[0] = jnp.concatenate(
        [energy, m_re, m_im, jnp.zeros((5, PD), F32)], axis=0
    )


def near_image(cur, w_re, w_im):
    weights = jnp.concatenate([w_re, w_im], axis=1)
    both = jnp.dot(cur, weights, precision=HIGHEST, preferred_element_type=F32)
    re = both[:VEC, :PD] - both[VEC:, PD:]
    im = both[VEC:, :PD] + both[:VEC, PD:]
    return jnp.concatenate([re, im], axis=0)


def far_image(slots, table_ref, lists_ref):
    values = []
    picks = []
    for r in range(PAIRS):
        m_re = table_ref[r, 1:2, :]
        m_im = table_ref[r, 2:3, :]
        c_re, c_im = slots[r][:VEC], slots[r][VEC:]
        values.append(
            jnp.concatenate([m_re * c_re - m_im * c_im, m_re * c_im + m_im * c_re], axis=0)
        )
        particle = lists_ref[r : r + 1, :].astype(jnp.int32)
        picks.append(one_hot(iota((PD, PD), 0) + 1 == particle))
    return exact_select(
        jnp.concatenate(values, axis=1), jnp.concatenate(picks, axis=1), NT
    )


def send_columns(cur, rx_ref, out_ref):
    picks = [one_hot(iota((PD, PD), 0) == wanted_row(rx_ref, r)) for r in range(PAIRS)]
    columns = exact_select(cur, jnp.concatenate(picks, axis=1))
    first = iota((VEC, PD), 1) < CAP
    for r in range(PAIRS):
        re = columns[:VEC, r * PD : (r + 1) * PD]
        im = columns[VEC:, r * PD : (r + 1) * PD]
        out_ref[2 * r] = jnp.where(first, re, pltpu.roll(im, CAP, 1))
        out_ref[2 * r + 1] = jnp.where(first, pltpu.roll(re, CAP, 1), im)


def received_columns(recv_ref):
    first = iota((VEC, PD), 1) < CAP
    slots = []
    for r in range(PAIRS):
        even = recv_ref[2 * r]
        odd = recv_ref[2 * r + 1]
        re = jnp.where(first, even, pltpu.roll(odd, CAP, 1))
        im = jnp.where(first, pltpu.roll(even, CAP, 1), odd)
        slots.append(jnp.concatenate([re, im], axis=0))
    return slots


def first_kernel(
    where_ref, nb_ref, code_ref, lists_ref, table_ref, e_ref, re_ref, im_ref,
    slots_ref, init_ref, rx_ref,
    align_ref, weights_ref, degree_ref, cur_ref, send_ref, near_ref,
):
    local = nb_ref[...] - where_ref[0]
    near = (local >> 7) == where_ref[1]
    near_ref[...] = jnp.where(near, local & (PD - 1), -1)
    rows = iota((PD, PD), 0)
    counts = jnp.zeros((PD, PD), F32)
    energy = []
    m_re = []
    m_im = []
    for n in range(NB):
        mine = rows == near_ref[n : n + 1, :]
        counts = counts + jnp.where(mine, 1.0, 0.0)
        energy.append(jnp.sum(jnp.where(mine, e_ref[...], 0.0), axis=0, keepdims=True))
        m_re.append(jnp.sum(jnp.where(mine, re_ref[...], 0.0), axis=0, keepdims=True))
        m_im.append(jnp.sum(jnp.where(mine, im_ref[...], 0.0), axis=0, keepdims=True))
    pad = [jnp.zeros((NBP - NB, PD), F32)]
    values = [jnp.concatenate(v + pad, axis=0) for v in (energy, m_re, m_im)]
    code = code_ref[...]
    pair = code >> 7
    lane = code & (PD - 1)
    for r in range(PAIRS):
        mine = pair == r
        for v in range(3):
            row = jnp.broadcast_to(table_ref[r, v : v + 1, :], (NBP, PD))
            found = jnp.take_along_axis(row, lane, axis=1, mode="promise_in_bounds")
            values[v] = jnp.where(mine, found, values[v])
    below = values[0] + EPS
    align_ref[0] = (values[1] / below)[:NB]
    align_ref[1] = (values[2] / below)[:NB]
    degree = EPS + jnp.sum(values[0], axis=0, keepdims=True)
    degree_ref[...] = jnp.broadcast_to(degree, (8, PD))
    w_re = counts * re_ref[...]
    w_im = counts * im_ref[...]
    weights_ref[0] = w_re
    weights_ref[1] = w_im
    slots = received_columns(slots_ref)
    image = near_image(init_ref[...], w_re, w_im) + far_image(slots, table_ref, lists_ref)
    image = image / degree
    cur_ref[...] = image
    send_columns(image, rx_ref, send_ref)


def next_image(recv_ref, cur_ref, weights_ref, degree_ref, table_ref, lists_ref):
    slots = received_columns(recv_ref)
    image = near_image(cur_ref[...], weights_ref[0], weights_ref[1])
    image = image + far_image(slots, table_ref, lists_ref)
    return image / degree_ref[:1, :]


def middle_kernel(
    recv_ref, cur_ref, weights_ref, degree_ref, table_ref, lists_ref, rx_ref,
    out_ref, send_ref,
):
    image = next_image(recv_ref, cur_ref, weights_ref, degree_ref, table_ref, lists_ref)
    out_ref[...] = image
    send_columns(image, rx_ref, send_ref)


def last_kernel(
    total, recv_ref, cur_ref, weights_ref, degree_ref, table_ref, lists_ref,
    out_ref, gram_ref,
):
    image = next_image(recv_ref, cur_ref, weights_ref, degree_ref, table_ref, lists_ref)
    out_ref[...] = image
    gram = lax.dot_general(
        image[:VEC], image[:VEC], NT, precision=HIGHEST, preferred_element_type=F32
    ) + lax.dot_general(
        image[VEC:], image[VEC:], NT, precision=HIGHEST, preferred_element_type=F32
    )
    gram = gram * (1.0 / total)
    wide = jnp.concatenate([gram] * 8, axis=1)
    mine = iota((VEC, PD), 1) // VEC == iota((VEC, PD), 0) % 8
    wide = jnp.where(mine, wide, 0.0)
    packed = jnp.concatenate(
        [
            jnp.sum(wide[:8], axis=0, keepdims=True),
            jnp.sum(wide[8:], axis=0, keepdims=True),
        ],
        axis=0,
    )
    gram_ref[...] = jnp.broadcast_to(packed[None], gram_ref.shape)


def finish_kernel(grams_ref, cur_ref, out_ref):
    packed = jnp.sum(grams_ref[...], axis=0)
    row = iota((VEC, PD), 0)
    lane = iota((VEC, PD), 1)
    wide = jnp.where(row < 8, packed[0:1, :], packed[1:2, :])
    wide = jnp.where(lane // VEC == row % 8, wide, 0.0)
    for shift in (64, 32, 16):
        wide = wide + pltpu.roll(wide, shift, 1)
    gram = wide
    re = cur_ref[:VEC, :]
    im = cur_ref[VEC:, :]
    for c in range(VEC):
        pivot = gram[c : c + 1, c : c + 1]
        scale = lax.rsqrt(pivot)
        scale = scale * (1.5 - 0.5 * pivot * scale * scale)
        column = gram[:, c : c + 1] * scale
        column = jnp.where(row[:, :1] > c, column, 0.0)
        top_gram = gram[c : c + 1, :] * scale
        top_re = re[c : c + 1, :] * scale
        top_im = im[c : c + 1, :] * scale
        here = row == c
        gram = gram - column * top_gram
        re = jnp.where(here, top_re, re - column * top_re)
        im = jnp.where(here, top_im, im - column * top_im)
    out_ref[:VEC, :] = re
    out_ref[VEC:, :] = im


def struct(shape, dtype=F32):
    return jax.ShapeDtypeStruct(shape, dtype)


SMEM = pl.BlockSpec(memory_space=pltpu.SMEM)
VMEM = pl.BlockSpec(memory_space=pltpu.VMEM)


def whole(*shape):
    return pl.BlockSpec(shape, lambda r: (0,) * len(shape))


def exchange(size, truncation, coefficients, names, asked, packed):
    sent = pl.pallas_call(
        functools.partial(pick_kernel, size),
        grid=(PAIRS,),
        out_shape=struct((PEERS, size, PD), BF16),
        in_specs=[whole(PEERS, 8, PD), whole(HEAD + FULL, 2 * PD)],
        out_specs=pl.BlockSpec((2, size, PD), lambda r: (r, 0, 0)),
        name="pick",
    )(asked, packed)
    received = lax.all_to_all(sent, REP, 0, 0, tiled=True)
    own = pl.pallas_call(
        own_kernel,
        out_shape=(struct((PD, PD)),) * 3,
        in_specs=[SMEM, VMEM],
        scratch_shapes=[
            pltpu.VMEM((CW, PD), F32),
            pltpu.VMEM((ANG, PD, 2 * PD), F32),
        ],
        cost_estimate=pl.CostEstimate(
            flops=20_000_000_000, bytes_accessed=1_000_000, transcendentals=0
        ),
        name="own",
    )(truncation, coefficients)
    far = pl.pallas_call(
        functools.partial(far_kernel, size),
        grid=(PAIRS,),
        out_shape=(struct((PAIRS, 8, PD)), struct((PEERS, VEC, PD))),
        in_specs=[
            SMEM,
            whole(PEERS, PD),
            whole(HEAD + FULL, 2 * PD),
            pl.BlockSpec((2, size, PD), lambda r: (r, 0, 0)),
        ],
        out_specs=(
            pl.BlockSpec((1, 8, PD), lambda r: (r, 0, 0)),
            pl.BlockSpec((2, VEC, PD), lambda r: (r, 0, 0)),
        ),
        scratch_shapes=[pltpu.VMEM((size - HEAD + ANG, PD), F32)] * 3,
        name="far",
    )(truncation, names, packed, received)
    return (*own, *far)


def shards(coefficients, truncation, neighbours, initial):
    groups = lax.axis_size(GRP)
    replicas = lax.axis_size(REP)
    devices = groups * replicas
    place = jnp.stack(
        [lax.axis_index(GRP) * (replicas * PD), lax.axis_index(REP)]
    ).astype(jnp.int32)
    code, lists, names, requests = pl.pallas_call(
        slot_kernel,
        out_shape=(
            struct((NBP, PD), jnp.int32),
            struct((PAIRS, PD)),
            struct((PEERS, PD)),
            struct((PEERS, 8, PD)),
        ),
        in_specs=[SMEM, VMEM],
        scratch_shapes=[
            pltpu.VMEM((NBP, PD), jnp.int32),
            pltpu.VMEM((2 * PAIRS, NB * PD), BF16),
            pltpu.VMEM((PD, NB * PD), BF16),
        ],
        name="slots",
    )(place, neighbours)
    asked = lax.all_to_all(requests, REP, 0, 0, tiled=True)
    packed = pl.pallas_call(
        pack_kernel,
        out_shape=struct((HEAD + FULL, 2 * PD), BF16),
        in_specs=[SMEM, VMEM, VMEM],
        scratch_shapes=[
            pltpu.VMEM((CW, PD), F32),
            pltpu.VMEM((FULL + ANG, PD), F32),
            pltpu.VMEM((FULL + ANG, PD), F32),
        ],
        cost_estimate=pl.CostEstimate(
            flops=5_000_000_000, bytes_accessed=1_000_000, transcendentals=0
        ),
        name="pack",
    )(truncation, coefficients, initial)
    sizes = list(range(LEAST, FULL + 1, STEP))
    total = jnp.sum(truncation)
    which = jnp.clip((total - LEAST + STEP - 1) // STEP, 0, len(sizes) - 1)
    e_own, re_own, im_own, table, slots = lax.switch(
        which,
        [functools.partial(exchange, HEAD + size) for size in sizes],
        truncation, coefficients, names, asked, packed,
    )
    alignment, weights, degree, current, columns = pl.pallas_call(
        first_kernel,
        out_shape=(
            struct((2, NB, PD)),
            struct((2, PD, PD)),
            struct((8, PD)),
            struct((32, PD)),
            struct((PEERS, VEC, PD)),
        ),
        in_specs=[SMEM] + [VMEM] * 10,
        scratch_shapes=[pltpu.VMEM((NB, PD), jnp.int32)],
        name="first",
    )(
        place, neighbours, code, lists, table, e_own, re_own, im_own,
        slots, initial, asked,
    )
    columns = lax.all_to_all(columns, REP, 0, 0, tiled=True)
    current, columns = pl.pallas_call(
        middle_kernel,
        out_shape=(struct((32, PD)), struct((PEERS, VEC, PD))),
        name="middle",
    )(columns, current, weights, degree, table, lists, asked)
    columns = lax.all_to_all(columns, REP, 0, 0, tiled=True)
    current, gram = pl.pallas_call(
        functools.partial(last_kernel, float(PD * devices)),
        out_shape=(struct((32, PD)), struct((devices, 2, PD))),
        name="last",
    )(columns, current, weights, degree, table, lists)
    grams = lax.all_to_all(gram, GRP_REP, 0, 0, tiled=True)
    vectors = pl.pallas_call(
        finish_kernel, out_shape=struct((32, PD)), name="finish"
    )(grams, current)
    return (alignment, vectors)


def solution(mesh):
    split = Mesh(mesh.devices.reshape(4, 2, 4, 4), GRP_REP)
    in_specs = (P(GRP_REP, None), P(), P(None, GRP_REP), P(None, GRP_REP))
    out_specs = (P(None, None, GRP_REP), P(None, GRP_REP))
    return jax.shard_map(
        shards, mesh=split, in_specs=in_specs, out_specs=out_specs, check_vma=False
    )
```

```python
import functools

import jax
import jax.numpy as jnp
from jax import lax
from jax.experimental import pallas as pl
from jax.experimental.pallas import tpu as pltpu
from jax.sharding import Mesh
from jax.sharding import PartitionSpec as P

ANG = 64
RAD = 16
NB = 50
NBP = 56
VEC = 16
PD = 128
CAP = 64
CW = 2048
FULL = RAD * ANG
SIZES = (384, 512, 576, 640, 704, 768, 896, FULL)
HEAD = 2 * VEC
PEERS = 16
PAIRS = PEERS // 2
WIDE = 4
GRP = ("grp_0", "grp_1")
REP = ("rep_0", "rep_1")
GRP_REP = ("grp_0", "grp_1", "rep_0", "rep_1")
EPS = 1e-06
F32 = jnp.float32
BF16 = jnp.bfloat16
HIGHEST = lax.Precision.HIGHEST

NT = (((1,), (1,)), ((), ()))
TN = (((0,), (0,)), ((), ()))


def iota(shape, dim):
    return lax.broadcasted_iota(jnp.int32, shape, dim)


def one_hot(cond):
    return jnp.where(cond, 1.0, 0.0).astype(BF16)


def three_parts(x):
    high = x.astype(BF16)
    rest = x - high.astype(F32)
    mid = rest.astype(BF16)
    low = (rest - mid.astype(F32)).astype(BF16)
    return jnp.concatenate([high, mid, low], axis=0)


def two_parts(x):
    high = x.astype(BF16)
    rest = (x - high.astype(F32)).astype(BF16)
    return jnp.concatenate([high, rest], axis=0)


def exact_select(x, selector, dims=(((1,), (0,)), ((), ()))):
    rows = x.shape[0]
    parts = lax.dot_general(three_parts(x), selector, dims, preferred_element_type=F32)
    return parts[:rows] + (parts[rows : 2 * rows] + parts[2 * rows :])


def kept_rows(trunc_ref, rows, lanes):
    row = iota((rows, lanes), 0) % RAD
    kept = jnp.zeros((rows, lanes), jnp.int32)
    for q in range(RAD):
        kept = jnp.where(row == q, trunc_ref[q], kept)
    return kept


def slot_kernel(
    where_ref, nb_ref, code_ref, lists_ref, names_ref, req_ref, nbp_ref, a_ref, b_ref
):
    nbp_ref[...] = jnp.full((NBP, PD), -1, jnp.int32)
    nbp_ref[:NB, :] = nb_ref[...] - where_ref[0]
    local = nbp_ref[...]
    me = where_ref[1]
    owner = local >> 7
    within = local & (PD - 1)
    remote = (owner != me) & (local >= 0)
    owner = jnp.where(remote, owner, -1)
    masks = [one_hot(owner == p) for p in range(PEERS)]
    before = one_hot(iota((NBP, NBP), 0) > iota((NBP, NBP), 1))
    in_column = jnp.dot(before, jnp.concatenate(masks, axis=1), preferred_element_type=F32)
    totals = jnp.concatenate(
        [jnp.sum(m.astype(F32), axis=0, keepdims=True) for m in masks], axis=0
    )
    left = one_hot(iota((PD, PD), 0) < iota((PD, PD), 1))
    columns = jnp.dot(totals.astype(BF16), left, preferred_element_type=F32)
    rank = jnp.zeros((NBP, PD), F32)
    for p in range(PEERS):
        here = in_column[:, p * PD : (p + 1) * PD] + columns[p : p + 1, :]
        rank = jnp.where(owner == p, here, rank)
    rank = rank.astype(jnp.int32)
    code = jnp.where(remote, owner * CAP + rank, -1)
    code_ref[...] = code
    pair = code >> 7
    lane = jnp.where(remote, code & (PD - 1), -1)
    particle = iota((1, PD), 1).astype(F32) + 1.0
    rows8 = iota((PAIRS, PD), 0)
    rows128 = iota((PD, PD), 0)
    for n in range(NB):
        mine = rows8 == pair[n : n + 1, :]
        names = within[n : n + 1, :].astype(F32)
        both = jnp.concatenate(
            [jnp.where(mine, names, 0.0), jnp.where(mine, particle, 0.0)], axis=0
        )
        a_ref[:, n * PD : (n + 1) * PD] = both.astype(BF16)
        b_ref[:, n * PD : (n + 1) * PD] = one_hot(rows128 == lane[n : n + 1, :])
    lists = lax.dot_general(a_ref[...], b_ref[...], NT, preferred_element_type=F32)
    lists_ref[...] = lists[PAIRS:]
    turned = pltpu.roll(lists, CAP, 1)
    first = iota((2 * PAIRS, PD), 1) < CAP
    both = (jnp.where(first, lists, turned), jnp.where(first, turned, lists))
    for p in range(PEERS):
        rows = both[p % 2]
        r = p // 2
        req_ref[p] = jnp.broadcast_to(rows[r : r + 1, :], (8, PD))
        names_ref[p : p + 1, :] = rows[PAIRS + r : PAIRS + r + 1, :]


def wanted_row(rx_ref, r):
    even = rx_ref[2 * r][:1, :]
    odd = rx_ref[2 * r + 1][:1, :]
    return jnp.where(iota((1, PD), 1) < CAP, even, odd).astype(jnp.int32)


def local_kernel(
    trunc_ref, coef_ref, init_ref, out_ref, e_ref, re_ref, im_ref,
    f_ref, wide_re_ref, wide_im_ref, s_ref,
):
    init = init_ref[...]
    parts = two_parts(jnp.concatenate([init[:VEC], init[VEC:]], axis=1))
    out_ref[:HEAD, :] = parts
    for c in range(CW // PD):
        block = coef_ref[:, c * PD : (c + 1) * PD].astype(F32)
        f_ref[c * PD : (c + 1) * PD, :] = block.T
    offset = 0
    for q in range(RAD):
        here = pl.ds(offset, ANG)
        wide_re_ref[here, :] = f_ref[q * ANG : (q + 1) * ANG, :]
        wide_im_ref[here, :] = f_ref[(RAD + q) * ANG : (RAD + q + 1) * ANG, :]
        offset = offset + trunc_ref[q]
    for b in range(FULL // PD):
        rows = slice(b * PD, (b + 1) * PD)
        to = slice(HEAD + b * PD, HEAD + (b + 1) * PD)
        kept = iota((PD, PD), 0) + b * PD < offset
        out_ref[to, :PD] = jnp.where(kept, wide_re_ref[rows, :], 0.0).astype(BF16)
        out_ref[to, PD:] = jnp.where(kept, wide_im_ref[rows, :], 0.0).astype(BF16)
    own_pairs(trunc_ref, e_ref, re_ref, im_ref, f_ref, s_ref)


def pick_kernel(size, rx_ref, pack_ref, out_ref):
    r = pl.program_id(0)
    rows = iota((PD, PD), 0)
    first = iota((PD, PD), 1) < CAP
    sides = []
    for p in range(WIDE):
        picked = rows == rx_ref[WIDE * r + p][:1, :].astype(jnp.int32)
        top = one_hot(picked & first)
        bottom = one_hot(picked & jnp.logical_not(first))
        sides.append(jnp.concatenate([top, bottom], axis=0))
    side = jnp.concatenate(sides, axis=1)
    chosen = jnp.dot(pack_ref[:size, :], side, preferred_element_type=F32).astype(BF16)
    for p in range(WIDE):
        out_ref[p] = chosen[:, p * PD : (p + 1) * PD]


def own_pairs(trunc_ref, e_ref, re_ref, im_ref, xt_ref, s_ref):
    kept = kept_rows(trunc_ref, 2 * RAD, PD)

    def per_frequency(k, carry):
        rows = xt_ref[pl.ds(k, 2 * RAD, stride=ANG), :]
        masked = jnp.where(kept > k, rows, 0.0)
        turned = jnp.concatenate([masked[RAD:], -masked[:RAD]], axis=0)
        right = jnp.concatenate([masked, turned], axis=1).astype(BF16)
        s_ref[k] = lax.dot_general(
            rows.astype(BF16), right, TN, preferred_element_type=F32
        )
        return carry

    lax.fori_loop(0, ANG, per_frequency, 0, unroll=4)

    def per_rows(b, carry):
        sub = pl.ds(b * 8, 8)
        last_re = s_ref[0, sub, :PD]
        energy = last_re * last_re
        re = s_ref[1, sub, :PD]
        im = s_ref[1, sub, PD:]
        half = re * re + im * im
        first_re = last_re * re
        first_im = last_re * im
        m_re = jnp.zeros_like(re)
        m_im = jnp.zeros_like(re)
        for k in range(2, ANG):
            next_re = s_ref[k, sub, :PD]
            next_im = s_ref[k, sub, PD:]
            half = half + (next_re * next_re + next_im * next_im)
            m_re = m_re + (re * next_re + im * next_im)
            m_im = m_im + (im * next_re - re * next_im)
            re, im = next_re, next_im
        e_ref[sub, :] = energy + 0.5 * half
        re_ref[sub, :] = first_re + 0.5 * m_re
        im_ref[sub, :] = 0.5 * m_im - first_im
        return carry

    lax.fori_loop(0, PD // 8, per_rows, 0)


def far_kernel(
    size, trunc_ref, names_ref, pack_ref, recv_ref, table_ref, cur_ref,
    mine_ref, other_ref, cross_ref,
):
    r = pl.program_id(0)
    kept = size - HEAD

    @pl.when(r == 0)
    def _():
        for p in range(WIDE):
            mine_ref[p, kept:, :] = jnp.zeros((ANG, PD), F32)
        other_ref[kept:, :] = jnp.zeros((ANG, PD), F32)
        cross_ref[kept:, :] = jnp.zeros((ANG, PD), F32)

    first = iota((PD, PD), 1) < CAP
    sides = []
    for p in range(WIDE):
        name = names_ref[pl.ds(WIDE * r + p, 1), :].astype(jnp.int32)
        named = iota((PD, PD), 0) + 1 == name
        low = one_hot(named & first)
        high = one_hot(named & jnp.logical_not(first))
        sides.append(jnp.concatenate([low, high], axis=0))
    mine = jnp.dot(
        pack_ref[HEAD:size, :], jnp.concatenate(sides, axis=1), preferred_element_type=F32
    )
    for p in range(WIDE):
        mine_ref[p, :kept, :] = mine[:, p * PD : (p + 1) * PD]
    freq = iota((ANG, PD), 0)
    halves = []
    for p in range(WIDE):
        arrived = recv_ref[p, HEAD:, :].astype(F32)
        other_ref[:kept, :] = arrived
        cross_ref[:kept, :] = pltpu.roll(arrived, CAP, 1)
        sum_re = jnp.zeros((ANG, PD), F32)
        sum_im = jnp.zeros((ANG, PD), F32)
        offset = 0
        for q in range(RAD):
            here = pl.ds(offset, ANG)
            own = jnp.where(freq < trunc_ref[q], mine_ref[p, here, :], 0.0)
            sum_re = sum_re + own * other_ref[here, :]
            sum_im = sum_im + own * cross_ref[here, :]
            offset = offset + trunc_ref[q]
        halves.append((sum_re, sum_im))
        parts = recv_ref[p, :HEAD, :].astype(F32)
        cur_ref[p] = parts[:VEC] + parts[VEC:]
    first = first[:ANG]
    inner = (freq > 0) & (freq < ANG - 1)
    for b in range(WIDE // 2):
        even, odd = halves[2 * b], halves[2 * b + 1]
        s_re = jnp.where(first, even[0], odd[0])
        s_re = s_re + pltpu.roll(jnp.where(first, odd[0], even[0]), CAP, 1)
        s_im = pltpu.roll(jnp.where(first, odd[1], even[1]), CAP, 1)
        s_im = jnp.where(first, s_im - even[1], odd[1] - s_im)
        power = s_re * s_re + s_im * s_im
        next_re = pltpu.roll(s_re, ANG - 1, 0)
        next_im = pltpu.roll(s_im, ANG - 1, 0)
        zero_re = s_re[:1]
        energy = zero_re * zero_re + 0.5 * jnp.sum(
            jnp.where(freq == 0, 0.0, power), axis=0, keepdims=True
        )
        m_re = zero_re * s_re[1:2] + 0.5 * jnp.sum(
            jnp.where(inner, s_re * next_re + s_im * next_im, 0.0), axis=0, keepdims=True
        )
        m_im = 0.5 * jnp.sum(
            jnp.where(inner, s_im * next_re - s_re * next_im, 0.0), axis=0, keepdims=True
        ) - zero_re * s_im[1:2]
        table_ref[b] = jnp.concatenate(
            [energy, m_re, m_im, jnp.zeros((5, PD), F32)], axis=0
        )


def near_image(cur, w_re, w_im):
    weights = jnp.concatenate([w_re, w_im], axis=1)
    both = jnp.dot(cur, weights, precision=HIGHEST, preferred_element_type=F32)
    re = both[:VEC, :PD] - both[VEC:, PD:]
    im = both[VEC:, :PD] + both[:VEC, PD:]
    return jnp.concatenate([re, im], axis=0)


def far_image(slots, table_ref, lists_ref):
    values = []
    picks = []
    for r in range(PAIRS):
        m_re = table_ref[r, 1:2, :]
        m_im = table_ref[r, 2:3, :]
        c_re, c_im = slots[r][:VEC], slots[r][VEC:]
        values.append(
            jnp.concatenate([m_re * c_re - m_im * c_im, m_re * c_im + m_im * c_re], axis=0)
        )
        particle = lists_ref[r : r + 1, :].astype(jnp.int32)
        picks.append(one_hot(iota((PD, PD), 0) + 1 == particle))
    return exact_select(
        jnp.concatenate(values, axis=1), jnp.concatenate(picks, axis=1), NT
    )


def send_columns(cur, rx_ref, out_ref):
    picks = [one_hot(iota((PD, PD), 0) == wanted_row(rx_ref, r)) for r in range(PAIRS)]
    columns = exact_select(cur, jnp.concatenate(picks, axis=1))
    first = iota((VEC, PD), 1) < CAP
    for r in range(PAIRS):
        re = columns[:VEC, r * PD : (r + 1) * PD]
        im = columns[VEC:, r * PD : (r + 1) * PD]
        out_ref[2 * r] = jnp.where(first, re, pltpu.roll(im, CAP, 1))
        out_ref[2 * r + 1] = jnp.where(first, pltpu.roll(re, CAP, 1), im)


def received_columns(recv_ref):
    first = iota((VEC, PD), 1) < CAP
    slots = []
    for r in range(PAIRS):
        even = recv_ref[2 * r]
        odd = recv_ref[2 * r + 1]
        re = jnp.where(first, even, pltpu.roll(odd, CAP, 1))
        im = jnp.where(first, pltpu.roll(even, CAP, 1), odd)
        slots.append(jnp.concatenate([re, im], axis=0))
    return slots


def first_kernel(
    where_ref, nb_ref, code_ref, lists_ref, table_ref, e_ref, re_ref, im_ref,
    slots_ref, init_ref, rx_ref,
    align_ref, weights_ref, degree_ref, cur_ref, send_ref, near_ref,
):
    local = nb_ref[...] - where_ref[0]
    near = (local >> 7) == where_ref[1]
    near_ref[...] = jnp.where(near, local & (PD - 1), -1)
    rows = iota((PD, PD), 0)
    counts = jnp.zeros((PD, PD), F32)
    energy = []
    m_re = []
    m_im = []
    for n in range(NB):
        mine = rows == near_ref[n : n + 1, :]
        counts = counts + jnp.where(mine, 1.0, 0.0)
        energy.append(jnp.sum(jnp.where(mine, e_ref[...], 0.0), axis=0, keepdims=True))
        m_re.append(jnp.sum(jnp.where(mine, re_ref[...], 0.0), axis=0, keepdims=True))
        m_im.append(jnp.sum(jnp.where(mine, im_ref[...], 0.0), axis=0, keepdims=True))
    pad = [jnp.zeros((NBP - NB, PD), F32)]
    values = [jnp.concatenate(v + pad, axis=0) for v in (energy, m_re, m_im)]
    code = code_ref[...]
    pair = code >> 7
    lane = code & (PD - 1)
    for r in range(PAIRS):
        mine = pair == r
        for v in range(3):
            row = jnp.broadcast_to(table_ref[r, v : v + 1, :], (NBP, PD))
            found = jnp.take_along_axis(row, lane, axis=1, mode="promise_in_bounds")
            values[v] = jnp.where(mine, found, values[v])
    below = values[0] + EPS
    align_ref[0] = (values[1] / below)[:NB]
    align_ref[1] = (values[2] / below)[:NB]
    degree = EPS + jnp.sum(values[0], axis=0, keepdims=True)
    degree_ref[...] = jnp.broadcast_to(degree, (8, PD))
    w_re = counts * re_ref[...]
    w_im = counts * im_ref[...]
    weights_ref[0] = w_re
    weights_ref[1] = w_im
    slots = received_columns(slots_ref)
    image = near_image(init_ref[...], w_re, w_im) + far_image(slots, table_ref, lists_ref)
    image = image / degree
    cur_ref[...] = image
    send_columns(image, rx_ref, send_ref)


def next_image(recv_ref, cur_ref, weights_ref, degree_ref, table_ref, lists_ref):
    slots = received_columns(recv_ref)
    image = near_image(cur_ref[...], weights_ref[0], weights_ref[1])
    image = image + far_image(slots, table_ref, lists_ref)
    return image / degree_ref[:1, :]


def middle_kernel(
    recv_ref, cur_ref, weights_ref, degree_ref, table_ref, lists_ref, rx_ref,
    out_ref, send_ref,
):
    image = next_image(recv_ref, cur_ref, weights_ref, degree_ref, table_ref, lists_ref)
    out_ref[...] = image
    send_columns(image, rx_ref, send_ref)


def last_kernel(
    total, recv_ref, cur_ref, weights_ref, degree_ref, table_ref, lists_ref,
    out_ref, gram_ref,
):
    image = next_image(recv_ref, cur_ref, weights_ref, degree_ref, table_ref, lists_ref)
    out_ref[...] = image
    gram = lax.dot_general(
        image[:VEC], image[:VEC], NT, precision=HIGHEST, preferred_element_type=F32
    ) + lax.dot_general(
        image[VEC:], image[VEC:], NT, precision=HIGHEST, preferred_element_type=F32
    )
    gram = gram * (1.0 / total)
    wide = jnp.concatenate([gram] * 8, axis=1)
    mine = iota((VEC, PD), 1) // VEC == iota((VEC, PD), 0) % 8
    wide = jnp.where(mine, wide, 0.0)
    packed = jnp.concatenate(
        [
            jnp.sum(wide[:8], axis=0, keepdims=True),
            jnp.sum(wide[8:], axis=0, keepdims=True),
        ],
        axis=0,
    )
    gram_ref[...] = jnp.broadcast_to(packed[None], gram_ref.shape)


def finish_kernel(grams_ref, cur_ref, out_ref):
    packed = jnp.sum(grams_ref[...], axis=0)
    row = iota((VEC, PD), 0)
    lane = iota((VEC, PD), 1)
    wide = jnp.where(row < 8, packed[0:1, :], packed[1:2, :])
    wide = jnp.where(lane // VEC == row % 8, wide, 0.0)
    for shift in (64, 32, 16):
        wide = wide + pltpu.roll(wide, shift, 1)
    gram = wide
    re = cur_ref[:VEC, :]
    im = cur_ref[VEC:, :]
    for c in range(VEC):
        pivot = gram[c : c + 1, c : c + 1]
        scale = lax.rsqrt(pivot)
        scale = scale * (1.5 - 0.5 * pivot * scale * scale)
        column = gram[:, c : c + 1] * scale
        column = jnp.where(row[:, :1] > c, column, 0.0)
        top_gram = gram[c : c + 1, :] * scale
        top_re = re[c : c + 1, :] * scale
        top_im = im[c : c + 1, :] * scale
        here = row == c
        gram = gram - column * top_gram
        re = jnp.where(here, top_re, re - column * top_re)
        im = jnp.where(here, top_im, im - column * top_im)
    out_ref[:VEC, :] = re
    out_ref[VEC:, :] = im


def struct(shape, dtype=F32):
    return jax.ShapeDtypeStruct(shape, dtype)


SMEM = pl.BlockSpec(memory_space=pltpu.SMEM)
VMEM = pl.BlockSpec(memory_space=pltpu.VMEM)


def whole(*shape):
    return pl.BlockSpec(shape, lambda r: (0,) * len(shape))


def exchange(size, truncation, names, asked, packed):
    steps = PEERS // WIDE
    sent = pl.pallas_call(
        functools.partial(pick_kernel, size),
        grid=(steps,),
        out_shape=struct((PEERS, size, PD), BF16),
        in_specs=[whole(PEERS, 8, PD), whole(HEAD + FULL, 2 * PD)],
        out_specs=pl.BlockSpec((WIDE, size, PD), lambda r: (r, 0, 0)),
        name="pick",
    )(asked, packed)
    received = lax.all_to_all(sent, REP, 0, 0, tiled=True)
    return pl.pallas_call(
        functools.partial(far_kernel, size),
        grid=(steps,),
        out_shape=(struct((PAIRS, 8, PD)), struct((PEERS, VEC, PD))),
        in_specs=[
            SMEM,
            whole(PEERS, PD),
            whole(HEAD + FULL, 2 * PD),
            pl.BlockSpec((WIDE, size, PD), lambda r: (r, 0, 0)),
        ],
        out_specs=(
            pl.BlockSpec((WIDE // 2, 8, PD), lambda r: (r, 0, 0)),
            pl.BlockSpec((WIDE, VEC, PD), lambda r: (r, 0, 0)),
        ),
        scratch_shapes=[
            pltpu.VMEM((WIDE, size - HEAD + ANG, PD), F32),
            pltpu.VMEM((size - HEAD + ANG, PD), F32),
            pltpu.VMEM((size - HEAD + ANG, PD), F32),
        ],
        name="far",
    )(truncation, names, packed, received)


def shards(coefficients, truncation, neighbours, initial):
    groups = lax.axis_size(GRP)
    replicas = lax.axis_size(REP)
    devices = groups * replicas
    place = jnp.stack(
        [lax.axis_index(GRP) * (replicas * PD), lax.axis_index(REP)]
    ).astype(jnp.int32)
    code, lists, names, requests = pl.pallas_call(
        slot_kernel,
        out_shape=(
            struct((NBP, PD), jnp.int32),
            struct((PAIRS, PD)),
            struct((PEERS, PD)),
            struct((PEERS, 8, PD)),
        ),
        in_specs=[SMEM, VMEM],
        scratch_shapes=[
            pltpu.VMEM((NBP, PD), jnp.int32),
            pltpu.VMEM((2 * PAIRS, NB * PD), BF16),
            pltpu.VMEM((PD, NB * PD), BF16),
        ],
        name="slots",
    )(place, neighbours)
    asked = lax.all_to_all(requests, REP, 0, 0, tiled=True)
    packed, e_own, re_own, im_own = pl.pallas_call(
        local_kernel,
        out_shape=(struct((HEAD + FULL, 2 * PD), BF16),) + (struct((PD, PD)),) * 3,
        in_specs=[SMEM, VMEM, VMEM],
        scratch_shapes=[
            pltpu.VMEM((CW, PD), F32),
            pltpu.VMEM((FULL + ANG, PD), F32),
            pltpu.VMEM((FULL + ANG, PD), F32),
            pltpu.VMEM((ANG, PD, 2 * PD), F32),
        ],
        cost_estimate=pl.CostEstimate(
            flops=20_000_000_000, bytes_accessed=1_000_000, transcendentals=0
        ),
        name="local",
    )(truncation, coefficients, initial)
    total = jnp.sum(truncation)
    which = jnp.sum(total > jnp.array(SIZES[:-1], jnp.int32)).astype(jnp.int32)
    table, slots = lax.switch(
        which,
        [functools.partial(exchange, HEAD + size) for size in SIZES],
        truncation, names, asked, packed,
    )
    alignment, weights, degree, current, columns = pl.pallas_call(
        first_kernel,
        out_shape=(
            struct((2, NB, PD)),
            struct((2, PD, PD)),
            struct((8, PD)),
            struct((32, PD)),
            struct((PEERS, VEC, PD)),
        ),
        in_specs=[SMEM] + [VMEM] * 10,
        scratch_shapes=[pltpu.VMEM((NB, PD), jnp.int32)],
        name="first",
    )(
        place, neighbours, code, lists, table, e_own, re_own, im_own,
        slots, initial, asked,
    )
    columns = lax.all_to_all(columns, REP, 0, 0, tiled=True)
    current, columns = pl.pallas_call(
        middle_kernel,
        out_shape=(struct((32, PD)), struct((PEERS, VEC, PD))),
        name="middle",
    )(columns, current, weights, degree, table, lists, asked)
    columns = lax.all_to_all(columns, REP, 0, 0, tiled=True)
    current, gram = pl.pallas_call(
        functools.partial(last_kernel, float(PD * devices)),
        out_shape=(struct((32, PD)), struct((devices, 2, PD))),
        name="last",
    )(columns, current, weights, degree, table, lists)
    grams = lax.all_to_all(gram, GRP_REP, 0, 0, tiled=True)
    vectors = pl.pallas_call(
        finish_kernel, out_shape=struct((32, PD)), name="finish"
    )(grams, current)
    return (alignment, vectors)


def solution(mesh):
    split = Mesh(mesh.devices.reshape(4, 2, 4, 4), GRP_REP)
    in_specs = (P(GRP_REP, None), P(), P(None, GRP_REP), P(None, GRP_REP))
    out_specs = (P(None, None, GRP_REP), P(None, GRP_REP))
    return jax.shard_map(
        shards, mesh=split, in_specs=in_specs, out_specs=out_specs, check_vma=False
    )
```

```python
import functools

import jax
import jax.numpy as jnp
from jax import lax
from jax.experimental import pallas as pl
from jax.experimental.pallas import tpu as pltpu
from jax.sharding import Mesh
from jax.sharding import PartitionSpec as P

ANG = 64
RAD = 16
NB = 50
NBP = 56
VEC = 16
PD = 128
CAP = 64
CW = 2048
FULL = RAD * ANG
SIZES = (384, 512, 576, 640, 704, 768, 896, FULL)
HEAD = 2 * VEC
PEERS = 16
PAIRS = PEERS // 2
WIDE = 4
GRP = ("grp_0", "grp_1")
REP = ("rep_0", "rep_1")
GRP_REP = ("grp_0", "grp_1", "rep_0", "rep_1")
EPS = 1e-06
F32 = jnp.float32
BF16 = jnp.bfloat16
HIGHEST = lax.Precision.HIGHEST

NT = (((1,), (1,)), ((), ()))
TN = (((0,), (0,)), ((), ()))


def iota(shape, dim):
    return lax.broadcasted_iota(jnp.int32, shape, dim)


def one_hot(cond):
    return jnp.where(cond, 1.0, 0.0).astype(BF16)


def three_parts(x):
    high = x.astype(BF16)
    rest = x - high.astype(F32)
    mid = rest.astype(BF16)
    low = (rest - mid.astype(F32)).astype(BF16)
    return jnp.concatenate([high, mid, low], axis=0)


def two_parts(x):
    high = x.astype(BF16)
    rest = (x - high.astype(F32)).astype(BF16)
    return jnp.concatenate([high, rest], axis=0)


def exact_select(x, selector, dims=(((1,), (0,)), ((), ()))):
    rows = x.shape[0]
    parts = lax.dot_general(three_parts(x), selector, dims, preferred_element_type=F32)
    return parts[:rows] + (parts[rows : 2 * rows] + parts[2 * rows :])


def kept_rows(trunc_ref, rows, lanes):
    row = iota((rows, lanes), 0) % RAD
    kept = jnp.zeros((rows, lanes), jnp.int32)
    for q in range(RAD):
        kept = jnp.where(row == q, trunc_ref[q], kept)
    return kept


def place():
    index = [lax.axis_index(name) for name in GRP_REP]
    size = [lax.axis_size(name) for name in GRP_REP]
    group = index[0] * size[1] + index[1]
    member = index[2] * size[3] + index[3]
    return group * (size[2] * size[3] * PD), member


def slot_kernel(
    trunc_ref, nb_ref, which_ref, code_ref, lists_ref, names_ref, req_ref,
    nbp_ref, a_ref, b_ref,
):
    total = trunc_ref[0]
    for q in range(1, RAD):
        total = total + trunc_ref[q]
    which = jnp.int32(0)
    for size in SIZES[:-1]:
        which = which + (total > size).astype(jnp.int32)
    which_ref[0] = which
    start, me = place()
    nbp_ref[...] = jnp.full((NBP, PD), -1, jnp.int32)
    nbp_ref[:NB, :] = nb_ref[...] - start
    local = nbp_ref[...]
    owner = local >> 7
    within = local & (PD - 1)
    remote = (owner != me) & (local >= 0)
    owner = jnp.where(remote, owner, -1)
    masks = [one_hot(owner == p) for p in range(PEERS)]
    before = one_hot(iota((NBP, NBP), 0) > iota((NBP, NBP), 1))
    in_column = jnp.dot(before, jnp.concatenate(masks, axis=1), preferred_element_type=F32)
    totals = jnp.concatenate(
        [jnp.sum(m.astype(F32), axis=0, keepdims=True) for m in masks], axis=0
    )
    left = one_hot(iota((PD, PD), 0) < iota((PD, PD), 1))
    columns = jnp.dot(totals.astype(BF16), left, preferred_element_type=F32)
    rank = jnp.zeros((NBP, PD), F32)
    for p in range(PEERS):
        here = in_column[:, p * PD : (p + 1) * PD] + columns[p : p + 1, :]
        rank = jnp.where(owner == p, here, rank)
    rank = rank.astype(jnp.int32)
    code = jnp.where(remote, owner * CAP + rank, -1)
    code_ref[...] = code
    pair = code >> 7
    lane = jnp.where(remote, code & (PD - 1), -1)
    particle = iota((1, PD), 1).astype(F32) + 1.0
    rows8 = iota((PAIRS, PD), 0)
    rows128 = iota((PD, PD), 0)
    for n in range(NB):
        mine = rows8 == pair[n : n + 1, :]
        names = within[n : n + 1, :].astype(F32)
        both = jnp.concatenate(
            [jnp.where(mine, names, 0.0), jnp.where(mine, particle, 0.0)], axis=0
        )
        a_ref[:, n * PD : (n + 1) * PD] = both.astype(BF16)
        b_ref[:, n * PD : (n + 1) * PD] = one_hot(rows128 == lane[n : n + 1, :])
    lists = lax.dot_general(a_ref[...], b_ref[...], NT, preferred_element_type=F32)
    lists_ref[...] = lists[PAIRS:]
    turned = pltpu.roll(lists, CAP, 1)
    first = iota((2 * PAIRS, PD), 1) < CAP
    both = (jnp.where(first, lists, turned), jnp.where(first, turned, lists))
    for p in range(PEERS):
        rows = both[p % 2]
        r = p // 2
        req_ref[p] = jnp.broadcast_to(rows[r : r + 1, :], (8, PD))
        names_ref[p : p + 1, :] = rows[PAIRS + r : PAIRS + r + 1, :]


def wanted_row(rx_ref, r):
    even = rx_ref[2 * r][:1, :]
    odd = rx_ref[2 * r + 1][:1, :]
    return jnp.where(iota((1, PD), 1) < CAP, even, odd).astype(jnp.int32)


def local_kernel(
    trunc_ref, coef_ref, init_ref, out_ref, e_ref, re_ref, im_ref,
    f_ref, wide_re_ref, wide_im_ref, s_ref,
):
    init = init_ref[...]
    parts = two_parts(jnp.concatenate([init[:VEC], init[VEC:]], axis=1))
    out_ref[:HEAD, :] = parts
    for c in range(CW // PD):
        block = coef_ref[:, c * PD : (c + 1) * PD].astype(F32)
        f_ref[c * PD : (c + 1) * PD, :] = block.T
    offset = 0
    for q in range(RAD):
        here = pl.ds(offset, ANG)
        wide_re_ref[here, :] = f_ref[q * ANG : (q + 1) * ANG, :]
        wide_im_ref[here, :] = f_ref[(RAD + q) * ANG : (RAD + q + 1) * ANG, :]
        offset = offset + trunc_ref[q]
    for b in range(FULL // PD):
        rows = slice(b * PD, (b + 1) * PD)
        to = slice(HEAD + b * PD, HEAD + (b + 1) * PD)
        kept = iota((PD, PD), 0) + b * PD < offset
        out_ref[to, :PD] = jnp.where(kept, wide_re_ref[rows, :], 0.0).astype(BF16)
        out_ref[to, PD:] = jnp.where(kept, wide_im_ref[rows, :], 0.0).astype(BF16)
    own_pairs(trunc_ref, e_ref, re_ref, im_ref, f_ref, s_ref)


def pick_kernel(size, rx_ref, pack_ref, out_ref):
    r = pl.program_id(0)
    rows = iota((PD, PD), 0)
    first = iota((PD, PD), 1) < CAP
    sides = []
    for p in range(WIDE):
        picked = rows == rx_ref[WIDE * r + p][:1, :].astype(jnp.int32)
        top = one_hot(picked & first)
        bottom = one_hot(picked & jnp.logical_not(first))
        sides.append(jnp.concatenate([top, bottom], axis=0))
    side = jnp.concatenate(sides, axis=1)
    chosen = jnp.dot(pack_ref[:size, :], side, preferred_element_type=F32).astype(BF16)
    for p in range(WIDE):
        out_ref[p] = chosen[:, p * PD : (p + 1) * PD]


def own_pairs(trunc_ref, e_ref, re_ref, im_ref, xt_ref, s_ref):
    kept = kept_rows(trunc_ref, 2 * RAD, PD)

    def per_frequency(k, carry):
        rows = xt_ref[pl.ds(k, 2 * RAD, stride=ANG), :]
        masked = jnp.where(kept > k, rows, 0.0)
        turned = jnp.concatenate([masked[RAD:], -masked[:RAD]], axis=0)
        right = jnp.concatenate([masked, turned], axis=1).astype(BF16)
        s_ref[k] = lax.dot_general(
            rows.astype(BF16), right, TN, preferred_element_type=F32
        )
        return carry

    lax.fori_loop(0, ANG, per_frequency, 0, unroll=8)

    def per_rows(b, carry):
        sub = pl.ds(b * 8, 8)
        last_re = s_ref[0, sub, :PD]
        energy = last_re * last_re
        re = s_ref[1, sub, :PD]
        im = s_ref[1, sub, PD:]
        half = re * re + im * im
        first_re = last_re * re
        first_im = last_re * im
        m_re = jnp.zeros_like(re)
        m_im = jnp.zeros_like(re)
        for k in range(2, ANG):
            next_re = s_ref[k, sub, :PD]
            next_im = s_ref[k, sub, PD:]
            half = half + (next_re * next_re + next_im * next_im)
            m_re = m_re + (re * next_re + im * next_im)
            m_im = m_im + (im * next_re - re * next_im)
            re, im = next_re, next_im
        e_ref[sub, :] = energy + 0.5 * half
        re_ref[sub, :] = first_re + 0.5 * m_re
        im_ref[sub, :] = 0.5 * m_im - first_im
        return carry

    lax.fori_loop(0, PD // 8, per_rows, 0)


def far_kernel(
    size, trunc_ref, names_ref, pack_ref, recv_ref, table_ref, cur_ref,
    same_ref, cross_ref,
):
    r = pl.program_id(0)
    kept = size - HEAD

    @pl.when(r == 0)
    def _():
        for p in range(WIDE):
            same_ref[p, kept:, :] = jnp.zeros((ANG, PD), F32)
            cross_ref[p, kept:, :] = jnp.zeros((ANG, PD), F32)

    first = iota((PD, PD), 1) < CAP
    sides = []
    for p in range(WIDE):
        name = names_ref[pl.ds(WIDE * r + p, 1), :].astype(jnp.int32)
        named = iota((PD, PD), 0) + 1 == name
        low = one_hot(named & first)
        high = one_hot(named & jnp.logical_not(first))
        sides.append(jnp.concatenate([low, high], axis=0))
    mine = jnp.dot(
        pack_ref[HEAD:size, :], jnp.concatenate(sides, axis=1), preferred_element_type=F32
    )
    freq = iota((ANG, PD), 0)
    halves = []
    for p in range(WIDE):
        arrived = recv_ref[p, HEAD:, :].astype(F32)
        own = mine[:, p * PD : (p + 1) * PD]
        same_ref[p, :kept, :] = own * arrived
        cross_ref[p, :kept, :] = own * pltpu.roll(arrived, CAP, 1)
        parts = recv_ref[p, :HEAD, :].astype(F32)
        cur_ref[p] = parts[:VEC] + parts[VEC:]
    for p in range(WIDE):
        sum_re = jnp.zeros((ANG, PD), F32)
        sum_im = jnp.zeros((ANG, PD), F32)
        offset = 0
        for q in range(RAD):
            here = pl.ds(offset, ANG)
            inside = freq < trunc_ref[q]
            sum_re = sum_re + jnp.where(inside, same_ref[p, here, :], 0.0)
            sum_im = sum_im + jnp.where(inside, cross_ref[p, here, :], 0.0)
            offset = offset + trunc_ref[q]
        halves.append((sum_re, sum_im))
    first = first[:ANG]
    inner = (freq > 0) & (freq < ANG - 1)
    for b in range(WIDE // 2):
        even, odd = halves[2 * b], halves[2 * b + 1]
        s_re = jnp.where(first, even[0], odd[0])
        s_re = s_re + pltpu.roll(jnp.where(first, odd[0], even[0]), CAP, 1)
        s_im = pltpu.roll(jnp.where(first, odd[1], even[1]), CAP, 1)
        s_im = jnp.where(first, s_im - even[1], odd[1] - s_im)
        power = s_re * s_re + s_im * s_im
        next_re = pltpu.roll(s_re, ANG - 1, 0)
        next_im = pltpu.roll(s_im, ANG - 1, 0)
        zero_re = s_re[:1]
        energy = zero_re * zero_re + 0.5 * jnp.sum(
            jnp.where(freq == 0, 0.0, power), axis=0, keepdims=True
        )
        m_re = zero_re * s_re[1:2] + 0.5 * jnp.sum(
            jnp.where(inner, s_re * next_re + s_im * next_im, 0.0), axis=0, keepdims=True
        )
        m_im = 0.5 * jnp.sum(
            jnp.where(inner, s_im * next_re - s_re * next_im, 0.0), axis=0, keepdims=True
        ) - zero_re * s_im[1:2]
        table_ref[b] = jnp.concatenate(
            [energy, m_re, m_im, jnp.zeros((5, PD), F32)], axis=0
        )


def near_image(cur, w_re, w_im):
    weights = jnp.concatenate([w_re, w_im], axis=1)
    both = jnp.dot(cur, weights, precision=HIGHEST, preferred_element_type=F32)
    re = both[:VEC, :PD] - both[VEC:, PD:]
    im = both[VEC:, :PD] + both[:VEC, PD:]
    return jnp.concatenate([re, im], axis=0)


def far_image(slots, table_ref, lists_ref):
    values = []
    picks = []
    for r in range(PAIRS):
        m_re = table_ref[r, 1:2, :]
        m_im = table_ref[r, 2:3, :]
        c_re, c_im = slots[r][:VEC], slots[r][VEC:]
        values.append(
            jnp.concatenate([m_re * c_re - m_im * c_im, m_re * c_im + m_im * c_re], axis=0)
        )
        particle = lists_ref[r : r + 1, :].astype(jnp.int32)
        picks.append(one_hot(iota((PD, PD), 0) + 1 == particle))
    return exact_select(
        jnp.concatenate(values, axis=1), jnp.concatenate(picks, axis=1), NT
    )


def send_columns(cur, rx_ref, out_ref):
    picks = [one_hot(iota((PD, PD), 0) == wanted_row(rx_ref, r)) for r in range(PAIRS)]
    columns = exact_select(cur, jnp.concatenate(picks, axis=1))
    first = iota((VEC, PD), 1) < CAP
    for r in range(PAIRS):
        re = columns[:VEC, r * PD : (r + 1) * PD]
        im = columns[VEC:, r * PD : (r + 1) * PD]
        out_ref[2 * r] = jnp.where(first, re, pltpu.roll(im, CAP, 1))
        out_ref[2 * r + 1] = jnp.where(first, pltpu.roll(re, CAP, 1), im)


def received_columns(recv_ref):
    first = iota((VEC, PD), 1) < CAP
    slots = []
    for r in range(PAIRS):
        even = recv_ref[2 * r]
        odd = recv_ref[2 * r + 1]
        re = jnp.where(first, even, pltpu.roll(odd, CAP, 1))
        im = jnp.where(first, pltpu.roll(even, CAP, 1), odd)
        slots.append(jnp.concatenate([re, im], axis=0))
    return slots


def first_kernel(
    nb_ref, code_ref, lists_ref, table_ref, e_ref, re_ref, im_ref,
    slots_ref, init_ref, rx_ref,
    align_ref, weights_ref, degree_ref, cur_ref, send_ref, near_ref,
):
    start, me = place()
    local = nb_ref[...] - start
    near = (local >> 7) == me
    near_ref[...] = jnp.where(near, local & (PD - 1), -1)
    rows = iota((PD, PD), 0)
    counts = jnp.zeros((PD, PD), F32)
    energy = []
    m_re = []
    m_im = []
    for n in range(NB):
        mine = rows == near_ref[n : n + 1, :]
        counts = counts + jnp.where(mine, 1.0, 0.0)
        energy.append(jnp.sum(jnp.where(mine, e_ref[...], 0.0), axis=0, keepdims=True))
        m_re.append(jnp.sum(jnp.where(mine, re_ref[...], 0.0), axis=0, keepdims=True))
        m_im.append(jnp.sum(jnp.where(mine, im_ref[...], 0.0), axis=0, keepdims=True))
    pad = [jnp.zeros((NBP - NB, PD), F32)]
    values = [jnp.concatenate(v + pad, axis=0) for v in (energy, m_re, m_im)]
    code = code_ref[...]
    pair = code >> 7
    lane = code & (PD - 1)
    for r in range(PAIRS):
        mine = pair == r
        for v in range(3):
            row = jnp.broadcast_to(table_ref[r, v : v + 1, :], (NBP, PD))
            found = jnp.take_along_axis(row, lane, axis=1, mode="promise_in_bounds")
            values[v] = jnp.where(mine, found, values[v])
    below = values[0] + EPS
    align_ref[0] = (values[1] / below)[:NB]
    align_ref[1] = (values[2] / below)[:NB]
    degree = EPS + jnp.sum(values[0], axis=0, keepdims=True)
    degree_ref[...] = jnp.broadcast_to(degree, (8, PD))
    w_re = counts * re_ref[...]
    w_im = counts * im_ref[...]
    weights_ref[0] = w_re
    weights_ref[1] = w_im
    slots = received_columns(slots_ref)
    image = near_image(init_ref[...], w_re, w_im) + far_image(slots, table_ref, lists_ref)
    image = image / degree
    cur_ref[...] = image
    send_columns(image, rx_ref, send_ref)


def next_image(recv_ref, cur_ref, weights_ref, degree_ref, table_ref, lists_ref):
    slots = received_columns(recv_ref)
    image = near_image(cur_ref[...], weights_ref[0], weights_ref[1])
    image = image + far_image(slots, table_ref, lists_ref)
    return image / degree_ref[:1, :]


def middle_kernel(
    recv_ref, cur_ref, weights_ref, degree_ref, table_ref, lists_ref, rx_ref,
    out_ref, send_ref,
):
    image = next_image(recv_ref, cur_ref, weights_ref, degree_ref, table_ref, lists_ref)
    out_ref[...] = image
    send_columns(image, rx_ref, send_ref)


def last_kernel(
    total, recv_ref, cur_ref, weights_ref, degree_ref, table_ref, lists_ref,
    out_ref, gram_ref,
):
    image = next_image(recv_ref, cur_ref, weights_ref, degree_ref, table_ref, lists_ref)
    out_ref[...] = image
    gram = lax.dot_general(
        image[:VEC], image[:VEC], NT, precision=HIGHEST, preferred_element_type=F32
    ) + lax.dot_general(
        image[VEC:], image[VEC:], NT, precision=HIGHEST, preferred_element_type=F32
    )
    gram = gram * (1.0 / total)
    wide = jnp.concatenate([gram] * 8, axis=1)
    mine = iota((VEC, PD), 1) // VEC == iota((VEC, PD), 0) % 8
    wide = jnp.where(mine, wide, 0.0)
    packed = jnp.concatenate(
        [
            jnp.sum(wide[:8], axis=0, keepdims=True),
            jnp.sum(wide[8:], axis=0, keepdims=True),
        ],
        axis=0,
    )
    gram_ref[...] = jnp.broadcast_to(packed[None], gram_ref.shape)


def finish_kernel(grams_ref, cur_ref, out_ref):
    packed = jnp.sum(grams_ref[...], axis=0)
    row = iota((VEC, PD), 0)
    lane = iota((VEC, PD), 1)
    wide = jnp.where(row < 8, packed[0:1, :], packed[1:2, :])
    wide = jnp.where(lane // VEC == row % 8, wide, 0.0)
    for shift in (64, 32, 16):
        wide = wide + pltpu.roll(wide, shift, 1)
    columns = [jnp.broadcast_to(wide[:, c : c + 1], (VEC, PD)) for c in range(VEC)]
    re = cur_ref[:VEC, :]
    im = cur_ref[VEC:, :]
    for c in range(VEC):
        pivot = columns[c][c : c + 1, :]
        scale = lax.rsqrt(pivot)
        scale = scale * (1.5 - 0.5 * pivot * scale * scale)
        column = jnp.where(row > c, columns[c] * scale, 0.0)
        for d in range(c + 1, VEC):
            columns[d] = columns[d] - column * (columns[d][c : c + 1, :] * scale)
        top_re = re[c : c + 1, :] * scale
        top_im = im[c : c + 1, :] * scale
        here = row == c
        re = jnp.where(here, top_re, re - column * top_re)
        im = jnp.where(here, top_im, im - column * top_im)
    out_ref[:VEC, :] = re
    out_ref[VEC:, :] = im


def struct(shape, dtype=F32):
    return jax.ShapeDtypeStruct(shape, dtype)


SMEM = pl.BlockSpec(memory_space=pltpu.SMEM)
VMEM = pl.BlockSpec(memory_space=pltpu.VMEM)


def grant(mib):
    return pltpu.CompilerParams(vmem_limit_bytes=mib << 20)


def whole(*shape):
    return pl.BlockSpec(shape, lambda r: (0,) * len(shape))


def exchange(size, truncation, names, asked, packed):
    steps = PEERS // WIDE
    sent = pl.pallas_call(
        functools.partial(pick_kernel, size),
        grid=(steps,),
        out_shape=struct((PEERS, size, PD), BF16),
        in_specs=[whole(PEERS, 8, PD), whole(HEAD + FULL, 2 * PD)],
        out_specs=pl.BlockSpec((WIDE, size, PD), lambda r: (r, 0, 0)),
        compiler_params=grant(16),
        name="pick",
    )(asked, packed)
    received = lax.all_to_all(sent, REP, 0, 0, tiled=True)
    return pl.pallas_call(
        functools.partial(far_kernel, size),
        grid=(steps,),
        out_shape=(struct((PAIRS, 8, PD)), struct((PEERS, VEC, PD))),
        in_specs=[
            SMEM,
            whole(PEERS, PD),
            whole(HEAD + FULL, 2 * PD),
            pl.BlockSpec((WIDE, size, PD), lambda r: (r, 0, 0)),
        ],
        out_specs=(
            pl.BlockSpec((WIDE // 2, 8, PD), lambda r: (r, 0, 0)),
            pl.BlockSpec((WIDE, VEC, PD), lambda r: (r, 0, 0)),
        ),
        scratch_shapes=[
            pltpu.VMEM((WIDE, size - HEAD + ANG, PD), F32),
            pltpu.VMEM((WIDE, size - HEAD + ANG, PD), F32),
        ],
        compiler_params=grant(20),
        name="far",
    )(truncation, names, packed, received)


def shards(coefficients, truncation, neighbours, initial):
    groups = lax.axis_size(GRP)
    replicas = lax.axis_size(REP)
    devices = groups * replicas
    which, code, lists, names, requests = pl.pallas_call(
        slot_kernel,
        out_shape=(
            struct((1,), jnp.int32),
            struct((NBP, PD), jnp.int32),
            struct((PAIRS, PD)),
            struct((PEERS, PD)),
            struct((PEERS, 8, PD)),
        ),
        in_specs=[SMEM, VMEM],
        out_specs=(SMEM, VMEM, VMEM, VMEM, VMEM),
        compiler_params=grant(6),
        scratch_shapes=[
            pltpu.VMEM((NBP, PD), jnp.int32),
            pltpu.VMEM((2 * PAIRS, NB * PD), BF16),
            pltpu.VMEM((PD, NB * PD), BF16),
        ],
        name="slots",
    )(truncation, neighbours)
    asked = lax.all_to_all(requests, REP, 0, 0, tiled=True)
    packed, e_own, re_own, im_own = pl.pallas_call(
        local_kernel,
        out_shape=(struct((HEAD + FULL, 2 * PD), BF16),) + (struct((PD, PD)),) * 3,
        in_specs=[SMEM, VMEM, VMEM],
        scratch_shapes=[
            pltpu.VMEM((CW, PD), F32),
            pltpu.VMEM((FULL + ANG, PD), F32),
            pltpu.VMEM((FULL + ANG, PD), F32),
            pltpu.VMEM((ANG, PD, 2 * PD), F32),
        ],
        cost_estimate=pl.CostEstimate(
            flops=20_000_000_000, bytes_accessed=1_000_000, transcendentals=0
        ),
        compiler_params=grant(20),
        name="local",
    )(truncation, coefficients, initial)
    table, slots = lax.switch(
        which[0],
        [functools.partial(exchange, HEAD + size) for size in SIZES],
        truncation, names, asked, packed,
    )
    alignment, weights, degree, current, columns = pl.pallas_call(
        first_kernel,
        out_shape=(
            struct((2, NB, PD)),
            struct((2, PD, PD)),
            struct((8, PD)),
            struct((32, PD)),
            struct((PEERS, VEC, PD)),
        ),
        in_specs=[VMEM] * 10,
        compiler_params=grant(6),
        scratch_shapes=[pltpu.VMEM((NB, PD), jnp.int32)],
        name="first",
    )(
        neighbours, code, lists, table, e_own, re_own, im_own,
        slots, initial, asked,
    )
    columns = lax.all_to_all(columns, REP, 0, 0, tiled=True)
    current, columns = pl.pallas_call(
        middle_kernel,
        out_shape=(struct((32, PD)), struct((PEERS, VEC, PD))),
        compiler_params=grant(6),
        name="middle",
    )(columns, current, weights, degree, table, lists, asked)
    columns = lax.all_to_all(columns, REP, 0, 0, tiled=True)
    current, gram = pl.pallas_call(
        functools.partial(last_kernel, float(PD * devices)),
        out_shape=(struct((32, PD)), struct((devices, 2, PD))),
        compiler_params=grant(6),
        name="last",
    )(columns, current, weights, degree, table, lists)
    grams = lax.all_to_all(gram, GRP_REP, 0, 0, tiled=True)
    vectors = pl.pallas_call(
        finish_kernel,
        out_shape=struct((32, PD)),
        compiler_params=grant(6),
        name="finish",
    )(grams, current)
    return (alignment, vectors)


def solution(mesh):
    split = Mesh(mesh.devices.reshape(4, 2, 4, 4), GRP_REP)
    in_specs = (P(GRP_REP, None), P(), P(None, GRP_REP), P(None, GRP_REP))
    out_specs = (P(None, None, GRP_REP), P(None, GRP_REP))
    return jax.shard_map(
        shards, mesh=split, in_specs=in_specs, out_specs=out_specs, check_vma=False
    )
```

```python
import functools

import jax
import jax.numpy as jnp
from jax import lax
from jax.experimental import pallas as pl
from jax.experimental.pallas import tpu as pltpu
from jax.sharding import Mesh
from jax.sharding import PartitionSpec as P

ANG = 64
RAD = 16
NB = 50
NBP = 56
VEC = 16
PD = 128
CAP = 64
CW = 2048
FULL = RAD * ANG
SIZES = (384, 512, 544, 576, 608, 640, 672, 704, 736, 768, 896, FULL)
HEAD = 2 * VEC
PEERS = 16
PAIRS = PEERS // 2
WIDE = 4
GRP = ("grp_0", "grp_1")
REP = ("rep_0", "rep_1")
GRP_REP = ("grp_0", "grp_1", "rep_0", "rep_1")
EPS = 1e-06
F32 = jnp.float32
BF16 = jnp.bfloat16
HIGHEST = lax.Precision.HIGHEST

NT = (((1,), (1,)), ((), ()))
TN = (((0,), (0,)), ((), ()))


def iota(shape, dim):
    return lax.broadcasted_iota(jnp.int32, shape, dim)


def one_hot(cond):
    return jnp.where(cond, 1.0, 0.0).astype(BF16)


def three_parts(x):
    high = x.astype(BF16)
    rest = x - high.astype(F32)
    mid = rest.astype(BF16)
    low = (rest - mid.astype(F32)).astype(BF16)
    return jnp.concatenate([high, mid, low], axis=0)


def two_parts(x):
    high = x.astype(BF16)
    rest = (x - high.astype(F32)).astype(BF16)
    return jnp.concatenate([high, rest], axis=0)


def exact_select(x, selector, dims=(((1,), (0,)), ((), ()))):
    rows = x.shape[0]
    parts = lax.dot_general(three_parts(x), selector, dims, preferred_element_type=F32)
    return parts[:rows] + (parts[rows : 2 * rows] + parts[2 * rows :])


def kept_rows(trunc_ref, rows, lanes):
    row = iota((rows, lanes), 0) % RAD
    kept = jnp.zeros((rows, lanes), jnp.int32)
    for q in range(RAD):
        kept = jnp.where(row == q, trunc_ref[q], kept)
    return kept


def place():
    index = [lax.axis_index(name) for name in GRP_REP]
    size = [lax.axis_size(name) for name in GRP_REP]
    group = index[0] * size[1] + index[1]
    member = index[2] * size[3] + index[3]
    return group * (size[2] * size[3] * PD), member


def slot_kernel(
    trunc_ref, nb_hbm, coef_hbm, init_hbm,
    which_ref, code_ref, lists_ref, names_ref, req_ref, coef_ref, init_ref,
    nb_ref, nbp_ref, a_ref, b_ref, sem_ref,
):
    bring = (
        pltpu.make_async_copy(coef_hbm, coef_ref, sem_ref.at[0]),
        pltpu.make_async_copy(init_hbm, init_ref, sem_ref.at[1]),
    )
    slots = pltpu.make_async_copy(nb_hbm, nb_ref, sem_ref.at[2])
    for copy in (slots,) + bring:
        copy.start()
    total = trunc_ref[0]
    for q in range(1, RAD):
        total = total + trunc_ref[q]
    which = jnp.int32(0)
    for size in SIZES[:-1]:
        which = which + (total > size).astype(jnp.int32)
    which_ref[0] = which
    start, me = place()
    slots.wait()
    nbp_ref[...] = jnp.full((NBP, PD), -1, jnp.int32)
    nbp_ref[:NB, :] = nb_ref[...] - start
    local = nbp_ref[...]
    owner = local >> 7
    within = local & (PD - 1)
    remote = (owner != me) & (local >= 0)
    owner = jnp.where(remote, owner, -1)
    masks = [one_hot(owner == p) for p in range(PEERS)]
    before = one_hot(iota((NBP, NBP), 0) > iota((NBP, NBP), 1))
    in_column = jnp.dot(before, jnp.concatenate(masks, axis=1), preferred_element_type=F32)
    totals = jnp.concatenate(
        [jnp.sum(m.astype(F32), axis=0, keepdims=True) for m in masks], axis=0
    )
    left = one_hot(iota((PD, PD), 0) < iota((PD, PD), 1))
    columns = jnp.dot(totals.astype(BF16), left, preferred_element_type=F32)
    rank = jnp.zeros((NBP, PD), F32)
    for p in range(PEERS):
        here = in_column[:, p * PD : (p + 1) * PD] + columns[p : p + 1, :]
        rank = jnp.where(owner == p, here, rank)
    rank = rank.astype(jnp.int32)
    code = jnp.where(remote, owner * CAP + rank, -1)
    code_ref[...] = code
    pair = code >> 7
    lane = jnp.where(remote, code & (PD - 1), -1)
    particle = iota((1, PD), 1).astype(F32) + 1.0
    rows8 = iota((PAIRS, PD), 0)
    rows128 = iota((PD, PD), 0)
    for n in range(NB):
        mine = rows8 == pair[n : n + 1, :]
        names = within[n : n + 1, :].astype(F32)
        both = jnp.concatenate(
            [jnp.where(mine, names, 0.0), jnp.where(mine, particle, 0.0)], axis=0
        )
        a_ref[:, n * PD : (n + 1) * PD] = both.astype(BF16)
        b_ref[:, n * PD : (n + 1) * PD] = one_hot(rows128 == lane[n : n + 1, :])
    lists = lax.dot_general(a_ref[...], b_ref[...], NT, preferred_element_type=F32)
    lists_ref[...] = lists[PAIRS:]
    turned = pltpu.roll(lists, CAP, 1)
    first = iota((2 * PAIRS, PD), 1) < CAP
    both = (jnp.where(first, lists, turned), jnp.where(first, turned, lists))
    for p in range(PEERS):
        rows = both[p % 2]
        r = p // 2
        req_ref[p] = jnp.broadcast_to(rows[r : r + 1, :], (8, PD))
        names_ref[p : p + 1, :] = rows[PAIRS + r : PAIRS + r + 1, :]
    for copy in bring:
        copy.wait()


def wanted_row(rx_ref, r):
    even = rx_ref[2 * r][:1, :]
    odd = rx_ref[2 * r + 1][:1, :]
    return jnp.where(iota((1, PD), 1) < CAP, even, odd).astype(jnp.int32)


def local_kernel(
    trunc_ref, coef_ref, init_ref, out_ref, e_ref, re_ref, im_ref,
    f_ref, wide_re_ref, wide_im_ref, s_ref,
):
    init = init_ref[...]
    parts = two_parts(jnp.concatenate([init[:VEC], init[VEC:]], axis=1))
    out_ref[:HEAD, :] = parts
    for c in range(CW // PD):
        block = coef_ref[:, c * PD : (c + 1) * PD].astype(F32)
        f_ref[c * PD : (c + 1) * PD, :] = block.T
    offset = 0
    for q in range(RAD):
        here = pl.ds(offset, ANG)
        wide_re_ref[here, :] = f_ref[q * ANG : (q + 1) * ANG, :]
        wide_im_ref[here, :] = f_ref[(RAD + q) * ANG : (RAD + q + 1) * ANG, :]
        offset = offset + trunc_ref[q]
    for b in range(FULL // PD):
        rows = slice(b * PD, (b + 1) * PD)
        to = slice(HEAD + b * PD, HEAD + (b + 1) * PD)
        kept = iota((PD, PD), 0) + b * PD < offset
        out_ref[to, :PD] = jnp.where(kept, wide_re_ref[rows, :], 0.0).astype(BF16)
        out_ref[to, PD:] = jnp.where(kept, wide_im_ref[rows, :], 0.0).astype(BF16)
    own_pairs(trunc_ref, e_ref, re_ref, im_ref, f_ref, s_ref)


def pick_kernel(size, rx_ref, pack_ref, out_ref):
    r = pl.program_id(0)
    rows = iota((PD, PD), 0)
    first = iota((PD, PD), 1) < CAP
    sides = []
    for p in range(WIDE):
        picked = rows == rx_ref[WIDE * r + p][:1, :].astype(jnp.int32)
        top = one_hot(picked & first)
        bottom = one_hot(picked & jnp.logical_not(first))
        sides.append(jnp.concatenate([top, bottom], axis=0))
    side = jnp.concatenate(sides, axis=1)
    chosen = jnp.dot(pack_ref[:size, :], side, preferred_element_type=F32).astype(BF16)
    for p in range(WIDE):
        out_ref[p] = chosen[:, p * PD : (p + 1) * PD]


def own_pairs(trunc_ref, e_ref, re_ref, im_ref, xt_ref, s_ref):
    kept = kept_rows(trunc_ref, 2 * RAD, PD)

    def per_frequency(k, carry):
        rows = xt_ref[pl.ds(k, 2 * RAD, stride=ANG), :]
        masked = jnp.where(kept > k, rows, 0.0)
        turned = jnp.concatenate([masked[RAD:], -masked[:RAD]], axis=0)
        right = jnp.concatenate([masked, turned], axis=1).astype(BF16)
        s_ref[k] = lax.dot_general(
            rows.astype(BF16), right, TN, preferred_element_type=F32
        )
        return carry

    lax.fori_loop(0, ANG, per_frequency, 0, unroll=8)

    def per_rows(b, carry):
        sub = pl.ds(b * 8, 8)
        last_re = s_ref[0, sub, :PD]
        energy = last_re * last_re
        re = s_ref[1, sub, :PD]
        im = s_ref[1, sub, PD:]
        half = re * re + im * im
        first_re = last_re * re
        first_im = last_re * im
        m_re = jnp.zeros_like(re)
        m_im = jnp.zeros_like(re)
        for k in range(2, ANG):
            next_re = s_ref[k, sub, :PD]
            next_im = s_ref[k, sub, PD:]
            half = half + (next_re * next_re + next_im * next_im)
            m_re = m_re + (re * next_re + im * next_im)
            m_im = m_im + (im * next_re - re * next_im)
            re, im = next_re, next_im
        e_ref[sub, :] = energy + 0.5 * half
        re_ref[sub, :] = first_re + 0.5 * m_re
        im_ref[sub, :] = 0.5 * m_im - first_im
        return carry

    lax.fori_loop(0, PD // 8, per_rows, 0)


def far_kernel(
    size, trunc_ref, names_ref, pack_ref, recv_ref, table_ref, cur_ref,
    same_ref, cross_ref,
):
    r = pl.program_id(0)
    kept = size - HEAD

    @pl.when(r == 0)
    def _():
        for p in range(WIDE):
            same_ref[p, kept:, :] = jnp.zeros((ANG, PD), F32)
            cross_ref[p, kept:, :] = jnp.zeros((ANG, PD), F32)

    first = iota((PD, PD), 1) < CAP
    sides = []
    for p in range(WIDE):
        name = names_ref[pl.ds(WIDE * r + p, 1), :].astype(jnp.int32)
        named = iota((PD, PD), 0) + 1 == name
        low = one_hot(named & first)
        high = one_hot(named & jnp.logical_not(first))
        sides.append(jnp.concatenate([low, high], axis=0))
    mine = jnp.dot(
        pack_ref[HEAD:size, :], jnp.concatenate(sides, axis=1), preferred_element_type=F32
    )
    freq = iota((ANG, PD), 0)
    halves = []
    for p in range(WIDE):
        arrived = recv_ref[p, HEAD:, :].astype(F32)
        own = mine[:, p * PD : (p + 1) * PD]
        same_ref[p, :kept, :] = own * arrived
        cross_ref[p, :kept, :] = own * pltpu.roll(arrived, CAP, 1)
        parts = recv_ref[p, :HEAD, :].astype(F32)
        cur_ref[p] = parts[:VEC] + parts[VEC:]
    for p in range(WIDE):
        sum_re = jnp.zeros((ANG, PD), F32)
        sum_im = jnp.zeros((ANG, PD), F32)
        offset = 0
        for q in range(RAD):
            here = pl.ds(offset, ANG)
            inside = freq < trunc_ref[q]
            sum_re = sum_re + jnp.where(inside, same_ref[p, here, :], 0.0)
            sum_im = sum_im + jnp.where(inside, cross_ref[p, here, :], 0.0)
            offset = offset + trunc_ref[q]
        halves.append((sum_re, sum_im))
    first = first[:ANG]
    inner = (freq > 0) & (freq < ANG - 1)
    for b in range(WIDE // 2):
        even, odd = halves[2 * b], halves[2 * b + 1]
        s_re = jnp.where(first, even[0], odd[0])
        s_re = s_re + pltpu.roll(jnp.where(first, odd[0], even[0]), CAP, 1)
        s_im = pltpu.roll(jnp.where(first, odd[1], even[1]), CAP, 1)
        s_im = jnp.where(first, s_im - even[1], odd[1] - s_im)
        power = s_re * s_re + s_im * s_im
        next_re = pltpu.roll(s_re, ANG - 1, 0)
        next_im = pltpu.roll(s_im, ANG - 1, 0)
        zero_re = s_re[:1]
        energy = zero_re * zero_re + 0.5 * jnp.sum(
            jnp.where(freq == 0, 0.0, power), axis=0, keepdims=True
        )
        m_re = zero_re * s_re[1:2] + 0.5 * jnp.sum(
            jnp.where(inner, s_re * next_re + s_im * next_im, 0.0), axis=0, keepdims=True
        )
        m_im = 0.5 * jnp.sum(
            jnp.where(inner, s_im * next_re - s_re * next_im, 0.0), axis=0, keepdims=True
        ) - zero_re * s_im[1:2]
        table_ref[b] = jnp.concatenate(
            [energy, m_re, m_im, jnp.zeros((5, PD), F32)], axis=0
        )


def near_image(cur, w_re, w_im):
    weights = jnp.concatenate([w_re, w_im], axis=1)
    both = jnp.dot(cur, weights, precision=HIGHEST, preferred_element_type=F32)
    re = both[:VEC, :PD] - both[VEC:, PD:]
    im = both[VEC:, :PD] + both[:VEC, PD:]
    return jnp.concatenate([re, im], axis=0)


def far_image(slots, table_ref, lists_ref):
    values = []
    picks = []
    for r in range(PAIRS):
        m_re = table_ref[r, 1:2, :]
        m_im = table_ref[r, 2:3, :]
        c_re, c_im = slots[r][:VEC], slots[r][VEC:]
        values.append(
            jnp.concatenate([m_re * c_re - m_im * c_im, m_re * c_im + m_im * c_re], axis=0)
        )
        particle = lists_ref[r : r + 1, :].astype(jnp.int32)
        picks.append(one_hot(iota((PD, PD), 0) + 1 == particle))
    return exact_select(
        jnp.concatenate(values, axis=1), jnp.concatenate(picks, axis=1), NT
    )


def send_columns(cur, rx_ref, out_ref):
    picks = [one_hot(iota((PD, PD), 0) == wanted_row(rx_ref, r)) for r in range(PAIRS)]
    columns = exact_select(cur, jnp.concatenate(picks, axis=1))
    first = iota((VEC, PD), 1) < CAP
    for r in range(PAIRS):
        re = columns[:VEC, r * PD : (r + 1) * PD]
        im = columns[VEC:, r * PD : (r + 1) * PD]
        out_ref[2 * r] = jnp.where(first, re, pltpu.roll(im, CAP, 1))
        out_ref[2 * r + 1] = jnp.where(first, pltpu.roll(re, CAP, 1), im)


def received_columns(recv_ref):
    first = iota((VEC, PD), 1) < CAP
    slots = []
    for r in range(PAIRS):
        even = recv_ref[2 * r]
        odd = recv_ref[2 * r + 1]
        re = jnp.where(first, even, pltpu.roll(odd, CAP, 1))
        im = jnp.where(first, pltpu.roll(even, CAP, 1), odd)
        slots.append(jnp.concatenate([re, im], axis=0))
    return slots


def first_kernel(
    nb_ref, code_ref, lists_ref, table_ref, e_ref, re_ref, im_ref,
    slots_ref, init_ref, rx_ref,
    align_ref, weights_ref, degree_ref, cur_ref, send_ref, near_ref,
):
    start, me = place()
    local = nb_ref[...] - start
    near = (local >> 7) == me
    near_ref[...] = jnp.full((PD, PD), -1.0, F32)
    near_ref[:NB, :] = jnp.where(near, local & (PD - 1), -1).astype(F32)
    rows = iota((PD, PD), 0).astype(F32)
    counts = jnp.zeros((PD, PD), F32)
    for n in range(NB):
        counts = counts + jnp.where(rows == near_ref[n : n + 1, :], 1.0, 0.0)
    named = near_ref[...].T.astype(jnp.int32)
    inside = jnp.maximum(named, 0)
    values = []
    for ref, sign in ((e_ref, 1.0), (re_ref, 1.0), (im_ref, -1.0)):
        found = jnp.take_along_axis(ref[...], inside, axis=1, mode="promise_in_bounds")
        values.append(jnp.where(named >= 0, sign * found, 0.0).T[:NBP])
    code = code_ref[...]
    pair = code >> 7
    lane = code & (PD - 1)
    for r in range(PAIRS):
        mine = pair == r
        for v in range(3):
            row = jnp.broadcast_to(table_ref[r, v : v + 1, :], (NBP, PD))
            found = jnp.take_along_axis(row, lane, axis=1, mode="promise_in_bounds")
            values[v] = jnp.where(mine, found, values[v])
    below = values[0] + EPS
    align_ref[:, 0, :] = (values[1] / below)[:NB]
    align_ref[:, 1, :] = (values[2] / below)[:NB]
    degree = EPS + jnp.sum(values[0], axis=0, keepdims=True)
    degree_ref[...] = jnp.broadcast_to(degree, (8, PD))
    w_re = counts * re_ref[...]
    w_im = counts * im_ref[...]
    weights_ref[0] = w_re
    weights_ref[1] = w_im
    slots = received_columns(slots_ref)
    image = near_image(init_ref[...], w_re, w_im) + far_image(slots, table_ref, lists_ref)
    image = image / degree
    cur_ref[...] = image
    send_columns(image, rx_ref, send_ref)


def next_image(recv_ref, cur_ref, weights_ref, degree_ref, table_ref, lists_ref):
    slots = received_columns(recv_ref)
    image = near_image(cur_ref[...], weights_ref[0], weights_ref[1])
    image = image + far_image(slots, table_ref, lists_ref)
    return image / degree_ref[:1, :]


def middle_kernel(
    recv_ref, cur_ref, weights_ref, degree_ref, table_ref, lists_ref, rx_ref,
    out_ref, send_ref,
):
    image = next_image(recv_ref, cur_ref, weights_ref, degree_ref, table_ref, lists_ref)
    out_ref[...] = image
    send_columns(image, rx_ref, send_ref)


def last_kernel(
    total, recv_ref, cur_ref, weights_ref, degree_ref, table_ref, lists_ref,
    out_ref, gram_ref,
):
    image = next_image(recv_ref, cur_ref, weights_ref, degree_ref, table_ref, lists_ref)
    out_ref[...] = image
    gram = lax.dot_general(
        image[:VEC], image[:VEC], NT, precision=HIGHEST, preferred_element_type=F32
    ) + lax.dot_general(
        image[VEC:], image[VEC:], NT, precision=HIGHEST, preferred_element_type=F32
    )
    gram = gram * (1.0 / total)
    wide = jnp.concatenate([gram] * 8, axis=1)
    mine = iota((VEC, PD), 1) // VEC == iota((VEC, PD), 0) % 8
    wide = jnp.where(mine, wide, 0.0)
    packed = jnp.concatenate(
        [
            jnp.sum(wide[:8], axis=0, keepdims=True),
            jnp.sum(wide[8:], axis=0, keepdims=True),
        ],
        axis=0,
    )
    gram_ref[...] = jnp.broadcast_to(packed[None], gram_ref.shape)


def finish_kernel(grams_ref, cur_ref, out_ref):
    packed = jnp.sum(grams_ref[...], axis=0)
    row = iota((VEC, PD), 0)
    lane = iota((VEC, PD), 1)
    wide = jnp.where(row < 8, packed[0:1, :], packed[1:2, :])
    wide = jnp.where(lane // VEC == row % 8, wide, 0.0)
    for shift in (64, 32, 16):
        wide = wide + pltpu.roll(wide, shift, 1)
    columns = [jnp.broadcast_to(wide[:, c : c + 1], (VEC, PD)) for c in range(VEC)]
    re = cur_ref[:VEC, :]
    im = cur_ref[VEC:, :]
    for c in range(VEC):
        pivot = columns[c][c : c + 1, :]
        scale = lax.rsqrt(pivot)
        scale = scale * (1.5 - 0.5 * pivot * scale * scale)
        column = jnp.where(row > c, columns[c] * scale, 0.0)
        for d in range(c + 1, VEC):
            columns[d] = columns[d] - column * (columns[d][c : c + 1, :] * scale)
        top_re = re[c : c + 1, :] * scale
        top_im = im[c : c + 1, :] * scale
        here = row == c
        re = jnp.where(here, top_re, re - column * top_re)
        im = jnp.where(here, top_im, im - column * top_im)
    out_ref[:VEC, :] = re
    out_ref[VEC:, :] = im


def struct(shape, dtype=F32):
    return jax.ShapeDtypeStruct(shape, dtype)


SMEM = pl.BlockSpec(memory_space=pltpu.SMEM)
VMEM = pl.BlockSpec(memory_space=pltpu.VMEM)
HBM = pl.BlockSpec(memory_space=pltpu.HBM)


def grant(mib):
    return pltpu.CompilerParams(vmem_limit_bytes=mib << 20)


def whole(*shape):
    return pl.BlockSpec(shape, lambda r: (0,) * len(shape))


def exchange(size, truncation, names, asked, packed):
    steps = PEERS // WIDE
    sent = pl.pallas_call(
        functools.partial(pick_kernel, size),
        grid=(steps,),
        out_shape=struct((PEERS, size, PD), BF16),
        in_specs=[whole(PEERS, 8, PD), whole(HEAD + FULL, 2 * PD)],
        out_specs=pl.BlockSpec((WIDE, size, PD), lambda r: (r, 0, 0)),
        compiler_params=grant(16),
        name="pick",
    )(asked, packed)
    received = lax.all_to_all(sent, REP, 0, 0, tiled=True)
    return pl.pallas_call(
        functools.partial(far_kernel, size),
        grid=(steps,),
        out_shape=(struct((PAIRS, 8, PD)), struct((PEERS, VEC, PD))),
        in_specs=[
            SMEM,
            whole(PEERS, PD),
            whole(HEAD + FULL, 2 * PD),
            pl.BlockSpec((WIDE, size, PD), lambda r: (r, 0, 0)),
        ],
        out_specs=(
            pl.BlockSpec((WIDE // 2, 8, PD), lambda r: (r, 0, 0)),
            pl.BlockSpec((WIDE, VEC, PD), lambda r: (r, 0, 0)),
        ),
        scratch_shapes=[
            pltpu.VMEM((WIDE, size - HEAD + ANG, PD), F32),
            pltpu.VMEM((WIDE, size - HEAD + ANG, PD), F32),
        ],
        compiler_params=grant(20),
        name="far",
    )(truncation, names, packed, received)


def shards(coefficients, truncation, neighbours, initial):
    groups = lax.axis_size(GRP)
    replicas = lax.axis_size(REP)
    devices = groups * replicas
    which, code, lists, names, requests, coefficients, initial = pl.pallas_call(
        slot_kernel,
        out_shape=(
            struct((1,), jnp.int32),
            struct((NBP, PD), jnp.int32),
            struct((PAIRS, PD)),
            struct((PEERS, PD)),
            struct((PEERS, 8, PD)),
            struct((PD, CW), BF16),
            struct((32, PD)),
        ),
        in_specs=[SMEM, HBM, HBM, HBM],
        out_specs=(SMEM,) + (VMEM,) * 6,
        compiler_params=grant(6),
        scratch_shapes=[
            pltpu.VMEM((NB, PD), jnp.int32),
            pltpu.VMEM((NBP, PD), jnp.int32),
            pltpu.VMEM((2 * PAIRS, NB * PD), BF16),
            pltpu.VMEM((PD, NB * PD), BF16),
            pltpu.SemaphoreType.DMA((3,)),
        ],
        name="slots",
    )(
        truncation,
        *(
            pltpu.with_memory_space_constraint(x, pltpu.HBM)
            for x in (neighbours, coefficients, initial)
        ),
    )
    asked = lax.all_to_all(requests, REP, 0, 0, tiled=True)
    packed, e_own, re_own, im_own = pl.pallas_call(
        local_kernel,
        out_shape=(struct((HEAD + FULL, 2 * PD), BF16),) + (struct((PD, PD)),) * 3,
        in_specs=[SMEM, VMEM, VMEM],
        scratch_shapes=[
            pltpu.VMEM((CW, PD), F32),
            pltpu.VMEM((FULL + ANG, PD), F32),
            pltpu.VMEM((FULL + ANG, PD), F32),
            pltpu.VMEM((ANG, PD, 2 * PD), F32),
        ],
        cost_estimate=pl.CostEstimate(
            flops=20_000_000_000, bytes_accessed=1_000_000, transcendentals=0
        ),
        compiler_params=grant(20),
        name="local",
    )(truncation, coefficients, initial)
    table, slots = lax.switch(
        which[0],
        [functools.partial(exchange, HEAD + size) for size in SIZES],
        truncation, names, asked, packed,
    )
    alignment, weights, degree, current, columns = pl.pallas_call(
        first_kernel,
        out_shape=(
            struct((NB, 2, PD)),
            struct((2, PD, PD)),
            struct((8, PD)),
            struct((32, PD)),
            struct((PEERS, VEC, PD)),
        ),
        in_specs=[VMEM] * 10,
        compiler_params=grant(6),
        scratch_shapes=[pltpu.VMEM((PD, PD), F32)],
        name="first",
    )(
        neighbours, code, lists, table, e_own, re_own, im_own,
        slots, initial, asked,
    )
    columns = lax.all_to_all(columns, REP, 0, 0, tiled=True)
    current, columns = pl.pallas_call(
        middle_kernel,
        out_shape=(struct((32, PD)), struct((PEERS, VEC, PD))),
        compiler_params=grant(6),
        name="middle",
    )(columns, current, weights, degree, table, lists, asked)
    columns = lax.all_to_all(columns, REP, 0, 0, tiled=True)
    current, gram = pl.pallas_call(
        functools.partial(last_kernel, float(PD * devices)),
        out_shape=(struct((32, PD)), struct((devices, 2, PD))),
        compiler_params=grant(6),
        name="last",
    )(columns, current, weights, degree, table, lists)
    grams = lax.all_to_all(gram, GRP_REP, 0, 0, tiled=True)
    vectors = pl.pallas_call(
        finish_kernel,
        out_shape=struct((32, PD)),
        compiler_params=grant(6),
        name="finish",
    )(grams, current)
    return (jnp.transpose(alignment, (1, 0, 2)), vectors)


def solution(mesh):
    split = Mesh(mesh.devices.reshape(4, 2, 4, 4), GRP_REP)
    in_specs = (P(GRP_REP, None), P(), P(None, GRP_REP), P(None, GRP_REP))
    out_specs = (P(None, None, GRP_REP), P(None, GRP_REP))
    return jax.shard_map(
        shards, mesh=split, in_specs=in_specs, out_specs=out_specs, check_vma=False
    )
```

```python
import functools

import jax
import jax.numpy as jnp
from jax import lax
from jax.experimental import pallas as pl
from jax.experimental.pallas import tpu as pltpu
from jax.sharding import Mesh
from jax.sharding import PartitionSpec as P

ANG = 64
RAD = 16
NB = 50
NBP = 56
VEC = 16
PD = 128
CAP = 64
CW = 2048
FULL = RAD * ANG
SIZES = (384, 512, 544, 576, 608, 640, 672, 704, 736, 768, 896, FULL)
HEAD = 2 * VEC
PEERS = 16
PAIRS = PEERS // 2
WIDE = 4
GROUP = 8
GRP = ("grp_0", "grp_1")
REP = ("rep_0", "rep_1")
GRP_REP = ("grp_0", "grp_1", "rep_0", "rep_1")
EPS = 1e-06
F32 = jnp.float32
BF16 = jnp.bfloat16
HIGHEST = lax.Precision.HIGHEST

NT = (((1,), (1,)), ((), ()))
TN = (((0,), (0,)), ((), ()))


def iota(shape, dim):
    return lax.broadcasted_iota(jnp.int32, shape, dim)


def one_hot(cond):
    return jnp.where(cond, 1.0, 0.0).astype(BF16)


def three_parts(x):
    high = x.astype(BF16)
    rest = x - high.astype(F32)
    mid = rest.astype(BF16)
    low = (rest - mid.astype(F32)).astype(BF16)
    return jnp.concatenate([high, mid, low], axis=0)


def two_parts(x):
    high = x.astype(BF16)
    rest = (x - high.astype(F32)).astype(BF16)
    return jnp.concatenate([high, rest], axis=0)


def exact_select(x, selector, dims=(((1,), (0,)), ((), ()))):
    rows = x.shape[0]
    parts = lax.dot_general(three_parts(x), selector, dims, preferred_element_type=F32)
    return parts[:rows] + (parts[rows : 2 * rows] + parts[2 * rows :])


def kept_rows(trunc_ref, rows, lanes):
    row = iota((rows, lanes), 0) % RAD
    kept = jnp.zeros((rows, lanes), jnp.int32)
    for q in range(RAD):
        kept = jnp.where(row == q, trunc_ref[q], kept)
    return kept


def place():
    index = [lax.axis_index(name) for name in GRP_REP]
    size = [lax.axis_size(name) for name in GRP_REP]
    group = index[0] * size[1] + index[1]
    member = index[2] * size[3] + index[3]
    return group * (size[2] * size[3] * PD), member


def slot_kernel(
    trunc_ref, nb_hbm, coef_hbm, init_hbm,
    which_ref, code_ref, lists_ref, names_ref, req_ref, coef_ref, init_ref,
    nb_ref, nbp_ref, a_ref, b_ref, sem_ref,
):
    bring = (
        pltpu.make_async_copy(coef_hbm, coef_ref, sem_ref.at[0]),
        pltpu.make_async_copy(init_hbm, init_ref, sem_ref.at[1]),
    )
    slots = pltpu.make_async_copy(nb_hbm, nb_ref, sem_ref.at[2])
    for copy in (slots,) + bring:
        copy.start()
    total = trunc_ref[0]
    for q in range(1, RAD):
        total = total + trunc_ref[q]
    which = jnp.int32(0)
    for size in SIZES[:-1]:
        which = which + (total > size).astype(jnp.int32)
    which_ref[0] = which
    start, me = place()
    slots.wait()
    nbp_ref[...] = jnp.full((NBP, PD), -1, jnp.int32)
    nbp_ref[:NB, :] = nb_ref[...] - start
    local = nbp_ref[...]
    owner = local >> 7
    within = local & (PD - 1)
    remote = (owner != me) & (local >= 0)
    owner = jnp.where(remote, owner, -1)
    masks = [one_hot(owner == p) for p in range(PEERS)]
    before = one_hot(iota((NBP, NBP), 0) > iota((NBP, NBP), 1))
    in_column = jnp.dot(before, jnp.concatenate(masks, axis=1), preferred_element_type=F32)
    totals = jnp.concatenate(
        [jnp.sum(m.astype(F32), axis=0, keepdims=True) for m in masks], axis=0
    )
    left = one_hot(iota((PD, PD), 0) < iota((PD, PD), 1))
    columns = jnp.dot(totals.astype(BF16), left, preferred_element_type=F32)
    rank = jnp.zeros((NBP, PD), F32)
    for p in range(PEERS):
        here = in_column[:, p * PD : (p + 1) * PD] + columns[p : p + 1, :]
        rank = jnp.where(owner == p, here, rank)
    rank = rank.astype(jnp.int32)
    code = jnp.where(remote, owner * CAP + rank, -1)
    code_ref[...] = code
    pair = code >> 7
    lane = jnp.where(remote, code & (PD - 1), -1)
    particle = iota((1, PD), 1).astype(F32) + 1.0
    rows8 = iota((PAIRS, PD), 0)
    rows128 = iota((PD, PD), 0)
    for n in range(NB):
        mine = rows8 == pair[n : n + 1, :]
        names = within[n : n + 1, :].astype(F32)
        both = jnp.concatenate(
            [jnp.where(mine, names, 0.0), jnp.where(mine, particle, 0.0)], axis=0
        )
        a_ref[:, n * PD : (n + 1) * PD] = both.astype(BF16)
        b_ref[:, n * PD : (n + 1) * PD] = one_hot(rows128 == lane[n : n + 1, :])
    lists = lax.dot_general(a_ref[...], b_ref[...], NT, preferred_element_type=F32)
    lists_ref[...] = lists[PAIRS:]
    turned = pltpu.roll(lists, CAP, 1)
    first = iota((2 * PAIRS, PD), 1) < CAP
    both = (jnp.where(first, lists, turned), jnp.where(first, turned, lists))
    for p in range(PEERS):
        rows = both[p % 2]
        r = p // 2
        req_ref[p] = jnp.broadcast_to(rows[r : r + 1, :], (8, PD))
        names_ref[p : p + 1, :] = rows[PAIRS + r : PAIRS + r + 1, :]
    for copy in bring:
        copy.wait()


def wanted_row(rx_ref, r):
    even = rx_ref[2 * r][:1, :]
    odd = rx_ref[2 * r + 1][:1, :]
    return jnp.where(iota((1, PD), 1) < CAP, even, odd).astype(jnp.int32)


def local_kernel(
    trunc_ref, coef_ref, init_ref, out_ref, e_ref, re_ref, im_ref,
    f_ref, wide_re_ref, wide_im_ref, s_ref,
):
    init = init_ref[...]
    parts = two_parts(jnp.concatenate([init[:VEC], init[VEC:]], axis=1))
    out_ref[:HEAD, :] = parts
    for c in range(CW // PD):
        block = coef_ref[:, c * PD : (c + 1) * PD].astype(F32)
        f_ref[c * PD : (c + 1) * PD, :] = block.T
    offset = 0
    for q in range(RAD):
        here = pl.ds(offset, ANG)
        wide_re_ref[here, :] = f_ref[q * ANG : (q + 1) * ANG, :]
        wide_im_ref[here, :] = f_ref[(RAD + q) * ANG : (RAD + q + 1) * ANG, :]
        offset = offset + trunc_ref[q]
    for b in range(FULL // PD):
        rows = slice(b * PD, (b + 1) * PD)
        to = slice(HEAD + b * PD, HEAD + (b + 1) * PD)
        kept = iota((PD, PD), 0) + b * PD < offset
        out_ref[to, :PD] = jnp.where(kept, wide_re_ref[rows, :], 0.0).astype(BF16)
        out_ref[to, PD:] = jnp.where(kept, wide_im_ref[rows, :], 0.0).astype(BF16)
    own_pairs(trunc_ref, e_ref, re_ref, im_ref, f_ref, s_ref)


def pick_kernel(size, rx_ref, pack_ref, out_ref):
    r = pl.program_id(0)
    rows = iota((PD, PD), 0)
    first = iota((PD, PD), 1) < CAP
    sides = []
    for p in range(WIDE):
        picked = rows == rx_ref[WIDE * r + p][:1, :].astype(jnp.int32)
        top = one_hot(picked & first)
        bottom = one_hot(picked & jnp.logical_not(first))
        sides.append(jnp.concatenate([top, bottom], axis=0))
    side = jnp.concatenate(sides, axis=1)
    chosen = jnp.dot(pack_ref[:size, :], side, preferred_element_type=F32).astype(BF16)
    for p in range(WIDE):
        out_ref[p] = chosen[:, p * PD : (p + 1) * PD]


def own_pairs(trunc_ref, e_ref, re_ref, im_ref, xt_ref, s_ref):
    kept = kept_rows(trunc_ref, 2 * RAD, PD)
    e_ref[...] = jnp.zeros((PD, PD), F32)
    re_ref[...] = jnp.zeros((PD, PD), F32)
    im_ref[...] = jnp.zeros((PD, PD), F32)

    def sums(first):
        for b in range(PD // 8):
            sub = slice(b * 8, (b + 1) * 8)
            energy = e_ref[sub, :]
            m_re = re_ref[sub, :]
            m_im = im_ref[sub, :]
            before = max(first - 1, 0)
            re = s_ref[before, sub, :PD]
            im = s_ref[before, sub, PD:]
            for k in range(first, first + GROUP):
                if k == 0:
                    energy = energy + re * re
                    continue
                next_re = s_ref[k, sub, :PD]
                next_im = s_ref[k, sub, PD:]
                half_re = 0.5 * next_re
                half_im = 0.5 * next_im
                energy = energy + (half_re * next_re + half_im * next_im)
                if k == 1:
                    m_re = m_re + re * next_re
                    m_im = m_im - re * next_im
                else:
                    m_re = m_re + (re * half_re + im * half_im)
                    m_im = m_im + (im * half_re - re * half_im)
                re, im = next_re, next_im
            e_ref[sub, :] = energy
            re_ref[sub, :] = m_re
            im_ref[sub, :] = m_im

    for first in range(0, ANG, GROUP):
        for k in range(first, first + GROUP):
            rows = xt_ref[pl.ds(k, 2 * RAD, stride=ANG), :]
            masked = rows if k < 16 else jnp.where(kept > k, rows, 0.0)
            turned = jnp.concatenate([masked[RAD:], -masked[:RAD]], axis=0)
            right = jnp.concatenate([masked, turned], axis=1).astype(BF16)
            s_ref[k] = lax.dot_general(
                rows.astype(BF16), right, TN, preferred_element_type=F32
            )
        if first > 0:
            sums(first - GROUP)
    sums(ANG - GROUP)


def far_kernel(
    size, trunc_ref, names_ref, pack_ref, recv_ref, table_ref, cur_ref,
    same_ref, cross_ref,
):
    r = pl.program_id(0)
    kept = size - HEAD

    @pl.when(r == 0)
    def _():
        for p in range(WIDE):
            same_ref[p, kept:, :] = jnp.zeros((ANG, PD), F32)
            cross_ref[p, kept:, :] = jnp.zeros((ANG, PD), F32)

    first = iota((PD, PD), 1) < CAP
    sides = []
    for p in range(WIDE):
        name = names_ref[pl.ds(WIDE * r + p, 1), :].astype(jnp.int32)
        named = iota((PD, PD), 0) + 1 == name
        low = one_hot(named & first)
        high = one_hot(named & jnp.logical_not(first))
        sides.append(jnp.concatenate([low, high], axis=0))
    mine = jnp.dot(
        pack_ref[HEAD:size, :], jnp.concatenate(sides, axis=1), preferred_element_type=F32
    )
    freq = iota((ANG, PD), 0)
    halves = []
    for p in range(WIDE):
        arrived = recv_ref[p, HEAD:, :].astype(F32)
        own = mine[:, p * PD : (p + 1) * PD]
        same_ref[p, :kept, :] = own * arrived
        cross_ref[p, :kept, :] = own * pltpu.roll(arrived, CAP, 1)
        parts = recv_ref[p, :HEAD, :].astype(F32)
        cur_ref[p] = parts[:VEC] + parts[VEC:]
    for b in range(WIDE // 2):
        both = (2 * b, 2 * b + 1)
        totals = [[jnp.zeros((ANG, PD), F32)] * 2 for _ in both]
        offset = 0
        for q in range(RAD):
            here = pl.ds(offset, ANG)
            inside = freq < trunc_ref[q]
            for p in both:
                for v, ref in enumerate((same_ref, cross_ref)):
                    total = totals[p % 2][v]
                    totals[p % 2][v] = total + jnp.where(inside, ref[p, here, :], 0.0)
            offset = offset + trunc_ref[q]
        halves.extend(totals)
    first = first[:ANG]
    inner = (freq > 0) & (freq < ANG - 1)
    for b in range(WIDE // 2):
        even, odd = halves[2 * b], halves[2 * b + 1]
        s_re = jnp.where(first, even[0], odd[0])
        s_re = s_re + pltpu.roll(jnp.where(first, odd[0], even[0]), CAP, 1)
        s_im = pltpu.roll(jnp.where(first, odd[1], even[1]), CAP, 1)
        s_im = jnp.where(first, s_im - even[1], odd[1] - s_im)
        power = s_re * s_re + s_im * s_im
        next_re = pltpu.roll(s_re, ANG - 1, 0)
        next_im = pltpu.roll(s_im, ANG - 1, 0)
        zero_re = s_re[:1]
        energy = zero_re * zero_re + 0.5 * jnp.sum(
            jnp.where(freq == 0, 0.0, power), axis=0, keepdims=True
        )
        m_re = zero_re * s_re[1:2] + 0.5 * jnp.sum(
            jnp.where(inner, s_re * next_re + s_im * next_im, 0.0), axis=0, keepdims=True
        )
        m_im = 0.5 * jnp.sum(
            jnp.where(inner, s_im * next_re - s_re * next_im, 0.0), axis=0, keepdims=True
        ) - zero_re * s_im[1:2]
        table_ref[b] = jnp.concatenate(
            [energy, m_re, m_im, jnp.zeros((5, PD), F32)], axis=0
        )


def near_image(cur, w_re, w_im):
    weights = jnp.concatenate([w_re, w_im], axis=1)
    both = jnp.dot(cur, weights, precision=HIGHEST, preferred_element_type=F32)
    re = both[:VEC, :PD] - both[VEC:, PD:]
    im = both[VEC:, :PD] + both[:VEC, PD:]
    return jnp.concatenate([re, im], axis=0)


def far_image(slots, table_ref, lists_ref):
    values = []
    picks = []
    for r in range(PAIRS):
        m_re = table_ref[r, 1:2, :]
        m_im = table_ref[r, 2:3, :]
        c_re, c_im = slots[r][:VEC], slots[r][VEC:]
        values.append(
            jnp.concatenate([m_re * c_re - m_im * c_im, m_re * c_im + m_im * c_re], axis=0)
        )
        particle = lists_ref[r : r + 1, :].astype(jnp.int32)
        picks.append(one_hot(iota((PD, PD), 0) + 1 == particle))
    return exact_select(
        jnp.concatenate(values, axis=1), jnp.concatenate(picks, axis=1), NT
    )


def send_columns(cur, rx_ref, out_ref):
    picks = [one_hot(iota((PD, PD), 0) == wanted_row(rx_ref, r)) for r in range(PAIRS)]
    columns = exact_select(cur, jnp.concatenate(picks, axis=1))
    first = iota((VEC, PD), 1) < CAP
    for r in range(PAIRS):
        re = columns[:VEC, r * PD : (r + 1) * PD]
        im = columns[VEC:, r * PD : (r + 1) * PD]
        out_ref[2 * r] = jnp.where(first, re, pltpu.roll(im, CAP, 1))
        out_ref[2 * r + 1] = jnp.where(first, pltpu.roll(re, CAP, 1), im)


def received_columns(recv_ref):
    first = iota((VEC, PD), 1) < CAP
    slots = []
    for r in range(PAIRS):
        even = recv_ref[2 * r]
        odd = recv_ref[2 * r + 1]
        re = jnp.where(first, even, pltpu.roll(odd, CAP, 1))
        im = jnp.where(first, pltpu.roll(even, CAP, 1), odd)
        slots.append(jnp.concatenate([re, im], axis=0))
    return slots


def first_kernel(
    nb_ref, code_ref, lists_ref, table_ref, e_ref, re_ref, im_ref,
    slots_ref, init_ref, rx_ref,
    align_ref, weights_ref, degree_ref, cur_ref, send_ref, near_ref,
):
    start, me = place()
    local = nb_ref[...] - start
    near = (local >> 7) == me
    near_ref[...] = jnp.full((PD, PD), -1.0, F32)
    near_ref[:NB, :] = jnp.where(near, local & (PD - 1), -1).astype(F32)
    rows = iota((PD, PD), 0).astype(F32)
    counts = jnp.zeros((PD, PD), F32)
    for n in range(NB):
        counts = counts + jnp.where(rows == near_ref[n : n + 1, :], 1.0, 0.0)
    named = near_ref[...].T.astype(jnp.int32)
    inside = jnp.maximum(named, 0)
    values = []
    for ref, sign in ((e_ref, 1.0), (re_ref, 1.0), (im_ref, -1.0)):
        found = jnp.take_along_axis(ref[...], inside, axis=1, mode="promise_in_bounds")
        values.append(jnp.where(named >= 0, sign * found, 0.0).T[:NBP])
    code = code_ref[...]
    pair = code >> 7
    lane = code & (PD - 1)
    for r in range(PAIRS):
        mine = pair == r
        for v in range(3):
            row = jnp.broadcast_to(table_ref[r, v : v + 1, :], (NBP, PD))
            found = jnp.take_along_axis(row, lane, axis=1, mode="promise_in_bounds")
            values[v] = jnp.where(mine, found, values[v])
    below = values[0] + EPS
    align_ref[:, 0, :] = (values[1] / below)[:NB]
    align_ref[:, 1, :] = (values[2] / below)[:NB]
    degree = EPS + jnp.sum(values[0], axis=0, keepdims=True)
    degree_ref[...] = jnp.broadcast_to(degree, (8, PD))
    w_re = counts * re_ref[...]
    w_im = counts * im_ref[...]
    weights_ref[0] = w_re
    weights_ref[1] = w_im
    slots = received_columns(slots_ref)
    image = near_image(init_ref[...], w_re, w_im) + far_image(slots, table_ref, lists_ref)
    image = image / degree
    cur_ref[...] = image
    send_columns(image, rx_ref, send_ref)


def next_image(recv_ref, cur_ref, weights_ref, degree_ref, table_ref, lists_ref):
    slots = received_columns(recv_ref)
    image = near_image(cur_ref[...], weights_ref[0], weights_ref[1])
    image = image + far_image(slots, table_ref, lists_ref)
    return image / degree_ref[:1, :]


def middle_kernel(
    recv_ref, cur_ref, weights_ref, degree_ref, table_ref, lists_ref, rx_ref,
    out_ref, send_ref,
):
    image = next_image(recv_ref, cur_ref, weights_ref, degree_ref, table_ref, lists_ref)
    out_ref[...] = image
    send_columns(image, rx_ref, send_ref)


def last_kernel(
    total, recv_ref, cur_ref, weights_ref, degree_ref, table_ref, lists_ref,
    out_ref, gram_ref,
):
    image = next_image(recv_ref, cur_ref, weights_ref, degree_ref, table_ref, lists_ref)
    out_ref[...] = image
    gram = lax.dot_general(
        image[:VEC], image[:VEC], NT, precision=HIGHEST, preferred_element_type=F32
    ) + lax.dot_general(
        image[VEC:], image[VEC:], NT, precision=HIGHEST, preferred_element_type=F32
    )
    gram = gram * (1.0 / total)
    wide = jnp.concatenate([gram] * 8, axis=1)
    mine = iota((VEC, PD), 1) // VEC == iota((VEC, PD), 0) % 8
    wide = jnp.where(mine, wide, 0.0)
    packed = jnp.concatenate(
        [
            jnp.sum(wide[:8], axis=0, keepdims=True),
            jnp.sum(wide[8:], axis=0, keepdims=True),
        ],
        axis=0,
    )
    gram_ref[...] = jnp.broadcast_to(packed[None], gram_ref.shape)


def finish_kernel(grams_ref, cur_ref, out_ref):
    packed = jnp.sum(grams_ref[...], axis=0)
    row = iota((VEC, PD), 0)
    lane = iota((VEC, PD), 1)
    wide = jnp.where(row < 8, packed[0:1, :], packed[1:2, :])
    wide = jnp.where(lane // VEC == row % 8, wide, 0.0)
    for shift in (64, 32, 16):
        wide = wide + pltpu.roll(wide, shift, 1)
    columns = [jnp.broadcast_to(wide[:, c : c + 1], (VEC, PD)) for c in range(VEC)]
    re = cur_ref[:VEC, :]
    im = cur_ref[VEC:, :]
    for c in range(VEC):
        pivot = columns[c][c : c + 1, :]
        scale = lax.rsqrt(pivot)
        scale = scale * (1.5 - 0.5 * pivot * scale * scale)
        column = jnp.where(row > c, columns[c] * scale, 0.0)
        for d in range(c + 1, VEC):
            columns[d] = columns[d] - column * (columns[d][c : c + 1, :] * scale)
        top_re = re[c : c + 1, :] * scale
        top_im = im[c : c + 1, :] * scale
        here = row == c
        re = jnp.where(here, top_re, re - column * top_re)
        im = jnp.where(here, top_im, im - column * top_im)
    out_ref[:VEC, :] = re
    out_ref[VEC:, :] = im


def struct(shape, dtype=F32):
    return jax.ShapeDtypeStruct(shape, dtype)


SMEM = pl.BlockSpec(memory_space=pltpu.SMEM)
VMEM = pl.BlockSpec(memory_space=pltpu.VMEM)
HBM = pl.BlockSpec(memory_space=pltpu.HBM)


def grant(mib):
    return pltpu.CompilerParams(vmem_limit_bytes=mib << 20)


def whole(*shape):
    return pl.BlockSpec(shape, lambda r: (0,) * len(shape))


def exchange(size, truncation, names, asked, packed):
    steps = PEERS // WIDE
    sent = pl.pallas_call(
        functools.partial(pick_kernel, size),
        grid=(steps,),
        out_shape=struct((PEERS, size, PD), BF16),
        in_specs=[whole(PEERS, 8, PD), whole(HEAD + FULL, 2 * PD)],
        out_specs=pl.BlockSpec((WIDE, size, PD), lambda r: (r, 0, 0)),
        compiler_params=grant(16),
        name="pick",
    )(asked, packed)
    received = lax.all_to_all(sent, REP, 0, 0, tiled=True)
    return pl.pallas_call(
        functools.partial(far_kernel, size),
        grid=(steps,),
        out_shape=(struct((PAIRS, 8, PD)), struct((PEERS, VEC, PD))),
        in_specs=[
            SMEM,
            whole(PEERS, PD),
            whole(HEAD + FULL, 2 * PD),
            pl.BlockSpec((WIDE, size, PD), lambda r: (r, 0, 0)),
        ],
        out_specs=(
            pl.BlockSpec((WIDE // 2, 8, PD), lambda r: (r, 0, 0)),
            pl.BlockSpec((WIDE, VEC, PD), lambda r: (r, 0, 0)),
        ),
        scratch_shapes=[
            pltpu.VMEM((WIDE, size - HEAD + ANG, PD), F32),
            pltpu.VMEM((WIDE, size - HEAD + ANG, PD), F32),
        ],
        compiler_params=grant(20),
        name="far",
    )(truncation, names, packed, received)


def shards(coefficients, truncation, neighbours, initial):
    groups = lax.axis_size(GRP)
    replicas = lax.axis_size(REP)
    devices = groups * replicas
    which, code, lists, names, requests, coefficients, initial = pl.pallas_call(
        slot_kernel,
        out_shape=(
            struct((1,), jnp.int32),
            struct((NBP, PD), jnp.int32),
            struct((PAIRS, PD)),
            struct((PEERS, PD)),
            struct((PEERS, 8, PD)),
            struct((PD, CW), BF16),
            struct((32, PD)),
        ),
        in_specs=[SMEM, HBM, HBM, HBM],
        out_specs=(SMEM,) + (VMEM,) * 6,
        compiler_params=grant(6),
        scratch_shapes=[
            pltpu.VMEM((NB, PD), jnp.int32),
            pltpu.VMEM((NBP, PD), jnp.int32),
            pltpu.VMEM((2 * PAIRS, NB * PD), BF16),
            pltpu.VMEM((PD, NB * PD), BF16),
            pltpu.SemaphoreType.DMA((3,)),
        ],
        name="slots",
    )(
        truncation,
        *(
            pltpu.with_memory_space_constraint(x, pltpu.HBM)
            for x in (neighbours, coefficients, initial)
        ),
    )
    asked = lax.all_to_all(requests, REP, 0, 0, tiled=True)
    packed, e_own, re_own, im_own = pl.pallas_call(
        local_kernel,
        out_shape=(struct((HEAD + FULL, 2 * PD), BF16),) + (struct((PD, PD)),) * 3,
        in_specs=[SMEM, VMEM, VMEM],
        scratch_shapes=[
            pltpu.VMEM((CW, PD), F32),
            pltpu.VMEM((FULL + ANG, PD), F32),
            pltpu.VMEM((FULL + ANG, PD), F32),
            pltpu.VMEM((ANG, PD, 2 * PD), F32),
        ],
        cost_estimate=pl.CostEstimate(
            flops=20_000_000_000, bytes_accessed=1_000_000, transcendentals=0
        ),
        compiler_params=grant(20),
        name="local",
    )(truncation, coefficients, initial)
    table, slots = lax.switch(
        which[0],
        [functools.partial(exchange, HEAD + size) for size in SIZES],
        truncation, names, asked, packed,
    )
    alignment, weights, degree, current, columns = pl.pallas_call(
        first_kernel,
        out_shape=(
            struct((NB, 2, PD)),
            struct((2, PD, PD)),
            struct((8, PD)),
            struct((32, PD)),
            struct((PEERS, VEC, PD)),
        ),
        in_specs=[VMEM] * 10,
        compiler_params=grant(6),
        scratch_shapes=[pltpu.VMEM((PD, PD), F32)],
        name="first",
    )(
        neighbours, code, lists, table, e_own, re_own, im_own,
        slots, initial, asked,
    )
    columns = lax.all_to_all(columns, REP, 0, 0, tiled=True)
    current, columns = pl.pallas_call(
        middle_kernel,
        out_shape=(struct((32, PD)), struct((PEERS, VEC, PD))),
        compiler_params=grant(6),
        name="middle",
    )(columns, current, weights, degree, table, lists, asked)
    columns = lax.all_to_all(columns, REP, 0, 0, tiled=True)
    current, gram = pl.pallas_call(
        functools.partial(last_kernel, float(PD * devices)),
        out_shape=(struct((32, PD)), struct((devices, 2, PD))),
        compiler_params=grant(6),
        name="last",
    )(columns, current, weights, degree, table, lists)
    grams = lax.all_to_all(gram, GRP_REP, 0, 0, tiled=True)
    vectors = pl.pallas_call(
        finish_kernel,
        out_shape=struct((32, PD)),
        compiler_params=grant(6),
        name="finish",
    )(grams, current)
    return (jnp.transpose(alignment, (1, 0, 2)), vectors)


def solution(mesh):
    split = Mesh(mesh.devices.reshape(4, 2, 4, 4), GRP_REP)
    in_specs = (P(GRP_REP, None), P(), P(None, GRP_REP), P(None, GRP_REP))
    out_specs = (P(None, None, GRP_REP), P(None, GRP_REP))
    return jax.shard_map(
        shards, mesh=split, in_specs=in_specs, out_specs=out_specs, check_vma=False
    )
```

```python
import functools

import jax
import jax.numpy as jnp
from jax import lax
from jax.experimental import pallas as pl
from jax.experimental.pallas import tpu as pltpu
from jax.sharding import Mesh
from jax.sharding import PartitionSpec as P

ANG = 64
RAD = 16
NB = 50
NBP = 56
VEC = 16
PD = 128
CAP = 64
CW = 2048
FULL = RAD * ANG
SIZES = (384, 512, 544, 576, 608, 640, 672, 704, 736, 768, 896, FULL)
HEAD = 2 * VEC
PEERS = 16
PAIRS = PEERS // 2
WIDE = 4
GROUP = 8
GRP = ("grp_0", "grp_1")
REP = ("rep_0", "rep_1")
GRP_REP = ("grp_0", "grp_1", "rep_0", "rep_1")
EPS = 1e-06
F32 = jnp.float32
BF16 = jnp.bfloat16
HIGHEST = lax.Precision.HIGHEST

NT = (((1,), (1,)), ((), ()))
TN = (((0,), (0,)), ((), ()))


def iota(shape, dim):
    return lax.broadcasted_iota(jnp.int32, shape, dim)


def one_hot(cond):
    return jnp.where(cond, 1.0, 0.0).astype(BF16)


def three_parts(x):
    high = x.astype(BF16)
    rest = x - high.astype(F32)
    mid = rest.astype(BF16)
    low = (rest - mid.astype(F32)).astype(BF16)
    return jnp.concatenate([high, mid, low], axis=0)


def two_parts(x):
    high = x.astype(BF16)
    rest = (x - high.astype(F32)).astype(BF16)
    return jnp.concatenate([high, rest], axis=0)


def exact_select(x, selector, dims=(((1,), (0,)), ((), ()))):
    rows = x.shape[0]
    parts = lax.dot_general(three_parts(x), selector, dims, preferred_element_type=F32)
    return parts[:rows] + (parts[rows : 2 * rows] + parts[2 * rows :])


def kept_rows(trunc_ref, rows, lanes):
    row = iota((rows, lanes), 0) % RAD
    kept = jnp.zeros((rows, lanes), jnp.int32)
    for q in range(RAD):
        kept = jnp.where(row == q, trunc_ref[q], kept)
    return kept


def place():
    index = [lax.axis_index(name) for name in GRP_REP]
    size = [lax.axis_size(name) for name in GRP_REP]
    group = index[0] * size[1] + index[1]
    member = index[2] * size[3] + index[3]
    return group * (size[2] * size[3] * PD), member


def slot_kernel(
    trunc_ref, nb_hbm, coef_hbm, init_hbm,
    which_ref, code_ref, lists_ref, names_ref, req_ref, coef_ref, init_ref,
    nb_ref, nbp_ref, a_ref, b_ref, sem_ref,
):
    bring = (
        pltpu.make_async_copy(coef_hbm, coef_ref, sem_ref.at[0]),
        pltpu.make_async_copy(init_hbm, init_ref, sem_ref.at[1]),
    )
    slots = pltpu.make_async_copy(nb_hbm, nb_ref, sem_ref.at[2])
    for copy in (slots,) + bring:
        copy.start()
    total = trunc_ref[0]
    for q in range(1, RAD):
        total = total + trunc_ref[q]
    which = jnp.int32(0)
    for size in SIZES[:-1]:
        which = which + (total > size).astype(jnp.int32)
    which_ref[0] = which
    start, me = place()
    slots.wait()
    nbp_ref[...] = jnp.full((NBP, PD), -1, jnp.int32)
    nbp_ref[:NB, :] = nb_ref[...] - start
    local = nbp_ref[...]
    owner = local >> 7
    within = local & (PD - 1)
    remote = (owner != me) & (local >= 0)
    owner = jnp.where(remote, owner, -1)
    masks = [one_hot(owner == p) for p in range(PEERS)]
    before = one_hot(iota((NBP, NBP), 0) > iota((NBP, NBP), 1))
    in_column = jnp.dot(before, jnp.concatenate(masks, axis=1), preferred_element_type=F32)
    totals = jnp.concatenate(
        [jnp.sum(m.astype(F32), axis=0, keepdims=True) for m in masks], axis=0
    )
    left = one_hot(iota((PD, PD), 0) < iota((PD, PD), 1))
    columns = jnp.dot(totals.astype(BF16), left, preferred_element_type=F32)
    rank = jnp.zeros((NBP, PD), F32)
    for p in range(PEERS):
        here = in_column[:, p * PD : (p + 1) * PD] + columns[p : p + 1, :]
        rank = jnp.where(owner == p, here, rank)
    rank = rank.astype(jnp.int32)
    code = jnp.where(remote, owner * CAP + rank, -1)
    code_ref[...] = code
    pair = code >> 7
    lane = jnp.where(remote, code & (PD - 1), -1)
    particle = iota((1, PD), 1).astype(F32) + 1.0
    rows8 = iota((PAIRS, PD), 0)
    rows128 = iota((PD, PD), 0)
    for n in range(NB):
        mine = rows8 == pair[n : n + 1, :]
        names = within[n : n + 1, :].astype(F32)
        both = jnp.concatenate(
            [jnp.where(mine, names, 0.0), jnp.where(mine, particle, 0.0)], axis=0
        )
        a_ref[:, n * PD : (n + 1) * PD] = both.astype(BF16)
        b_ref[:, n * PD : (n + 1) * PD] = one_hot(rows128 == lane[n : n + 1, :])
    lists = lax.dot_general(a_ref[...], b_ref[...], NT, preferred_element_type=F32)
    lists_ref[...] = lists[PAIRS:]
    turned = pltpu.roll(lists, CAP, 1)
    first = iota((2 * PAIRS, PD), 1) < CAP
    both = (jnp.where(first, lists, turned), jnp.where(first, turned, lists))
    for p in range(PEERS):
        rows = both[p % 2]
        r = p // 2
        req_ref[p] = jnp.broadcast_to(rows[r : r + 1, :], (8, PD))
        names_ref[p : p + 1, :] = rows[PAIRS + r : PAIRS + r + 1, :]
    for copy in bring:
        copy.wait()


def wanted_row(rx_ref, r):
    even = rx_ref[2 * r][:1, :]
    odd = rx_ref[2 * r + 1][:1, :]
    return jnp.where(iota((1, PD), 1) < CAP, even, odd).astype(jnp.int32)


def local_kernel(
    trunc_ref, coef_ref, init_ref, out_ref, e_ref, re_ref, im_ref,
    f_ref, wide_re_ref, wide_im_ref, s_ref,
):
    init = init_ref[...]
    parts = two_parts(jnp.concatenate([init[:VEC], init[VEC:]], axis=1))
    out_ref[:HEAD, :] = parts
    for c in range(CW // PD):
        block = coef_ref[:, c * PD : (c + 1) * PD].astype(F32)
        f_ref[c * PD : (c + 1) * PD, :] = block.T
    offset = 0
    for q in range(RAD):
        here = pl.ds(offset, ANG)
        wide_re_ref[here, :] = f_ref[q * ANG : (q + 1) * ANG, :]
        wide_im_ref[here, :] = f_ref[(RAD + q) * ANG : (RAD + q + 1) * ANG, :]
        offset = offset + trunc_ref[q]
    for b in range(FULL // PD):
        rows = slice(b * PD, (b + 1) * PD)
        to = slice(HEAD + b * PD, HEAD + (b + 1) * PD)
        kept = iota((PD, PD), 0) + b * PD < offset
        out_ref[to, :PD] = jnp.where(kept, wide_re_ref[rows, :], 0.0).astype(BF16)
        out_ref[to, PD:] = jnp.where(kept, wide_im_ref[rows, :], 0.0).astype(BF16)
    own_pairs(trunc_ref, e_ref, re_ref, im_ref, f_ref, s_ref)


def pick_kernel(size, rx_ref, pack_ref, out_ref):
    rows = iota((PD, PD), 0)
    first = iota((PD, PD), 1) < CAP

    def step(r, carry):
        sides = []
        for p in range(WIDE):
            picked = rows == rx_ref[WIDE * r + p][:1, :].astype(jnp.int32)
            top = one_hot(picked & first)
            bottom = one_hot(picked & jnp.logical_not(first))
            sides.append(jnp.concatenate([top, bottom], axis=0))
        side = jnp.concatenate(sides, axis=1)
        chosen = jnp.dot(pack_ref[:size, :], side, preferred_element_type=F32)
        for p in range(WIDE):
            out_ref[WIDE * r + p] = chosen[:, p * PD : (p + 1) * PD].astype(BF16)
        return carry

    lax.fori_loop(0, PEERS // WIDE, step, 0)


def own_pairs(trunc_ref, e_ref, re_ref, im_ref, xt_ref, s_ref):
    kept = kept_rows(trunc_ref, 2 * RAD, PD)
    e_ref[...] = jnp.zeros((PD, PD), F32)
    re_ref[...] = jnp.zeros((PD, PD), F32)
    im_ref[...] = jnp.zeros((PD, PD), F32)

    def sums(first):
        for b in range(PD // 8):
            sub = slice(b * 8, (b + 1) * 8)
            energy = e_ref[sub, :]
            m_re = re_ref[sub, :]
            m_im = im_ref[sub, :]
            before = max(first - 1, 0)
            re = s_ref[before, sub, :PD]
            im = s_ref[before, sub, PD:]
            for k in range(first, first + GROUP):
                if k == 0:
                    energy = energy + re * re
                    continue
                next_re = s_ref[k, sub, :PD]
                next_im = s_ref[k, sub, PD:]
                half_re = 0.5 * next_re
                half_im = 0.5 * next_im
                energy = energy + (half_re * next_re + half_im * next_im)
                if k == 1:
                    m_re = m_re + re * next_re
                    m_im = m_im - re * next_im
                else:
                    m_re = m_re + (re * half_re + im * half_im)
                    m_im = m_im + (im * half_re - re * half_im)
                re, im = next_re, next_im
            e_ref[sub, :] = energy
            re_ref[sub, :] = m_re
            im_ref[sub, :] = m_im

    for first in range(0, ANG, GROUP):
        for k in range(first, first + GROUP):
            rows = xt_ref[pl.ds(k, 2 * RAD, stride=ANG), :]
            masked = rows if k < 16 else jnp.where(kept > k, rows, 0.0)
            turned = jnp.concatenate([masked[RAD:], -masked[:RAD]], axis=0)
            right = jnp.concatenate([masked, turned], axis=1).astype(BF16)
            s_ref[k] = lax.dot_general(
                rows.astype(BF16), right, TN, preferred_element_type=F32
            )
        if first > 0:
            sums(first - GROUP)
    sums(ANG - GROUP)


def far_kernel(
    size, trunc_ref, names_ref, pack_ref, recv_ref, table_ref, cur_ref,
    same_ref, cross_ref,
):
    kept = size - HEAD
    for p in range(WIDE):
        same_ref[p, kept:, :] = jnp.zeros((ANG, PD), F32)
        cross_ref[p, kept:, :] = jnp.zeros((ANG, PD), F32)

    def step(r, carry):
        far_step(
            size, r, trunc_ref, names_ref, pack_ref, recv_ref, table_ref, cur_ref,
            same_ref, cross_ref,
        )
        return carry

    lax.fori_loop(0, PEERS // WIDE, step, 0)


def far_step(
    size, r, trunc_ref, names_ref, pack_ref, recv_ref, table_ref, cur_ref,
    same_ref, cross_ref,
):
    kept = size - HEAD
    first = iota((PD, PD), 1) < CAP
    sides = []
    for p in range(WIDE):
        name = names_ref[pl.ds(WIDE * r + p, 1), :].astype(jnp.int32)
        named = iota((PD, PD), 0) + 1 == name
        low = one_hot(named & first)
        high = one_hot(named & jnp.logical_not(first))
        sides.append(jnp.concatenate([low, high], axis=0))
    mine = jnp.dot(
        pack_ref[HEAD:size, :], jnp.concatenate(sides, axis=1), preferred_element_type=F32
    )
    freq = iota((ANG, PD), 0)
    halves = []
    for p in range(WIDE):
        arrived = recv_ref[WIDE * r + p, HEAD:, :].astype(F32)
        own = mine[:, p * PD : (p + 1) * PD]
        same_ref[p, :kept, :] = own * arrived
        cross_ref[p, :kept, :] = own * pltpu.roll(arrived, CAP, 1)
        parts = recv_ref[WIDE * r + p, :HEAD, :].astype(F32)
        cur_ref[WIDE * r + p] = parts[:VEC] + parts[VEC:]
    for b in range(WIDE // 2):
        both = (2 * b, 2 * b + 1)
        totals = [[jnp.zeros((ANG, PD), F32)] * 2 for _ in both]
        offset = 0
        for q in range(RAD):
            here = pl.ds(offset, ANG)
            inside = freq < trunc_ref[q]
            for p in both:
                for v, ref in enumerate((same_ref, cross_ref)):
                    total = totals[p % 2][v]
                    totals[p % 2][v] = total + jnp.where(inside, ref[p, here, :], 0.0)
            offset = offset + trunc_ref[q]
        halves.extend(totals)
    first = first[:ANG]
    inner = (freq > 0) & (freq < ANG - 1)
    for b in range(WIDE // 2):
        even, odd = halves[2 * b], halves[2 * b + 1]
        s_re = jnp.where(first, even[0], odd[0])
        s_re = s_re + pltpu.roll(jnp.where(first, odd[0], even[0]), CAP, 1)
        s_im = pltpu.roll(jnp.where(first, odd[1], even[1]), CAP, 1)
        s_im = jnp.where(first, s_im - even[1], odd[1] - s_im)
        power = s_re * s_re + s_im * s_im
        next_re = pltpu.roll(s_re, ANG - 1, 0)
        next_im = pltpu.roll(s_im, ANG - 1, 0)
        zero_re = s_re[:1]
        energy = zero_re * zero_re + 0.5 * jnp.sum(
            jnp.where(freq == 0, 0.0, power), axis=0, keepdims=True
        )
        m_re = zero_re * s_re[1:2] + 0.5 * jnp.sum(
            jnp.where(inner, s_re * next_re + s_im * next_im, 0.0), axis=0, keepdims=True
        )
        m_im = 0.5 * jnp.sum(
            jnp.where(inner, s_im * next_re - s_re * next_im, 0.0), axis=0, keepdims=True
        ) - zero_re * s_im[1:2]
        table_ref[WIDE // 2 * r + b] = jnp.concatenate(
            [energy, m_re, m_im, jnp.zeros((5, PD), F32)], axis=0
        )


def near_image(cur, w_re, w_im):
    weights = jnp.concatenate([w_re, w_im], axis=1)
    both = jnp.dot(cur, weights, precision=HIGHEST, preferred_element_type=F32)
    re = both[:VEC, :PD] - both[VEC:, PD:]
    im = both[VEC:, :PD] + both[:VEC, PD:]
    return jnp.concatenate([re, im], axis=0)


def far_image(slots, table_ref, lists_ref):
    values = []
    picks = []
    for r in range(PAIRS):
        m_re = table_ref[r, 1:2, :]
        m_im = table_ref[r, 2:3, :]
        c_re, c_im = slots[r][:VEC], slots[r][VEC:]
        values.append(
            jnp.concatenate([m_re * c_re - m_im * c_im, m_re * c_im + m_im * c_re], axis=0)
        )
        particle = lists_ref[r : r + 1, :].astype(jnp.int32)
        picks.append(one_hot(iota((PD, PD), 0) + 1 == particle))
    return exact_select(
        jnp.concatenate(values, axis=1), jnp.concatenate(picks, axis=1), NT
    )


def send_columns(cur, rx_ref, out_ref):
    picks = [one_hot(iota((PD, PD), 0) == wanted_row(rx_ref, r)) for r in range(PAIRS)]
    columns = exact_select(cur, jnp.concatenate(picks, axis=1))
    first = iota((VEC, PD), 1) < CAP
    for r in range(PAIRS):
        re = columns[:VEC, r * PD : (r + 1) * PD]
        im = columns[VEC:, r * PD : (r + 1) * PD]
        out_ref[2 * r] = jnp.where(first, re, pltpu.roll(im, CAP, 1))
        out_ref[2 * r + 1] = jnp.where(first, pltpu.roll(re, CAP, 1), im)


def received_columns(recv_ref):
    first = iota((VEC, PD), 1) < CAP
    slots = []
    for r in range(PAIRS):
        even = recv_ref[2 * r]
        odd = recv_ref[2 * r + 1]
        re = jnp.where(first, even, pltpu.roll(odd, CAP, 1))
        im = jnp.where(first, pltpu.roll(even, CAP, 1), odd)
        slots.append(jnp.concatenate([re, im], axis=0))
    return slots


def first_kernel(
    nb_ref, code_ref, lists_ref, table_ref, e_ref, re_ref, im_ref,
    slots_ref, init_ref, rx_ref,
    align_ref, weights_ref, degree_ref, cur_ref, send_ref, near_ref,
):
    start, me = place()
    local = nb_ref[...] - start
    near = (local >> 7) == me
    near_ref[...] = jnp.full((PD, PD), -1.0, F32)
    near_ref[:NB, :] = jnp.where(near, local & (PD - 1), -1).astype(F32)
    rows = iota((PD, PD), 0).astype(F32)
    counts = jnp.zeros((PD, PD), F32)
    for n in range(NB):
        counts = counts + jnp.where(rows == near_ref[n : n + 1, :], 1.0, 0.0)
    named = near_ref[...].T.astype(jnp.int32)
    inside = jnp.maximum(named, 0)
    values = []
    for ref, sign in ((e_ref, 1.0), (re_ref, 1.0), (im_ref, -1.0)):
        found = jnp.take_along_axis(ref[...], inside, axis=1, mode="promise_in_bounds")
        values.append(jnp.where(named >= 0, sign * found, 0.0).T[:NBP])
    code = code_ref[...]
    pair = code >> 7
    lane = code & (PD - 1)
    for r in range(PAIRS):
        mine = pair == r
        for v in range(3):
            row = jnp.broadcast_to(table_ref[r, v : v + 1, :], (NBP, PD))
            found = jnp.take_along_axis(row, lane, axis=1, mode="promise_in_bounds")
            values[v] = jnp.where(mine, found, values[v])
    below = values[0] + EPS
    align_ref[:, 0, :] = (values[1] / below)[:NB]
    align_ref[:, 1, :] = (values[2] / below)[:NB]
    degree = EPS + jnp.sum(values[0], axis=0, keepdims=True)
    degree_ref[...] = jnp.broadcast_to(degree, (8, PD))
    w_re = counts * re_ref[...]
    w_im = counts * im_ref[...]
    weights_ref[0] = w_re
    weights_ref[1] = w_im
    slots = received_columns(slots_ref)
    image = near_image(init_ref[...], w_re, w_im) + far_image(slots, table_ref, lists_ref)
    image = image / degree
    cur_ref[...] = image
    send_columns(image, rx_ref, send_ref)


def next_image(recv_ref, cur_ref, weights_ref, degree_ref, table_ref, lists_ref):
    slots = received_columns(recv_ref)
    image = near_image(cur_ref[...], weights_ref[0], weights_ref[1])
    image = image + far_image(slots, table_ref, lists_ref)
    return image / degree_ref[:1, :]


def middle_kernel(
    recv_ref, cur_ref, weights_ref, degree_ref, table_ref, lists_ref, rx_ref,
    out_ref, send_ref,
):
    image = next_image(recv_ref, cur_ref, weights_ref, degree_ref, table_ref, lists_ref)
    out_ref[...] = image
    send_columns(image, rx_ref, send_ref)


def last_kernel(
    total, recv_ref, cur_ref, weights_ref, degree_ref, table_ref, lists_ref,
    out_ref, gram_ref,
):
    image = next_image(recv_ref, cur_ref, weights_ref, degree_ref, table_ref, lists_ref)
    out_ref[...] = image
    gram = lax.dot_general(
        image[:VEC], image[:VEC], NT, precision=HIGHEST, preferred_element_type=F32
    ) + lax.dot_general(
        image[VEC:], image[VEC:], NT, precision=HIGHEST, preferred_element_type=F32
    )
    gram = gram * (1.0 / total)
    wide = jnp.concatenate([gram] * 8, axis=1)
    mine = iota((VEC, PD), 1) // VEC == iota((VEC, PD), 0) % 8
    wide = jnp.where(mine, wide, 0.0)
    packed = jnp.concatenate(
        [
            jnp.sum(wide[:8], axis=0, keepdims=True),
            jnp.sum(wide[8:], axis=0, keepdims=True),
        ],
        axis=0,
    )
    gram_ref[...] = jnp.broadcast_to(packed[None], gram_ref.shape)


def finish_kernel(grams_ref, cur_ref, out_ref):
    packed = jnp.sum(grams_ref[...], axis=0)
    row = iota((VEC, PD), 0)
    lane = iota((VEC, PD), 1)
    wide = jnp.where(row < 8, packed[0:1, :], packed[1:2, :])
    wide = jnp.where(lane // VEC == row % 8, wide, 0.0)
    for shift in (64, 32, 16):
        wide = wide + pltpu.roll(wide, shift, 1)
    columns = [jnp.broadcast_to(wide[:, c : c + 1], (VEC, PD)) for c in range(VEC)]
    re = cur_ref[:VEC, :]
    im = cur_ref[VEC:, :]
    for c in range(VEC):
        pivot = columns[c][c : c + 1, :]
        scale = lax.rsqrt(pivot)
        scale = scale * (1.5 - 0.5 * pivot * scale * scale)
        column = jnp.where(row > c, columns[c] * scale, 0.0)
        for d in range(c + 1, VEC):
            columns[d] = columns[d] - column * (columns[d][c : c + 1, :] * scale)
        top_re = re[c : c + 1, :] * scale
        top_im = im[c : c + 1, :] * scale
        here = row == c
        re = jnp.where(here, top_re, re - column * top_re)
        im = jnp.where(here, top_im, im - column * top_im)
    out_ref[:VEC, :] = re
    out_ref[VEC:, :] = im


def struct(shape, dtype=F32):
    return jax.ShapeDtypeStruct(shape, dtype)


SMEM = pl.BlockSpec(memory_space=pltpu.SMEM)
VMEM = pl.BlockSpec(memory_space=pltpu.VMEM)
HBM = pl.BlockSpec(memory_space=pltpu.HBM)


def grant(mib):
    return pltpu.CompilerParams(vmem_limit_bytes=mib << 20)


def exchange(size, truncation, names, asked, packed):
    sent = pl.pallas_call(
        functools.partial(pick_kernel, size),
        out_shape=struct((PEERS, size, PD), BF16),
        in_specs=[VMEM, VMEM],
        out_specs=VMEM,
        compiler_params=grant(16),
        name="pick",
    )(asked, packed)
    received = lax.all_to_all(sent, REP, 0, 0, tiled=True)
    return pl.pallas_call(
        functools.partial(far_kernel, size),
        out_shape=(struct((PAIRS, 8, PD)), struct((PEERS, VEC, PD))),
        in_specs=[SMEM, VMEM, VMEM, VMEM],
        out_specs=(VMEM, VMEM),
        scratch_shapes=[
            pltpu.VMEM((WIDE, size - HEAD + ANG, PD), F32),
            pltpu.VMEM((WIDE, size - HEAD + ANG, PD), F32),
        ],
        compiler_params=grant(20),
        name="far",
    )(truncation, names, packed, received)


def shards(coefficients, truncation, neighbours, initial):
    groups = lax.axis_size(GRP)
    replicas = lax.axis_size(REP)
    devices = groups * replicas
    which, code, lists, names, requests, coefficients, initial = pl.pallas_call(
        slot_kernel,
        out_shape=(
            struct((1,), jnp.int32),
            struct((NBP, PD), jnp.int32),
            struct((PAIRS, PD)),
            struct((PEERS, PD)),
            struct((PEERS, 8, PD)),
            struct((PD, CW), BF16),
            struct((32, PD)),
        ),
        in_specs=[SMEM, HBM, HBM, HBM],
        out_specs=(SMEM,) + (VMEM,) * 6,
        compiler_params=grant(6),
        scratch_shapes=[
            pltpu.VMEM((NB, PD), jnp.int32),
            pltpu.VMEM((NBP, PD), jnp.int32),
            pltpu.VMEM((2 * PAIRS, NB * PD), BF16),
            pltpu.VMEM((PD, NB * PD), BF16),
            pltpu.SemaphoreType.DMA((3,)),
        ],
        name="slots",
    )(
        truncation,
        *(
            pltpu.with_memory_space_constraint(x, pltpu.HBM)
            for x in (neighbours, coefficients, initial)
        ),
    )
    asked = lax.all_to_all(requests, REP, 0, 0, tiled=True)
    packed, e_own, re_own, im_own = pl.pallas_call(
        local_kernel,
        out_shape=(struct((HEAD + FULL, 2 * PD), BF16),) + (struct((PD, PD)),) * 3,
        in_specs=[SMEM, VMEM, VMEM],
        scratch_shapes=[
            pltpu.VMEM((CW, PD), F32),
            pltpu.VMEM((FULL + ANG, PD), F32),
            pltpu.VMEM((FULL + ANG, PD), F32),
            pltpu.VMEM((ANG, PD, 2 * PD), F32),
        ],
        cost_estimate=pl.CostEstimate(
            flops=20_000_000_000, bytes_accessed=1_000_000, transcendentals=0
        ),
        compiler_params=grant(20),
        name="local",
    )(truncation, coefficients, initial)
    table, slots = lax.switch(
        which[0],
        [functools.partial(exchange, HEAD + size) for size in SIZES],
        truncation, names, asked, packed,
    )
    alignment, weights, degree, current, columns = pl.pallas_call(
        first_kernel,
        out_shape=(
            struct((NB, 2, PD)),
            struct((2, PD, PD)),
            struct((8, PD)),
            struct((32, PD)),
            struct((PEERS, VEC, PD)),
        ),
        in_specs=[VMEM] * 10,
        compiler_params=grant(6),
        scratch_shapes=[pltpu.VMEM((PD, PD), F32)],
        name="first",
    )(
        neighbours, code, lists, table, e_own, re_own, im_own,
        slots, initial, asked,
    )
    columns = lax.all_to_all(columns, REP, 0, 0, tiled=True)
    current, columns = pl.pallas_call(
        middle_kernel,
        out_shape=(struct((32, PD)), struct((PEERS, VEC, PD))),
        compiler_params=grant(6),
        name="middle",
    )(columns, current, weights, degree, table, lists, asked)
    columns = lax.all_to_all(columns, REP, 0, 0, tiled=True)
    current, gram = pl.pallas_call(
        functools.partial(last_kernel, float(PD * devices)),
        out_shape=(struct((32, PD)), struct((devices, 2, PD))),
        compiler_params=grant(6),
        name="last",
    )(columns, current, weights, degree, table, lists)
    grams = lax.all_to_all(gram, GRP_REP, 0, 0, tiled=True)
    vectors = pl.pallas_call(
        finish_kernel,
        out_shape=struct((32, PD)),
        compiler_params=grant(6),
        name="finish",
    )(grams, current)
    return (jnp.transpose(alignment, (1, 0, 2)), vectors)


def solution(mesh):
    split = Mesh(mesh.devices.reshape(4, 2, 4, 4), GRP_REP)
    in_specs = (P(GRP_REP, None), P(), P(None, GRP_REP), P(None, GRP_REP))
    out_specs = (P(None, None, GRP_REP), P(None, GRP_REP))
    return jax.shard_map(
        shards, mesh=split, in_specs=in_specs, out_specs=out_specs, check_vma=False
    )
```

```python
import functools

import jax
import jax.numpy as jnp
from jax import lax
from jax.experimental import pallas as pl
from jax.experimental.pallas import tpu as pltpu
from jax.sharding import Mesh
from jax.sharding import PartitionSpec as P

ANG = 64
RAD = 16
NB = 50
NBP = 56
VEC = 16
PD = 128
CAP = 64
CW = 2048
FULL = RAD * ANG
SIZES = (384, 512, 544, 576, 608, 640, 672, 704, 736, 768, 896, FULL)
HEAD = 2 * VEC
PEERS = 16
PAIRS = PEERS // 2
WIDE = 4
GROUP = 8
GRP = ("grp_0", "grp_1")
REP = ("rep_0", "rep_1")
GRP_REP = ("grp_0", "grp_1", "rep_0", "rep_1")
EPS = 1e-06
F32 = jnp.float32
BF16 = jnp.bfloat16
HIGHEST = lax.Precision.HIGHEST

NT = (((1,), (1,)), ((), ()))
TN = (((0,), (0,)), ((), ()))


def iota(shape, dim):
    return lax.broadcasted_iota(jnp.int32, shape, dim)


def one_hot(cond):
    return jnp.where(cond, 1.0, 0.0).astype(BF16)


def three_parts(x):
    high = x.astype(BF16)
    rest = x - high.astype(F32)
    mid = rest.astype(BF16)
    low = (rest - mid.astype(F32)).astype(BF16)
    return jnp.concatenate([high, mid, low], axis=0)


def two_parts(x):
    high = x.astype(BF16)
    rest = (x - high.astype(F32)).astype(BF16)
    return jnp.concatenate([high, rest], axis=0)


def exact_select(x, selector, dims=(((1,), (0,)), ((), ()))):
    rows = x.shape[0]
    parts = lax.dot_general(three_parts(x), selector, dims, preferred_element_type=F32)
    return parts[:rows] + (parts[rows : 2 * rows] + parts[2 * rows :])


def kept_rows(trunc_ref, rows, lanes):
    row = iota((rows, lanes), 0) % RAD
    kept = jnp.zeros((rows, lanes), jnp.int32)
    for q in range(RAD):
        kept = jnp.where(row == q, trunc_ref[q], kept)
    return kept


def place():
    index = [lax.axis_index(name) for name in GRP_REP]
    size = [lax.axis_size(name) for name in GRP_REP]
    group = index[0] * size[1] + index[1]
    member = index[2] * size[3] + index[3]
    return group * (size[2] * size[3] * PD), member


def slot_kernel(
    trunc_ref, nb_hbm, coef_hbm, init_hbm,
    which_ref, code_ref, lists_ref, names_ref, req_hbm, coef_ref, init_ref,
    nb_ref, nbp_ref, req_ref, a_ref, b_ref, sem_ref,
):
    bring = (
        pltpu.make_async_copy(coef_hbm, coef_ref, sem_ref.at[0]),
        pltpu.make_async_copy(init_hbm, init_ref, sem_ref.at[1]),
    )
    slots = pltpu.make_async_copy(nb_hbm, nb_ref, sem_ref.at[2])
    for copy in (slots,) + bring:
        copy.start()
    total = trunc_ref[0]
    for q in range(1, RAD):
        total = total + trunc_ref[q]
    which = jnp.int32(0)
    for size in SIZES[:-1]:
        which = which + (total > size).astype(jnp.int32)
    which_ref[0] = which
    start, me = place()
    slots.wait()
    nbp_ref[...] = jnp.full((NBP, PD), -1, jnp.int32)
    nbp_ref[:NB, :] = nb_ref[...] - start
    local = nbp_ref[...]
    owner = local >> 7
    within = local & (PD - 1)
    remote = (owner != me) & (local >= 0)
    owner = jnp.where(remote, owner, -1)
    masks = [one_hot(owner == p) for p in range(PEERS)]
    before = one_hot(iota((NBP, NBP), 0) > iota((NBP, NBP), 1))
    in_column = jnp.dot(before, jnp.concatenate(masks, axis=1), preferred_element_type=F32)
    totals = jnp.concatenate(
        [jnp.sum(m.astype(F32), axis=0, keepdims=True) for m in masks], axis=0
    )
    left = one_hot(iota((PD, PD), 0) < iota((PD, PD), 1))
    columns = jnp.dot(totals.astype(BF16), left, preferred_element_type=F32)
    rank = jnp.zeros((NBP, PD), F32)
    for p in range(PEERS):
        here = in_column[:, p * PD : (p + 1) * PD] + columns[p : p + 1, :]
        rank = jnp.where(owner == p, here, rank)
    rank = rank.astype(jnp.int32)
    code = jnp.where(remote, owner * CAP + rank, -1)
    pair = code >> 7
    lane = jnp.where(remote, code & (PD - 1), -1)
    particle = iota((1, PD), 1).astype(F32) + 1.0
    rows8 = iota((PAIRS, PD), 0)
    rows128 = iota((PD, PD), 0)
    for n in range(NB):
        mine = rows8 == pair[n : n + 1, :]
        names = within[n : n + 1, :].astype(F32)
        both = jnp.concatenate(
            [jnp.where(mine, names, 0.0), jnp.where(mine, particle, 0.0)], axis=0
        )
        a_ref[:, n * PD : (n + 1) * PD] = both.astype(BF16)
        b_ref[:, n * PD : (n + 1) * PD] = one_hot(rows128 == lane[n : n + 1, :])
    lists = lax.dot_general(a_ref[...], b_ref[...], NT, preferred_element_type=F32)
    turned = pltpu.roll(lists, CAP, 1)
    first = iota((2 * PAIRS, PD), 1) < CAP
    both = (jnp.where(first, lists, turned), jnp.where(first, turned, lists))
    for p in range(PEERS):
        r = p // 2
        req_ref[p] = jnp.broadcast_to(both[p % 2][r : r + 1, :], (8, PD))
    asking = pltpu.make_async_copy(req_ref, req_hbm, sem_ref.at[3])
    asking.start()
    lists_ref[...] = lists[PAIRS:]
    code_ref[...] = code
    for p in range(PEERS):
        r = p // 2
        names_ref[p : p + 1, :] = both[p % 2][PAIRS + r : PAIRS + r + 1, :]
    for copy in bring + (asking,):
        copy.wait()


def wanted_row(rx_ref, r):
    even = rx_ref[2 * r][:1, :]
    odd = rx_ref[2 * r + 1][:1, :]
    return jnp.where(iota((1, PD), 1) < CAP, even, odd).astype(jnp.int32)


def local_kernel(
    trunc_ref, coef_ref, init_ref, out_ref, e_ref, re_ref, im_ref,
    f_ref, wide_re_ref, wide_im_ref, s_ref,
):
    init = init_ref[...]
    parts = two_parts(jnp.concatenate([init[:VEC], init[VEC:]], axis=1))
    out_ref[:HEAD, :] = parts
    for c in range(CW // PD):
        block = coef_ref[:, c * PD : (c + 1) * PD].astype(F32)
        f_ref[c * PD : (c + 1) * PD, :] = block.T
    offset = 0
    for q in range(RAD):
        here = pl.ds(offset, ANG)
        wide_re_ref[here, :] = f_ref[q * ANG : (q + 1) * ANG, :]
        wide_im_ref[here, :] = f_ref[(RAD + q) * ANG : (RAD + q + 1) * ANG, :]
        offset = offset + trunc_ref[q]
    for b in range(FULL // PD):
        rows = slice(b * PD, (b + 1) * PD)
        to = slice(HEAD + b * PD, HEAD + (b + 1) * PD)
        kept = iota((PD, PD), 0) + b * PD < offset
        out_ref[to, :PD] = jnp.where(kept, wide_re_ref[rows, :], 0.0).astype(BF16)
        out_ref[to, PD:] = jnp.where(kept, wide_im_ref[rows, :], 0.0).astype(BF16)
    own_pairs(trunc_ref, e_ref, re_ref, im_ref, f_ref, s_ref)


def pick_kernel(size, rx_ref, pack_ref, out_ref):
    rows = iota((PD, PD), 0)
    first = iota((PD, PD), 1) < CAP

    def step(r, carry):
        sides = []
        for p in range(WIDE):
            picked = rows == rx_ref[WIDE * r + p][:1, :].astype(jnp.int32)
            top = one_hot(picked & first)
            bottom = one_hot(picked & jnp.logical_not(first))
            sides.append(jnp.concatenate([top, bottom], axis=0))
        side = jnp.concatenate(sides, axis=1)
        chosen = jnp.dot(pack_ref[:size, :], side, preferred_element_type=F32)
        for p in range(WIDE):
            out_ref[WIDE * r + p] = chosen[:, p * PD : (p + 1) * PD].astype(BF16)
        return carry

    lax.fori_loop(0, PEERS // WIDE, step, 0)


def own_pairs(trunc_ref, e_ref, re_ref, im_ref, xt_ref, s_ref):
    kept = kept_rows(trunc_ref, 2 * RAD, PD)
    e_ref[...] = jnp.zeros((PD, PD), F32)
    re_ref[...] = jnp.zeros((PD, PD), F32)
    im_ref[...] = jnp.zeros((PD, PD), F32)

    def sums(first):
        for b in range(PD // 8):
            sub = slice(b * 8, (b + 1) * 8)
            energy = e_ref[sub, :]
            m_re = re_ref[sub, :]
            m_im = im_ref[sub, :]
            before = max(first - 1, 0)
            re = s_ref[before, sub, :PD]
            im = s_ref[before, sub, PD:]
            for k in range(first, first + GROUP):
                if k == 0:
                    energy = energy + re * re
                    continue
                next_re = s_ref[k, sub, :PD]
                next_im = s_ref[k, sub, PD:]
                half_re = 0.5 * next_re
                half_im = 0.5 * next_im
                energy = energy + (half_re * next_re + half_im * next_im)
                if k == 1:
                    m_re = m_re + re * next_re
                    m_im = m_im - re * next_im
                else:
                    m_re = m_re + (re * half_re + im * half_im)
                    m_im = m_im + (im * half_re - re * half_im)
                re, im = next_re, next_im
            e_ref[sub, :] = energy
            re_ref[sub, :] = m_re
            im_ref[sub, :] = m_im

    for first in range(0, ANG, GROUP):
        for k in range(first, first + GROUP):
            rows = xt_ref[pl.ds(k, 2 * RAD, stride=ANG), :]
            masked = rows if k < 16 else jnp.where(kept > k, rows, 0.0)
            turned = jnp.concatenate([masked[RAD:], -masked[:RAD]], axis=0)
            right = jnp.concatenate([masked, turned], axis=1).astype(BF16)
            s_ref[k] = lax.dot_general(
                rows.astype(BF16), right, TN, preferred_element_type=F32
            )
        if first > 0:
            sums(first - GROUP)
    sums(ANG - GROUP)


def far_kernel(
    size, trunc_ref, names_ref, pack_ref, recv_ref, table_ref, cur_ref,
    same_ref, cross_ref,
):
    kept = size - HEAD
    for b in range(WIDE // 2):
        same_ref[b, kept:, :] = jnp.zeros((ANG, PD), F32)
        cross_ref[b, kept:, :] = jnp.zeros((ANG, PD), F32)

    def step(r, carry):
        far_step(
            size, r, trunc_ref, names_ref, pack_ref, recv_ref, table_ref, cur_ref,
            same_ref, cross_ref,
        )
        return carry

    lax.fori_loop(0, PEERS // WIDE, step, 0)


def far_step(
    size, r, trunc_ref, names_ref, pack_ref, recv_ref, table_ref, cur_ref,
    same_ref, cross_ref,
):
    kept = size - HEAD
    first = iota((1, PD), 1) < CAP
    picks = []
    for b in range(WIDE // 2):
        even = names_ref[pl.ds(WIDE * r + 2 * b, 1), :]
        odd = names_ref[pl.ds(WIDE * r + 2 * b + 1, 1), :]
        name = jnp.where(first, even, odd).astype(jnp.int32)
        picks.append(one_hot(iota((PD, PD), 0) + 1 == name))
    pick = jnp.concatenate(picks, axis=1)
    mine_re = jnp.dot(pack_ref[HEAD:size, :PD], pick, preferred_element_type=F32)
    mine_im = jnp.dot(pack_ref[HEAD:size, PD:], pick, preferred_element_type=F32)
    for p in range(WIDE):
        parts = recv_ref[WIDE * r + p, :HEAD, :].astype(F32)
        cur_ref[WIDE * r + p] = parts[:VEC] + parts[VEC:]
    for b in range(WIDE // 2):
        even = recv_ref[WIDE * r + 2 * b, HEAD:, :].astype(F32)
        odd = recv_ref[WIDE * r + 2 * b + 1, HEAD:, :].astype(F32)
        b_re = jnp.where(first, even, pltpu.roll(odd, CAP, 1))
        b_im = jnp.where(first, pltpu.roll(even, CAP, 1), odd)
        a_re = mine_re[:, b * PD : (b + 1) * PD]
        a_im = mine_im[:, b * PD : (b + 1) * PD]
        same_ref[b, :kept, :] = a_re * b_re + a_im * b_im
        cross_ref[b, :kept, :] = a_im * b_re - a_re * b_im
    freq = iota((ANG, PD), 0)
    totals = [[jnp.zeros((ANG, PD), F32)] * 2 for _ in range(WIDE // 2)]
    offset = 0
    for q in range(RAD):
        here = pl.ds(offset, ANG)
        inside = freq < trunc_ref[q]
        for b in range(WIDE // 2):
            for v, ref in enumerate((same_ref, cross_ref)):
                totals[b][v] = totals[b][v] + jnp.where(inside, ref[b, here, :], 0.0)
        offset = offset + trunc_ref[q]
    inner = (freq > 0) & (freq < ANG - 1)
    for b in range(WIDE // 2):
        s_re, s_im = totals[b]
        power = s_re * s_re + s_im * s_im
        next_re = pltpu.roll(s_re, ANG - 1, 0)
        next_im = pltpu.roll(s_im, ANG - 1, 0)
        zero_re = s_re[:1]
        energy = zero_re * zero_re + 0.5 * jnp.sum(
            jnp.where(freq == 0, 0.0, power), axis=0, keepdims=True
        )
        m_re = zero_re * s_re[1:2] + 0.5 * jnp.sum(
            jnp.where(inner, s_re * next_re + s_im * next_im, 0.0), axis=0, keepdims=True
        )
        m_im = 0.5 * jnp.sum(
            jnp.where(inner, s_im * next_re - s_re * next_im, 0.0), axis=0, keepdims=True
        ) - zero_re * s_im[1:2]
        table_ref[WIDE // 2 * r + b] = jnp.concatenate(
            [energy, m_re, m_im, jnp.zeros((5, PD), F32)], axis=0
        )


def near_image(cur, w_re, w_im):
    weights = jnp.concatenate([w_re, w_im], axis=1)
    both = jnp.dot(cur, weights, precision=HIGHEST, preferred_element_type=F32)
    re = both[:VEC, :PD] - both[VEC:, PD:]
    im = both[VEC:, :PD] + both[:VEC, PD:]
    return jnp.concatenate([re, im], axis=0)


def far_image(slots, table_ref, lists_ref):
    values = []
    picks = []
    for r in range(PAIRS):
        m_re = table_ref[r, 1:2, :]
        m_im = table_ref[r, 2:3, :]
        c_re, c_im = slots[r][:VEC], slots[r][VEC:]
        values.append(
            jnp.concatenate([m_re * c_re - m_im * c_im, m_re * c_im + m_im * c_re], axis=0)
        )
        particle = lists_ref[r : r + 1, :].astype(jnp.int32)
        picks.append(one_hot(iota((PD, PD), 0) + 1 == particle))
    return exact_select(
        jnp.concatenate(values, axis=1), jnp.concatenate(picks, axis=1), NT
    )


def send_columns(cur, rx_ref, out_ref):
    picks = [one_hot(iota((PD, PD), 0) == wanted_row(rx_ref, r)) for r in range(PAIRS)]
    columns = exact_select(cur, jnp.concatenate(picks, axis=1))
    first = iota((VEC, PD), 1) < CAP
    for r in range(PAIRS):
        re = columns[:VEC, r * PD : (r + 1) * PD]
        im = columns[VEC:, r * PD : (r + 1) * PD]
        out_ref[2 * r] = jnp.where(first, re, pltpu.roll(im, CAP, 1))
        out_ref[2 * r + 1] = jnp.where(first, pltpu.roll(re, CAP, 1), im)


def received_columns(recv_ref):
    first = iota((VEC, PD), 1) < CAP
    slots = []
    for r in range(PAIRS):
        even = recv_ref[2 * r]
        odd = recv_ref[2 * r + 1]
        re = jnp.where(first, even, pltpu.roll(odd, CAP, 1))
        im = jnp.where(first, pltpu.roll(even, CAP, 1), odd)
        slots.append(jnp.concatenate([re, im], axis=0))
    return slots


def first_kernel(
    nb_ref, code_ref, lists_ref, table_ref, e_ref, re_ref, im_ref,
    slots_ref, init_ref, rx_ref,
    align_hbm, weights_ref, degree_ref, cur_ref, send_ref,
    near_ref, align_ref, sem_ref,
):
    start, me = place()
    local = nb_ref[...] - start
    near = (local >> 7) == me
    near_ref[...] = jnp.full((PD, PD), -1.0, F32)
    near_ref[:NB, :] = jnp.where(near, local & (PD - 1), -1).astype(F32)
    rows = iota((PD, PD), 0).astype(F32)
    counts = jnp.zeros((PD, PD), F32)
    for n in range(NB):
        counts = counts + jnp.where(rows == near_ref[n : n + 1, :], 1.0, 0.0)
    named = near_ref[...].T.astype(jnp.int32)
    inside = jnp.maximum(named, 0)
    values = []
    for ref, sign in ((e_ref, 1.0), (re_ref, 1.0), (im_ref, -1.0)):
        found = jnp.take_along_axis(ref[...], inside, axis=1, mode="promise_in_bounds")
        values.append(jnp.where(named >= 0, sign * found, 0.0).T[:NBP])
    code = code_ref[...]
    pair = code >> 7
    lane = code & (PD - 1)
    for r in range(PAIRS):
        mine = pair == r
        for v in range(3):
            row = jnp.broadcast_to(table_ref[r, v : v + 1, :], (NBP, PD))
            found = jnp.take_along_axis(row, lane, axis=1, mode="promise_in_bounds")
            values[v] = jnp.where(mine, found, values[v])
    below = values[0] + EPS
    align_ref[:, 0, :] = (values[1] / below)[:NB]
    align_ref[:, 1, :] = (values[2] / below)[:NB]
    leaving = pltpu.make_async_copy(align_ref, align_hbm, sem_ref.at[0])
    leaving.start()
    degree = EPS + jnp.sum(values[0], axis=0, keepdims=True)
    degree_ref[...] = jnp.broadcast_to(degree, (8, PD))
    w_re = counts * re_ref[...]
    w_im = counts * im_ref[...]
    weights_ref[0] = w_re
    weights_ref[1] = w_im
    slots = received_columns(slots_ref)
    image = near_image(init_ref[...], w_re, w_im) + far_image(slots, table_ref, lists_ref)
    image = image / degree
    cur_ref[...] = image
    send_columns(image, rx_ref, send_ref)
    leaving.wait()


def next_image(recv_ref, cur_ref, weights_ref, degree_ref, table_ref, lists_ref):
    slots = received_columns(recv_ref)
    image = near_image(cur_ref[...], weights_ref[0], weights_ref[1])
    image = image + far_image(slots, table_ref, lists_ref)
    return image / degree_ref[:1, :]


def middle_kernel(
    recv_ref, cur_ref, weights_ref, degree_ref, table_ref, lists_ref, rx_ref,
    out_ref, send_ref,
):
    image = next_image(recv_ref, cur_ref, weights_ref, degree_ref, table_ref, lists_ref)
    out_ref[...] = image
    send_columns(image, rx_ref, send_ref)


def last_kernel(
    total, recv_ref, cur_ref, weights_ref, degree_ref, table_ref, lists_ref,
    out_ref, gram_ref,
):
    image = next_image(recv_ref, cur_ref, weights_ref, degree_ref, table_ref, lists_ref)
    out_ref[...] = image
    gram = lax.dot_general(
        image[:VEC], image[:VEC], NT, precision=HIGHEST, preferred_element_type=F32
    ) + lax.dot_general(
        image[VEC:], image[VEC:], NT, precision=HIGHEST, preferred_element_type=F32
    )
    gram = gram * (1.0 / total)
    wide = jnp.concatenate([gram] * 8, axis=1)
    mine = iota((VEC, PD), 1) // VEC == iota((VEC, PD), 0) % 8
    wide = jnp.where(mine, wide, 0.0)
    packed = jnp.concatenate(
        [
            jnp.sum(wide[:8], axis=0, keepdims=True),
            jnp.sum(wide[8:], axis=0, keepdims=True),
        ],
        axis=0,
    )
    gram_ref[...] = jnp.broadcast_to(packed[None], gram_ref.shape)


def finish_kernel(grams_ref, cur_ref, out_ref):
    packed = jnp.sum(grams_ref[...], axis=0)
    row = iota((VEC, PD), 0)
    lane = iota((VEC, PD), 1)
    wide = jnp.where(row < 8, packed[0:1, :], packed[1:2, :])
    wide = jnp.where(lane // VEC == row % 8, wide, 0.0)
    for shift in (64, 32, 16):
        wide = wide + pltpu.roll(wide, shift, 1)
    columns = [jnp.broadcast_to(wide[:, c : c + 1], (VEC, PD)) for c in range(VEC)]
    re = cur_ref[:VEC, :]
    im = cur_ref[VEC:, :]
    for c in range(VEC):
        pivot = columns[c][c : c + 1, :]
        scale = lax.rsqrt(pivot)
        scale = scale * (1.5 - 0.5 * pivot * scale * scale)
        column = jnp.where(row > c, columns[c] * scale, 0.0)
        for d in range(c + 1, VEC):
            columns[d] = columns[d] - column * (columns[d][c : c + 1, :] * scale)
        top_re = re[c : c + 1, :] * scale
        top_im = im[c : c + 1, :] * scale
        here = row == c
        re = jnp.where(here, top_re, re - column * top_re)
        im = jnp.where(here, top_im, im - column * top_im)
    out_ref[:VEC, :] = re
    out_ref[VEC:, :] = im


def struct(shape, dtype=F32):
    return jax.ShapeDtypeStruct(shape, dtype)


SMEM = pl.BlockSpec(memory_space=pltpu.SMEM)
VMEM = pl.BlockSpec(memory_space=pltpu.VMEM)
HBM = pl.BlockSpec(memory_space=pltpu.HBM)


def grant(mib):
    return pltpu.CompilerParams(vmem_limit_bytes=mib << 20)


def exchange(size, truncation, names, asked, packed):
    sent = pl.pallas_call(
        functools.partial(pick_kernel, size),
        out_shape=struct((PEERS, size, PD), BF16),
        in_specs=[VMEM, VMEM],
        out_specs=VMEM,
        compiler_params=grant(16),
        name="pick",
    )(asked, packed)
    received = lax.all_to_all(sent, REP, 0, 0, tiled=True)
    return pl.pallas_call(
        functools.partial(far_kernel, size),
        out_shape=(struct((PAIRS, 8, PD)), struct((PEERS, VEC, PD))),
        in_specs=[SMEM, VMEM, VMEM, VMEM],
        out_specs=(VMEM, VMEM),
        scratch_shapes=[
            pltpu.VMEM((WIDE // 2, size - HEAD + ANG, PD), F32),
            pltpu.VMEM((WIDE // 2, size - HEAD + ANG, PD), F32),
        ],
        compiler_params=grant(20),
        name="far",
    )(truncation, names, packed, received)


def shards(coefficients, truncation, neighbours, initial):
    groups = lax.axis_size(GRP)
    replicas = lax.axis_size(REP)
    devices = groups * replicas
    which, code, lists, names, requests, coefficients, initial = pl.pallas_call(
        slot_kernel,
        out_shape=(
            struct((1,), jnp.int32),
            struct((NBP, PD), jnp.int32),
            struct((PAIRS, PD)),
            struct((PEERS, PD)),
            struct((PEERS, 8, PD)),
            struct((PD, CW), BF16),
            struct((32, PD)),
        ),
        in_specs=[SMEM, HBM, HBM, HBM],
        out_specs=(SMEM, VMEM, VMEM, VMEM, HBM, VMEM, VMEM),
        compiler_params=grant(6),
        scratch_shapes=[
            pltpu.VMEM((NB, PD), jnp.int32),
            pltpu.VMEM((NBP, PD), jnp.int32),
            pltpu.VMEM((PEERS, 8, PD), F32),
            pltpu.VMEM((2 * PAIRS, NB * PD), BF16),
            pltpu.VMEM((PD, NB * PD), BF16),
            pltpu.SemaphoreType.DMA((4,)),
        ],
        name="slots",
    )(
        truncation,
        *(
            pltpu.with_memory_space_constraint(x, pltpu.HBM)
            for x in (neighbours, coefficients, initial)
        ),
    )
    asked = lax.all_to_all(requests, REP, 0, 0, tiled=True)
    packed, e_own, re_own, im_own = pl.pallas_call(
        local_kernel,
        out_shape=(struct((HEAD + FULL, 2 * PD), BF16),) + (struct((PD, PD)),) * 3,
        in_specs=[SMEM, VMEM, VMEM],
        scratch_shapes=[
            pltpu.VMEM((CW, PD), F32),
            pltpu.VMEM((FULL + ANG, PD), F32),
            pltpu.VMEM((FULL + ANG, PD), F32),
            pltpu.VMEM((ANG, PD, 2 * PD), F32),
        ],
        cost_estimate=pl.CostEstimate(
            flops=20_000_000_000, bytes_accessed=1_000_000, transcendentals=0
        ),
        compiler_params=grant(20),
        name="local",
    )(truncation, coefficients, initial)
    table, slots = lax.switch(
        which[0],
        [functools.partial(exchange, HEAD + size) for size in SIZES],
        truncation, names, asked, packed,
    )
    alignment, weights, degree, current, columns = pl.pallas_call(
        first_kernel,
        out_shape=(
            struct((NB, 2, PD)),
            struct((2, PD, PD)),
            struct((8, PD)),
            struct((32, PD)),
            struct((PEERS, VEC, PD)),
        ),
        in_specs=[VMEM] * 10,
        compiler_params=grant(6),
        out_specs=(HBM, VMEM, VMEM, VMEM, VMEM),
        scratch_shapes=[
            pltpu.VMEM((PD, PD), F32),
            pltpu.VMEM((NB, 2, PD), F32),
            pltpu.SemaphoreType.DMA((1,)),
        ],
        name="first",
    )(
        neighbours, code, lists, table, e_own, re_own, im_own,
        slots, initial, asked,
    )
    columns = lax.all_to_all(columns, REP, 0, 0, tiled=True)
    current, columns = pl.pallas_call(
        middle_kernel,
        out_shape=(struct((32, PD)), struct((PEERS, VEC, PD))),
        compiler_params=grant(6),
        name="middle",
    )(columns, current, weights, degree, table, lists, asked)
    columns = lax.all_to_all(columns, REP, 0, 0, tiled=True)
    current, gram = pl.pallas_call(
        functools.partial(last_kernel, float(PD * devices)),
        out_shape=(struct((32, PD)), struct((devices, 2, PD))),
        compiler_params=grant(6),
        name="last",
    )(columns, current, weights, degree, table, lists)
    grams = lax.all_to_all(gram, GRP_REP, 0, 0, tiled=True)
    vectors = pl.pallas_call(
        finish_kernel,
        out_shape=struct((32, PD)),
        compiler_params=grant(6),
        name="finish",
    )(grams, current)
    return (jnp.transpose(alignment, (1, 0, 2)), vectors)


def solution(mesh):
    split = Mesh(mesh.devices.reshape(4, 2, 4, 4), GRP_REP)
    in_specs = (P(GRP_REP, None), P(), P(None, GRP_REP), P(None, GRP_REP))
    out_specs = (P(None, None, GRP_REP), P(None, GRP_REP))
    return jax.shard_map(
        shards, mesh=split, in_specs=in_specs, out_specs=out_specs, check_vma=False
    )
```

```python
import functools

import jax
import jax.numpy as jnp
from jax import lax
from jax.experimental import pallas as pl
from jax.experimental.pallas import tpu as pltpu
from jax.sharding import Mesh
from jax.sharding import PartitionSpec as P

ANG = 64
RAD = 16
NB = 50
NBP = 56
VEC = 16
PD = 128
CAP = 64
CW = 2048
FULL = RAD * ANG
SIZES = (384, 512, 544, 576, 608, 640, 672, 704, 736, 768, 896, FULL)
HEAD = 2 * VEC
PEERS = 16
PAIRS = PEERS // 2
WIDE = 4
GROUP = 8
GRP = ("grp_0", "grp_1")
REP = ("rep_0", "rep_1")
GRP_REP = ("grp_0", "grp_1", "rep_0", "rep_1")
EPS = 1e-06
F32 = jnp.float32
BF16 = jnp.bfloat16
HIGHEST = lax.Precision.HIGHEST

NT = (((1,), (1,)), ((), ()))
TN = (((0,), (0,)), ((), ()))


def iota(shape, dim):
    return lax.broadcasted_iota(jnp.int32, shape, dim)


def one_hot(cond):
    return jnp.where(cond, 1.0, 0.0).astype(BF16)


def three_parts(x):
    high = x.astype(BF16)
    rest = x - high.astype(F32)
    mid = rest.astype(BF16)
    low = (rest - mid.astype(F32)).astype(BF16)
    return jnp.concatenate([high, mid, low], axis=0)


def two_parts(x):
    high = x.astype(BF16)
    rest = (x - high.astype(F32)).astype(BF16)
    return jnp.concatenate([high, rest], axis=0)


def exact_select(x, selector, dims=(((1,), (0,)), ((), ()))):
    rows = x.shape[0]
    parts = lax.dot_general(three_parts(x), selector, dims, preferred_element_type=F32)
    return parts[:rows] + (parts[rows : 2 * rows] + parts[2 * rows :])


def kept_rows(trunc_ref, rows, lanes):
    row = iota((rows, lanes), 0) % RAD
    kept = jnp.zeros((rows, lanes), jnp.int32)
    for q in range(RAD):
        kept = jnp.where(row == q, trunc_ref[q], kept)
    return kept


def place():
    index = [lax.axis_index(name) for name in GRP_REP]
    size = [lax.axis_size(name) for name in GRP_REP]
    group = index[0] * size[1] + index[1]
    member = index[2] * size[3] + index[3]
    return group * (size[2] * size[3] * PD), member


def slot_kernel(
    trunc_ref, nb_hbm, coef_hbm, init_hbm,
    which_ref, code_ref, lists_ref, names_ref, req_ref, coef_ref, init_ref,
    nb_ref, nbp_ref, a_ref, b_ref, sem_ref,
):
    bring = (
        pltpu.make_async_copy(coef_hbm, coef_ref, sem_ref.at[0]),
        pltpu.make_async_copy(init_hbm, init_ref, sem_ref.at[1]),
    )
    slots = pltpu.make_async_copy(nb_hbm, nb_ref, sem_ref.at[2])
    for copy in (slots,) + bring:
        copy.start()
    total = trunc_ref[0]
    for q in range(1, RAD):
        total = total + trunc_ref[q]
    which = jnp.int32(0)
    for size in SIZES[:-1]:
        which = which + (total > size).astype(jnp.int32)
    which_ref[0] = which
    start, me = place()
    slots.wait()
    nbp_ref[...] = jnp.full((NBP, PD), -1, jnp.int32)
    nbp_ref[:NB, :] = nb_ref[...] - start
    local = nbp_ref[...]
    owner = local >> 7
    within = local & (PD - 1)
    remote = (owner != me) & (local >= 0)
    owner = jnp.where(remote, owner, -1)
    masks = [one_hot(owner == p) for p in range(PEERS)]
    before = one_hot(iota((NBP, NBP), 0) > iota((NBP, NBP), 1))
    in_column = jnp.dot(before, jnp.concatenate(masks, axis=1), preferred_element_type=F32)
    totals = jnp.concatenate(
        [jnp.sum(m.astype(F32), axis=0, keepdims=True) for m in masks], axis=0
    )
    left = one_hot(iota((PD, PD), 0) < iota((PD, PD), 1))
    columns = jnp.dot(totals.astype(BF16), left, preferred_element_type=F32)
    rank = jnp.zeros((NBP, PD), F32)
    for p in range(PEERS):
        here = in_column[:, p * PD : (p + 1) * PD] + columns[p : p + 1, :]
        rank = jnp.where(owner == p, here, rank)
    rank = rank.astype(jnp.int32)
    code = jnp.where(remote, owner * CAP + rank, -1)
    pair = code >> 7
    lane = jnp.where(remote, code & (PD - 1), -1)
    particle = iota((1, PD), 1).astype(F32) + 1.0
    rows8 = iota((PAIRS, PD), 0)
    rows128 = iota((PD, PD), 0)
    for n in range(NB):
        mine = rows8 == pair[n : n + 1, :]
        names = within[n : n + 1, :].astype(F32)
        both = jnp.concatenate(
            [jnp.where(mine, names, 0.0), jnp.where(mine, particle, 0.0)], axis=0
        )
        a_ref[:, n * PD : (n + 1) * PD] = both.astype(BF16)
        b_ref[:, n * PD : (n + 1) * PD] = one_hot(rows128 == lane[n : n + 1, :])
    lists = lax.dot_general(a_ref[...], b_ref[...], NT, preferred_element_type=F32)
    turned = pltpu.roll(lists, CAP, 1)
    first = iota((2 * PAIRS, PD), 1) < CAP
    both = (jnp.where(first, lists, turned), jnp.where(first, turned, lists))
    for p in range(PEERS):
        r = p // 2
        req_ref[p] = both[p % 2][r : r + 1, :]
    lists_ref[...] = lists[PAIRS:]
    code_ref[...] = code
    for p in range(PEERS):
        r = p // 2
        names_ref[p : p + 1, :] = both[p % 2][PAIRS + r : PAIRS + r + 1, :]
    for copy in bring:
        copy.wait()


def wanted_row(rx_ref, r):
    even = rx_ref[2 * r]
    odd = rx_ref[2 * r + 1]
    return jnp.where(iota((1, PD), 1) < CAP, even, odd).astype(jnp.int32)


def local_kernel(
    trunc_ref, coef_ref, init_ref, out_ref, e_ref, re_ref, im_ref,
    f_ref, wide_re_ref, wide_im_ref, s_ref,
):
    init = init_ref[...]
    parts = two_parts(jnp.concatenate([init[:VEC], init[VEC:]], axis=1))
    out_ref[:HEAD, :] = parts
    for c in range(CW // PD):
        block = coef_ref[:, c * PD : (c + 1) * PD].astype(F32)
        f_ref[c * PD : (c + 1) * PD, :] = block.T
    offset = 0
    for q in range(RAD):
        here = pl.ds(offset, ANG)
        wide_re_ref[here, :] = f_ref[q * ANG : (q + 1) * ANG, :]
        wide_im_ref[here, :] = f_ref[(RAD + q) * ANG : (RAD + q + 1) * ANG, :]
        offset = offset + trunc_ref[q]
    for b in range(FULL // PD):
        rows = slice(b * PD, (b + 1) * PD)
        to = slice(HEAD + b * PD, HEAD + (b + 1) * PD)
        kept = iota((PD, PD), 0) + b * PD < offset
        out_ref[to, :PD] = jnp.where(kept, wide_re_ref[rows, :], 0.0).astype(BF16)
        out_ref[to, PD:] = jnp.where(kept, wide_im_ref[rows, :], 0.0).astype(BF16)
    own_pairs(trunc_ref, e_ref, re_ref, im_ref, f_ref, s_ref)


def pick_kernel(size, rx_ref, pack_ref, out_ref):
    rows = iota((PD, PD), 0)
    first = iota((PD, PD), 1) < CAP

    def step(r, carry):
        sides = []
        for p in range(WIDE):
            picked = rows == rx_ref[WIDE * r + p].astype(jnp.int32)
            top = one_hot(picked & first)
            bottom = one_hot(picked & jnp.logical_not(first))
            sides.append(jnp.concatenate([top, bottom], axis=0))
        side = jnp.concatenate(sides, axis=1)
        chosen = jnp.dot(pack_ref[:size, :], side, preferred_element_type=F32)
        for p in range(WIDE):
            out_ref[WIDE * r + p] = chosen[:, p * PD : (p + 1) * PD].astype(BF16)
        return carry

    lax.fori_loop(0, PEERS // WIDE, step, 0)


def own_pairs(trunc_ref, e_ref, re_ref, im_ref, xt_ref, s_ref):
    kept = kept_rows(trunc_ref, 2 * RAD, PD)
    e_ref[...] = jnp.zeros((PD, PD), F32)
    re_ref[...] = jnp.zeros((PD, PD), F32)
    im_ref[...] = jnp.zeros((PD, PD), F32)

    def sums(first):
        for b in range(PD // 8):
            sub = slice(b * 8, (b + 1) * 8)
            energy = e_ref[sub, :]
            m_re = re_ref[sub, :]
            m_im = im_ref[sub, :]
            before = max(first - 1, 0)
            re = s_ref[before, sub, :PD]
            im = s_ref[before, sub, PD:]
            for k in range(first, first + GROUP):
                if k == 0:
                    energy = energy + re * re
                    continue
                next_re = s_ref[k, sub, :PD]
                next_im = s_ref[k, sub, PD:]
                half_re = 0.5 * next_re
                half_im = 0.5 * next_im
                energy = energy + (half_re * next_re + half_im * next_im)
                if k == 1:
                    m_re = m_re + re * next_re
                    m_im = m_im - re * next_im
                else:
                    m_re = m_re + (re * half_re + im * half_im)
                    m_im = m_im + (im * half_re - re * half_im)
                re, im = next_re, next_im
            e_ref[sub, :] = energy
            re_ref[sub, :] = m_re
            im_ref[sub, :] = m_im

    for first in range(0, ANG, GROUP):
        for k in range(first, first + GROUP):
            rows = xt_ref[pl.ds(k, 2 * RAD, stride=ANG), :]
            masked = rows if k < 16 else jnp.where(kept > k, rows, 0.0)
            turned = jnp.concatenate([masked[RAD:], -masked[:RAD]], axis=0)
            right = jnp.concatenate([masked, turned], axis=1).astype(BF16)
            s_ref[k] = lax.dot_general(
                rows.astype(BF16), right, TN, preferred_element_type=F32
            )
        if first > 0:
            sums(first - GROUP)
    sums(ANG - GROUP)


def far_kernel(
    size, trunc_ref, names_ref, pack_ref, recv_ref, table_ref, cur_ref,
    same_ref, cross_ref,
):
    kept = size - HEAD
    for b in range(WIDE // 2):
        same_ref[b, kept:, :] = jnp.zeros((ANG, PD), F32)
        cross_ref[b, kept:, :] = jnp.zeros((ANG, PD), F32)

    def step(r, carry):
        far_step(
            size, r, trunc_ref, names_ref, pack_ref, recv_ref, table_ref, cur_ref,
            same_ref, cross_ref,
        )
        return carry

    lax.fori_loop(0, PEERS // WIDE, step, 0)


def far_step(
    size, r, trunc_ref, names_ref, pack_ref, recv_ref, table_ref, cur_ref,
    same_ref, cross_ref,
):
    kept = size - HEAD
    first = iota((1, PD), 1) < CAP
    picks = []
    for b in range(WIDE // 2):
        even = names_ref[pl.ds(WIDE * r + 2 * b, 1), :]
        odd = names_ref[pl.ds(WIDE * r + 2 * b + 1, 1), :]
        name = jnp.where(first, even, odd).astype(jnp.int32)
        picks.append(one_hot(iota((PD, PD), 0) + 1 == name))
    pick = jnp.concatenate(picks, axis=1)
    mine_re = jnp.dot(pack_ref[HEAD:size, :PD], pick, preferred_element_type=F32)
    mine_im = jnp.dot(pack_ref[HEAD:size, PD:], pick, preferred_element_type=F32)
    for p in range(WIDE):
        parts = recv_ref[WIDE * r + p, :HEAD, :].astype(F32)
        cur_ref[WIDE * r + p] = parts[:VEC] + parts[VEC:]
    for b in range(WIDE // 2):
        even = recv_ref[WIDE * r + 2 * b, HEAD:, :].astype(F32)
        odd = recv_ref[WIDE * r + 2 * b + 1, HEAD:, :].astype(F32)
        b_re = jnp.where(first, even, pltpu.roll(odd, CAP, 1))
        b_im = jnp.where(first, pltpu.roll(even, CAP, 1), odd)
        a_re = mine_re[:, b * PD : (b + 1) * PD]
        a_im = mine_im[:, b * PD : (b + 1) * PD]
        same_ref[b, :kept, :] = a_re * b_re + a_im * b_im
        cross_ref[b, :kept, :] = a_im * b_re - a_re * b_im
    freq = iota((ANG, PD), 0)
    totals = [[jnp.zeros((ANG, PD), F32)] * 2 for _ in range(WIDE // 2)]
    offset = 0
    for q in range(RAD):
        here = pl.ds(offset, ANG)
        inside = freq < trunc_ref[q]
        for b in range(WIDE // 2):
            for v, ref in enumerate((same_ref, cross_ref)):
                totals[b][v] = totals[b][v] + jnp.where(inside, ref[b, here, :], 0.0)
        offset = offset + trunc_ref[q]
    inner = (freq > 0) & (freq < ANG - 1)
    for b in range(WIDE // 2):
        s_re, s_im = totals[b]
        power = s_re * s_re + s_im * s_im
        next_re = pltpu.roll(s_re, ANG - 1, 0)
        next_im = pltpu.roll(s_im, ANG - 1, 0)
        zero_re = s_re[:1]
        energy = zero_re * zero_re + 0.5 * jnp.sum(
            jnp.where(freq == 0, 0.0, power), axis=0, keepdims=True
        )
        m_re = zero_re * s_re[1:2] + 0.5 * jnp.sum(
            jnp.where(inner, s_re * next_re + s_im * next_im, 0.0), axis=0, keepdims=True
        )
        m_im = 0.5 * jnp.sum(
            jnp.where(inner, s_im * next_re - s_re * next_im, 0.0), axis=0, keepdims=True
        ) - zero_re * s_im[1:2]
        table_ref[WIDE // 2 * r + b] = jnp.concatenate(
            [energy, m_re, m_im, jnp.zeros((5, PD), F32)], axis=0
        )


def near_image(cur, w_re, w_im):
    weights = jnp.concatenate([w_re, w_im], axis=1)
    both = jnp.dot(cur, weights, precision=HIGHEST, preferred_element_type=F32)
    re = both[:VEC, :PD] - both[VEC:, PD:]
    im = both[VEC:, :PD] + both[:VEC, PD:]
    return jnp.concatenate([re, im], axis=0)


def far_image(slots, table_ref, lists_ref):
    values = []
    picks = []
    for r in range(PAIRS):
        m_re = table_ref[r, 1:2, :]
        m_im = table_ref[r, 2:3, :]
        c_re, c_im = slots[r][:VEC], slots[r][VEC:]
        values.append(
            jnp.concatenate([m_re * c_re - m_im * c_im, m_re * c_im + m_im * c_re], axis=0)
        )
        particle = lists_ref[r : r + 1, :].astype(jnp.int32)
        picks.append(one_hot(iota((PD, PD), 0) + 1 == particle))
    return exact_select(
        jnp.concatenate(values, axis=1), jnp.concatenate(picks, axis=1), NT
    )


def send_columns(cur, rx_ref, out_ref):
    picks = [one_hot(iota((PD, PD), 0) == wanted_row(rx_ref, r)) for r in range(PAIRS)]
    columns = exact_select(cur, jnp.concatenate(picks, axis=1))
    first = iota((VEC, PD), 1) < CAP
    for r in range(PAIRS):
        re = columns[:VEC, r * PD : (r + 1) * PD]
        im = columns[VEC:, r * PD : (r + 1) * PD]
        out_ref[2 * r] = jnp.where(first, re, pltpu.roll(im, CAP, 1))
        out_ref[2 * r + 1] = jnp.where(first, pltpu.roll(re, CAP, 1), im)


def received_columns(recv_ref):
    first = iota((VEC, PD), 1) < CAP
    slots = []
    for r in range(PAIRS):
        even = recv_ref[2 * r]
        odd = recv_ref[2 * r + 1]
        re = jnp.where(first, even, pltpu.roll(odd, CAP, 1))
        im = jnp.where(first, pltpu.roll(even, CAP, 1), odd)
        slots.append(jnp.concatenate([re, im], axis=0))
    return slots


def first_kernel(
    nb_ref, code_ref, lists_ref, table_ref, e_ref, re_ref, im_ref,
    slots_ref, init_ref, rx_ref,
    align_hbm, weights_ref, degree_ref, cur_ref, send_ref,
    near_ref, align_ref, sem_ref,
):
    start, me = place()
    local = nb_ref[...] - start
    near = (local >> 7) == me
    near_ref[...] = jnp.full((PD, PD), -1.0, F32)
    near_ref[:NB, :] = jnp.where(near, local & (PD - 1), -1).astype(F32)
    rows = iota((PD, PD), 0).astype(F32)
    counts = jnp.zeros((PD, PD), F32)
    for n in range(NB):
        counts = counts + jnp.where(rows == near_ref[n : n + 1, :], 1.0, 0.0)
    named = near_ref[...].T.astype(jnp.int32)
    inside = jnp.maximum(named, 0)
    values = []
    for ref, sign in ((e_ref, 1.0), (re_ref, 1.0), (im_ref, -1.0)):
        found = jnp.take_along_axis(ref[...], inside, axis=1, mode="promise_in_bounds")
        values.append(jnp.where(named >= 0, sign * found, 0.0).T[:NBP])
    code = code_ref[...]
    pair = code >> 7
    lane = code & (PD - 1)
    for r in range(PAIRS):
        mine = pair == r
        for v in range(3):
            row = jnp.broadcast_to(table_ref[r, v : v + 1, :], (NBP, PD))
            found = jnp.take_along_axis(row, lane, axis=1, mode="promise_in_bounds")
            values[v] = jnp.where(mine, found, values[v])
    below = values[0] + EPS
    align_ref[:, 0, :] = (values[1] / below)[:NB]
    align_ref[:, 1, :] = (values[2] / below)[:NB]
    leaving = pltpu.make_async_copy(align_ref, align_hbm, sem_ref.at[0])
    leaving.start()
    degree = EPS + jnp.sum(values[0], axis=0, keepdims=True)
    degree_ref[...] = jnp.broadcast_to(degree, (8, PD))
    w_re = counts * re_ref[...]
    w_im = counts * im_ref[...]
    weights_ref[0] = w_re
    weights_ref[1] = w_im
    slots = received_columns(slots_ref)
    image = near_image(init_ref[...], w_re, w_im) + far_image(slots, table_ref, lists_ref)
    image = image / degree
    cur_ref[...] = image
    send_columns(image, rx_ref, send_ref)
    leaving.wait()


def next_image(recv_ref, cur_ref, weights_ref, degree_ref, table_ref, lists_ref):
    slots = received_columns(recv_ref)
    image = near_image(cur_ref[...], weights_ref[0], weights_ref[1])
    image = image + far_image(slots, table_ref, lists_ref)
    return image / degree_ref[:1, :]


def middle_kernel(
    recv_ref, cur_ref, weights_ref, degree_ref, table_ref, lists_ref, rx_ref,
    out_ref, send_ref,
):
    image = next_image(recv_ref, cur_ref, weights_ref, degree_ref, table_ref, lists_ref)
    out_ref[...] = image
    send_columns(image, rx_ref, send_ref)


def last_kernel(
    total, recv_ref, cur_ref, weights_ref, degree_ref, table_ref, lists_ref,
    out_ref, gram_ref,
):
    image = next_image(recv_ref, cur_ref, weights_ref, degree_ref, table_ref, lists_ref)
    out_ref[...] = image
    gram = lax.dot_general(
        image[:VEC], image[:VEC], NT, precision=HIGHEST, preferred_element_type=F32
    ) + lax.dot_general(
        image[VEC:], image[VEC:], NT, precision=HIGHEST, preferred_element_type=F32
    )
    gram = gram * (1.0 / total)
    wide = jnp.concatenate([gram] * 8, axis=1)
    mine = iota((VEC, PD), 1) // VEC == iota((VEC, PD), 0) % 8
    wide = jnp.where(mine, wide, 0.0)
    packed = jnp.concatenate(
        [
            jnp.sum(wide[:8], axis=0, keepdims=True),
            jnp.sum(wide[8:], axis=0, keepdims=True),
        ],
        axis=0,
    )
    gram_ref[...] = jnp.broadcast_to(packed[None], gram_ref.shape)


def finish_kernel(grams_ref, cur_ref, out_ref):
    packed = jnp.sum(grams_ref[...], axis=0)
    row = iota((VEC, PD), 0)
    lane = iota((VEC, PD), 1)
    wide = jnp.where(row < 8, packed[0:1, :], packed[1:2, :])
    wide = jnp.where(lane // VEC == row % 8, wide, 0.0)
    for shift in (64, 32, 16):
        wide = wide + pltpu.roll(wide, shift, 1)
    columns = [jnp.broadcast_to(wide[:, c : c + 1], (VEC, PD)) for c in range(VEC)]
    re = cur_ref[:VEC, :]
    im = cur_ref[VEC:, :]
    for c in range(VEC):
        pivot = columns[c][c : c + 1, :]
        scale = lax.rsqrt(pivot)
        scale = scale * (1.5 - 0.5 * pivot * scale * scale)
        column = jnp.where(row > c, columns[c] * scale, 0.0)
        for d in range(c + 1, VEC):
            columns[d] = columns[d] - column * (columns[d][c : c + 1, :] * scale)
        top_re = re[c : c + 1, :] * scale
        top_im = im[c : c + 1, :] * scale
        here = row == c
        re = jnp.where(here, top_re, re - column * top_re)
        im = jnp.where(here, top_im, im - column * top_im)
    out_ref[:VEC, :] = re
    out_ref[VEC:, :] = im


def struct(shape, dtype=F32):
    return jax.ShapeDtypeStruct(shape, dtype)


SMEM = pl.BlockSpec(memory_space=pltpu.SMEM)
VMEM = pl.BlockSpec(memory_space=pltpu.VMEM)
HBM = pl.BlockSpec(memory_space=pltpu.HBM)


def grant(mib):
    return pltpu.CompilerParams(vmem_limit_bytes=mib << 20)


def exchange(size, truncation, names, asked, packed):
    sent = pl.pallas_call(
        functools.partial(pick_kernel, size),
        out_shape=struct((PEERS, size, PD), BF16),
        in_specs=[VMEM, VMEM],
        out_specs=VMEM,
        compiler_params=grant(16),
        name="pick",
    )(asked, packed)
    received = lax.all_to_all(sent, REP, 0, 0, tiled=True)
    return pl.pallas_call(
        functools.partial(far_kernel, size),
        out_shape=(struct((PAIRS, 8, PD)), struct((PEERS, VEC, PD))),
        in_specs=[SMEM, VMEM, VMEM, VMEM],
        out_specs=(VMEM, VMEM),
        scratch_shapes=[
            pltpu.VMEM((WIDE // 2, size - HEAD + ANG, PD), F32),
            pltpu.VMEM((WIDE // 2, size - HEAD + ANG, PD), F32),
        ],
        compiler_params=grant(20),
        name="far",
    )(truncation, names, packed, received)


def shards(coefficients, truncation, neighbours, initial):
    groups = lax.axis_size(GRP)
    replicas = lax.axis_size(REP)
    devices = groups * replicas
    which, code, lists, names, requests, coefficients, initial = pl.pallas_call(
        slot_kernel,
        out_shape=(
            struct((1,), jnp.int32),
            struct((NBP, PD), jnp.int32),
            struct((PAIRS, PD)),
            struct((PEERS, PD)),
            struct((PEERS, 1, PD)),
            struct((PD, CW), BF16),
            struct((32, PD)),
        ),
        in_specs=[SMEM, HBM, HBM, HBM],
        out_specs=(SMEM,) + (VMEM,) * 6,
        compiler_params=grant(6),
        scratch_shapes=[
            pltpu.VMEM((NB, PD), jnp.int32),
            pltpu.VMEM((NBP, PD), jnp.int32),
            pltpu.VMEM((2 * PAIRS, NB * PD), BF16),
            pltpu.VMEM((PD, NB * PD), BF16),
            pltpu.SemaphoreType.DMA((3,)),
        ],
        name="slots",
    )(
        truncation,
        *(
            pltpu.with_memory_space_constraint(x, pltpu.HBM)
            for x in (neighbours, coefficients, initial)
        ),
    )
    asked = lax.all_to_all(requests, REP, 0, 0, tiled=True)
    packed, e_own, re_own, im_own = pl.pallas_call(
        local_kernel,
        out_shape=(struct((HEAD + FULL, 2 * PD), BF16),) + (struct((PD, PD)),) * 3,
        in_specs=[SMEM, VMEM, VMEM],
        scratch_shapes=[
            pltpu.VMEM((CW, PD), F32),
            pltpu.VMEM((FULL + ANG, PD), F32),
            pltpu.VMEM((FULL + ANG, PD), F32),
            pltpu.VMEM((ANG, PD, 2 * PD), F32),
        ],
        cost_estimate=pl.CostEstimate(
            flops=20_000_000_000, bytes_accessed=1_000_000, transcendentals=0
        ),
        compiler_params=grant(20),
        name="local",
    )(truncation, coefficients, initial)
    table, slots = lax.switch(
        which[0],
        [functools.partial(exchange, HEAD + size) for size in SIZES],
        truncation, names, asked, packed,
    )
    alignment, weights, degree, current, columns = pl.pallas_call(
        first_kernel,
        out_shape=(
            struct((NB, 2, PD)),
            struct((2, PD, PD)),
            struct((8, PD)),
            struct((32, PD)),
            struct((PEERS, VEC, PD)),
        ),
        in_specs=[VMEM] * 10,
        compiler_params=grant(6),
        out_specs=(HBM, VMEM, VMEM, VMEM, VMEM),
        scratch_shapes=[
            pltpu.VMEM((PD, PD), F32),
            pltpu.VMEM((NB, 2, PD), F32),
            pltpu.SemaphoreType.DMA((1,)),
        ],
        name="first",
    )(
        neighbours, code, lists, table, e_own, re_own, im_own,
        slots, initial, asked,
    )
    columns = lax.all_to_all(columns, REP, 0, 0, tiled=True)
    current, columns = pl.pallas_call(
        middle_kernel,
        out_shape=(struct((32, PD)), struct((PEERS, VEC, PD))),
        compiler_params=grant(6),
        name="middle",
    )(columns, current, weights, degree, table, lists, asked)
    columns = lax.all_to_all(columns, REP, 0, 0, tiled=True)
    current, gram = pl.pallas_call(
        functools.partial(last_kernel, float(PD * devices)),
        out_shape=(struct((32, PD)), struct((devices, 2, PD))),
        compiler_params=grant(6),
        name="last",
    )(columns, current, weights, degree, table, lists)
    grams = lax.all_to_all(gram, GRP_REP, 0, 0, tiled=True)
    vectors = pl.pallas_call(
        finish_kernel,
        out_shape=struct((32, PD)),
        compiler_params=grant(6),
        name="finish",
    )(grams, current)
    return (jnp.transpose(alignment, (1, 0, 2)), vectors)


def solution(mesh):
    split = Mesh(mesh.devices.reshape(4, 2, 4, 4), GRP_REP)
    in_specs = (P(GRP_REP, None), P(), P(None, GRP_REP), P(None, GRP_REP))
    out_specs = (P(None, None, GRP_REP), P(None, GRP_REP))
    return jax.shard_map(
        shards, mesh=split, in_specs=in_specs, out_specs=out_specs, check_vma=False
    )
```

```python
import functools

import jax
import jax.numpy as jnp
from jax import lax
from jax.experimental import pallas as pl
from jax.experimental.pallas import tpu as pltpu
from jax.sharding import Mesh
from jax.sharding import PartitionSpec as P

ANG = 64
RAD = 16
NB = 50
NBP = 56
VEC = 16
PD = 128
CAP = 64
CW = 2048
FULL = RAD * ANG
SIZES = (
    384, 512, 544, 576, 592, 608, 624, 640, 656, 672, 688, 704, 736, 768, 896, FULL
)
HEAD = 2 * VEC
PEERS = 16
PAIRS = PEERS // 2
WIDE = 4
GROUP = 8
ALWAYS = 16
GRP = ("grp_0", "grp_1")
REP = ("rep_0", "rep_1")
GRP_REP = ("grp_0", "grp_1", "rep_0", "rep_1")
EPS = 1e-06
F32 = jnp.float32
BF16 = jnp.bfloat16
HIGHEST = lax.Precision.HIGHEST

NT = (((1,), (1,)), ((), ()))
TN = (((0,), (0,)), ((), ()))


def iota(shape, dim):
    return lax.broadcasted_iota(jnp.int32, shape, dim)


def one_hot(cond):
    return jnp.where(cond, 1.0, 0.0).astype(BF16)


def three_parts(x):
    high = x.astype(BF16)
    rest = x - high.astype(F32)
    mid = rest.astype(BF16)
    low = (rest - mid.astype(F32)).astype(BF16)
    return jnp.concatenate([high, mid, low], axis=0)


def two_parts(x):
    high = x.astype(BF16)
    rest = (x - high.astype(F32)).astype(BF16)
    return jnp.concatenate([high, rest], axis=0)


def exact_select(x, selector, dims=(((1,), (0,)), ((), ()))):
    rows = x.shape[0]
    parts = lax.dot_general(three_parts(x), selector, dims, preferred_element_type=F32)
    return parts[:rows] + (parts[rows : 2 * rows] + parts[2 * rows :])


def kept_rows(trunc_ref, rows, lanes):
    row = iota((rows, lanes), 0) % RAD
    kept = jnp.zeros((rows, lanes), jnp.int32)
    for q in range(RAD):
        kept = jnp.where(row == q, trunc_ref[q], kept)
    return kept


def place():
    index = [lax.axis_index(name) for name in GRP_REP]
    size = [lax.axis_size(name) for name in GRP_REP]
    group = index[0] * size[1] + index[1]
    member = index[2] * size[3] + index[3]
    return group * (size[2] * size[3] * PD), member


def slot_kernel(
    trunc_ref, nb_hbm, coef_hbm, init_hbm,
    which_ref, code_ref, lists_ref, names_ref, req_ref, coef_ref, init_ref,
    nb_ref, nbp_ref, a_ref, b_ref, sem_ref,
):
    bring = (
        pltpu.make_async_copy(coef_hbm, coef_ref, sem_ref.at[0]),
        pltpu.make_async_copy(init_hbm, init_ref, sem_ref.at[1]),
    )
    slots = pltpu.make_async_copy(nb_hbm, nb_ref, sem_ref.at[2])
    for copy in (slots,) + bring:
        copy.start()
    total = trunc_ref[0]
    for q in range(1, RAD):
        total = total + trunc_ref[q]
    which = jnp.int32(0)
    for size in SIZES[:-1]:
        which = which + (total > size).astype(jnp.int32)
    which_ref[0] = which
    start, me = place()
    slots.wait()
    nbp_ref[...] = jnp.full((NBP, PD), -1, jnp.int32)
    nbp_ref[:NB, :] = nb_ref[...] - start
    local = nbp_ref[...]
    owner = local >> 7
    within = local & (PD - 1)
    remote = (owner != me) & (local >= 0)
    owner = jnp.where(remote, owner, -1)
    masks = [one_hot(owner == p) for p in range(PEERS)]
    before = one_hot(iota((NBP, NBP), 0) > iota((NBP, NBP), 1))
    in_column = jnp.dot(before, jnp.concatenate(masks, axis=1), preferred_element_type=F32)
    totals = jnp.concatenate(
        [jnp.sum(m.astype(F32), axis=0, keepdims=True) for m in masks], axis=0
    )
    left = one_hot(iota((PD, PD), 0) < iota((PD, PD), 1))
    columns = jnp.dot(totals.astype(BF16), left, preferred_element_type=F32)
    rank = jnp.zeros((NBP, PD), F32)
    for p in range(PEERS):
        here = in_column[:, p * PD : (p + 1) * PD] + columns[p : p + 1, :]
        rank = jnp.where(owner == p, here, rank)
    rank = rank.astype(jnp.int32)
    code = jnp.where(remote, owner * CAP + rank, -1)
    place_in_list = jnp.where(remote, rank, -1)
    particle = iota((1, PD), 1).astype(F32) + 1.0
    peer = iota((PEERS, PD), 0)
    target = iota((CAP, PD), 0)
    for n in range(NB):
        mine = peer == owner[n : n + 1, :]
        names = within[n : n + 1, :].astype(F32)
        both = jnp.concatenate(
            [jnp.where(mine, names, 0.0), jnp.where(mine, particle, 0.0)], axis=0
        )
        a_ref[:, n * PD : (n + 1) * PD] = both.astype(BF16)
        b_ref[:, n * PD : (n + 1) * PD] = one_hot(target == place_in_list[n : n + 1, :])
    lists = lax.dot_general(a_ref[...], b_ref[...], NT, preferred_element_type=F32)
    lists = jnp.concatenate([lists, lists], axis=1)
    for p in range(PEERS):
        req_ref[p] = lists[p : p + 1, :]
    names_ref[...] = lists[PEERS:]
    first = iota((1, PD), 1) < CAP
    for r in range(PAIRS):
        even = lists[PEERS + 2 * r : PEERS + 2 * r + 1, :]
        odd = lists[PEERS + 2 * r + 1 : PEERS + 2 * r + 2, :]
        lists_ref[r : r + 1, :] = jnp.where(first, even, odd)
    code_ref[...] = code
    for copy in bring:
        copy.wait()


def wanted_row(rx_ref, r):
    even = rx_ref[2 * r]
    odd = rx_ref[2 * r + 1]
    return jnp.where(iota((1, PD), 1) < CAP, even, odd).astype(jnp.int32)


def local_kernel(
    trunc_ref, coef_ref, init_ref, out_ref, e_ref, re_ref, im_ref,
    f_ref, wide_re_ref, wide_im_ref, s_ref,
):
    init = init_ref[...]
    parts = two_parts(jnp.concatenate([init[:VEC], init[VEC:]], axis=1))
    out_ref[:HEAD, :] = parts
    for c in range(CW // PD):
        block = coef_ref[:, c * PD : (c + 1) * PD].astype(F32)
        f_ref[c * PD : (c + 1) * PD, :] = block.T
    offset = 0
    for q in range(RAD):
        here = pl.ds(offset, ANG)
        wide_re_ref[here, :] = f_ref[q * ANG : (q + 1) * ANG, :]
        wide_im_ref[here, :] = f_ref[(RAD + q) * ANG : (RAD + q + 1) * ANG, :]
        offset = offset + trunc_ref[q]
    for b in range(FULL // PD):
        rows = slice(b * PD, (b + 1) * PD)
        to = slice(HEAD + b * PD, HEAD + (b + 1) * PD)
        kept = iota((PD, PD), 0) + b * PD < offset
        out_ref[to, :PD] = jnp.where(kept, wide_re_ref[rows, :], 0.0).astype(BF16)
        out_ref[to, PD:] = jnp.where(kept, wide_im_ref[rows, :], 0.0).astype(BF16)
    own_pairs(trunc_ref, e_ref, re_ref, im_ref, f_ref, s_ref)


def pick_kernel(size, rx_ref, pack_ref, out_ref):
    rows = iota((PD, PD), 0)
    first = iota((PD, PD), 1) < CAP

    def step(r, carry):
        sides = []
        for p in range(WIDE):
            picked = rows == rx_ref[WIDE * r + p].astype(jnp.int32)
            top = one_hot(picked & first)
            bottom = one_hot(picked & jnp.logical_not(first))
            sides.append(jnp.concatenate([top, bottom], axis=0))
        side = jnp.concatenate(sides, axis=1)
        chosen = jnp.dot(pack_ref[:size, :], side, preferred_element_type=F32)
        for p in range(WIDE):
            out_ref[WIDE * r + p] = chosen[:, p * PD : (p + 1) * PD].astype(BF16)
        return carry

    lax.fori_loop(0, PEERS // WIDE, step, 0)


def own_pairs(trunc_ref, e_ref, re_ref, im_ref, xt_ref, s_ref):
    kept = kept_rows(trunc_ref, 2 * RAD, PD)
    e_ref[...] = jnp.zeros((PD, PD), F32)
    re_ref[...] = jnp.zeros((PD, PD), F32)
    im_ref[...] = jnp.zeros((PD, PD), F32)

    def sums(first):
        for b in range(PD // 8):
            sub = slice(b * 8, (b + 1) * 8)
            energy = e_ref[sub, :]
            m_re = re_ref[sub, :]
            m_im = im_ref[sub, :]
            before = max(first - 1, 0)
            re = s_ref[before, sub, :PD]
            im = s_ref[before, sub, PD:]
            for k in range(first, first + GROUP):
                if k == 0:
                    energy = energy + re * re
                    continue
                next_re = s_ref[k, sub, :PD]
                next_im = s_ref[k, sub, PD:]
                half_re = 0.5 * next_re
                half_im = 0.5 * next_im
                energy = energy + (half_re * next_re + half_im * next_im)
                if k == 1:
                    m_re = m_re + re * next_re
                    m_im = m_im - re * next_im
                else:
                    m_re = m_re + (re * half_re + im * half_im)
                    m_im = m_im + (im * half_re - re * half_im)
                re, im = next_re, next_im
            e_ref[sub, :] = energy
            re_ref[sub, :] = m_re
            im_ref[sub, :] = m_im

    for first in range(0, ANG, GROUP):
        for k in range(first, first + GROUP):
            rows = xt_ref[pl.ds(k, 2 * RAD, stride=ANG), :]
            masked = rows if k < ALWAYS else jnp.where(kept > k, rows, 0.0)
            turned = jnp.concatenate([masked[RAD:], -masked[:RAD]], axis=0)
            right = jnp.concatenate([masked, turned], axis=1).astype(BF16)
            s_ref[k] = lax.dot_general(
                rows.astype(BF16), right, TN, preferred_element_type=F32
            )
        if first > 0:
            sums(first - GROUP)
    sums(ANG - GROUP)


def far_kernel(
    size, trunc_ref, names_ref, pack_ref, recv_ref, table_ref, cur_ref,
    same_ref, cross_ref,
):
    kept = size - HEAD
    for b in range(WIDE // 2):
        same_ref[b, kept:, :] = jnp.zeros((ANG, PD), F32)
        cross_ref[b, kept:, :] = jnp.zeros((ANG, PD), F32)

    def step(r, carry):
        far_step(
            size, r, trunc_ref, names_ref, pack_ref, recv_ref, table_ref, cur_ref,
            same_ref, cross_ref,
        )
        return carry

    lax.fori_loop(0, PEERS // WIDE, step, 0)


def far_step(
    size, r, trunc_ref, names_ref, pack_ref, recv_ref, table_ref, cur_ref,
    same_ref, cross_ref,
):
    kept = size - HEAD
    first = iota((1, PD), 1) < CAP
    picks = []
    for b in range(WIDE // 2):
        even = names_ref[pl.ds(WIDE * r + 2 * b, 1), :]
        odd = names_ref[pl.ds(WIDE * r + 2 * b + 1, 1), :]
        name = jnp.where(first, even, odd).astype(jnp.int32)
        picks.append(one_hot(iota((PD, PD), 0) + 1 == name))
    pick = jnp.concatenate(picks, axis=1)
    mine_re = jnp.dot(pack_ref[HEAD:size, :PD], pick, preferred_element_type=F32)
    mine_im = jnp.dot(pack_ref[HEAD:size, PD:], pick, preferred_element_type=F32)
    for p in range(WIDE):
        parts = recv_ref[WIDE * r + p, :HEAD, :].astype(F32)
        cur_ref[WIDE * r + p] = parts[:VEC] + parts[VEC:]
    for b in range(WIDE // 2):
        even = recv_ref[WIDE * r + 2 * b, HEAD:, :].astype(F32)
        odd = recv_ref[WIDE * r + 2 * b + 1, HEAD:, :].astype(F32)
        b_re = jnp.where(first, even, pltpu.roll(odd, CAP, 1))
        b_im = jnp.where(first, pltpu.roll(even, CAP, 1), odd)
        a_re = mine_re[:, b * PD : (b + 1) * PD]
        a_im = mine_im[:, b * PD : (b + 1) * PD]
        same_ref[b, :kept, :] = a_re * b_re + a_im * b_im
        cross_ref[b, :kept, :] = a_im * b_re - a_re * b_im
    freq = iota((ANG, PD), 0)
    totals = [[jnp.zeros((ANG, PD), F32)] * 2 for _ in range(WIDE // 2)]
    offset = 0
    for q in range(RAD):
        here = pl.ds(offset, ANG)
        inside = freq[ALWAYS:] < trunc_ref[q]
        for b in range(WIDE // 2):
            for v, ref in enumerate((same_ref, cross_ref)):
                window = ref[b, here, :]
                window = jnp.concatenate(
                    [window[:ALWAYS], jnp.where(inside, window[ALWAYS:], 0.0)], axis=0
                )
                totals[b][v] = totals[b][v] + window
        offset = offset + trunc_ref[q]
    inner = (freq > 0) & (freq < ANG - 1)
    for b in range(WIDE // 2):
        s_re, s_im = totals[b]
        power = s_re * s_re + s_im * s_im
        next_re = pltpu.roll(s_re, ANG - 1, 0)
        next_im = pltpu.roll(s_im, ANG - 1, 0)
        zero_re = s_re[:1]
        energy = zero_re * zero_re + 0.5 * jnp.sum(
            jnp.where(freq == 0, 0.0, power), axis=0, keepdims=True
        )
        m_re = zero_re * s_re[1:2] + 0.5 * jnp.sum(
            jnp.where(inner, s_re * next_re + s_im * next_im, 0.0), axis=0, keepdims=True
        )
        m_im = 0.5 * jnp.sum(
            jnp.where(inner, s_im * next_re - s_re * next_im, 0.0), axis=0, keepdims=True
        ) - zero_re * s_im[1:2]
        table_ref[WIDE // 2 * r + b] = jnp.concatenate(
            [energy, m_re, m_im, jnp.zeros((5, PD), F32)], axis=0
        )


def near_image(cur, w_re, w_im):
    weights = jnp.concatenate([w_re, w_im], axis=1)
    both = jnp.dot(cur, weights, precision=HIGHEST, preferred_element_type=F32)
    re = both[:VEC, :PD] - both[VEC:, PD:]
    im = both[VEC:, :PD] + both[:VEC, PD:]
    return jnp.concatenate([re, im], axis=0)


def far_image(slots, table_ref, lists_ref):
    values = []
    picks = []
    for r in range(PAIRS):
        m_re = table_ref[r, 1:2, :]
        m_im = table_ref[r, 2:3, :]
        c_re, c_im = slots[r][:VEC], slots[r][VEC:]
        values.append(
            jnp.concatenate([m_re * c_re - m_im * c_im, m_re * c_im + m_im * c_re], axis=0)
        )
        particle = lists_ref[r : r + 1, :].astype(jnp.int32)
        picks.append(one_hot(iota((PD, PD), 0) + 1 == particle))
    return exact_select(
        jnp.concatenate(values, axis=1), jnp.concatenate(picks, axis=1), NT
    )


def send_columns(cur, rx_ref, out_ref):
    picks = [one_hot(iota((PD, PD), 0) == wanted_row(rx_ref, r)) for r in range(PAIRS)]
    columns = exact_select(cur, jnp.concatenate(picks, axis=1))
    first = iota((VEC, PD), 1) < CAP
    for r in range(PAIRS):
        re = columns[:VEC, r * PD : (r + 1) * PD]
        im = columns[VEC:, r * PD : (r + 1) * PD]
        out_ref[2 * r] = jnp.where(first, re, pltpu.roll(im, CAP, 1))
        out_ref[2 * r + 1] = jnp.where(first, pltpu.roll(re, CAP, 1), im)


def received_columns(recv_ref):
    first = iota((VEC, PD), 1) < CAP
    slots = []
    for r in range(PAIRS):
        even = recv_ref[2 * r]
        odd = recv_ref[2 * r + 1]
        re = jnp.where(first, even, pltpu.roll(odd, CAP, 1))
        im = jnp.where(first, pltpu.roll(even, CAP, 1), odd)
        slots.append(jnp.concatenate([re, im], axis=0))
    return slots


def first_kernel(
    nb_ref, code_ref, lists_ref, table_ref, e_ref, re_ref, im_ref,
    slots_ref, init_ref, rx_ref,
    align_hbm, weights_ref, degree_ref, cur_ref, send_ref,
    near_ref, align_ref, sem_ref,
):
    start, me = place()
    local = nb_ref[...] - start
    near = (local >> 7) == me
    near_ref[...] = jnp.full((PD, PD), -1.0, F32)
    near_ref[:NB, :] = jnp.where(near, local & (PD - 1), -1).astype(F32)
    rows = iota((PD, PD), 0).astype(F32)
    counts = jnp.zeros((PD, PD), F32)
    for n in range(NB):
        counts = counts + jnp.where(rows == near_ref[n : n + 1, :], 1.0, 0.0)
    named = near_ref[...].T.astype(jnp.int32)
    inside = jnp.maximum(named, 0)
    values = []
    for ref, sign in ((e_ref, 1.0), (re_ref, 1.0), (im_ref, -1.0)):
        found = jnp.take_along_axis(ref[...], inside, axis=1, mode="promise_in_bounds")
        values.append(jnp.where(named >= 0, sign * found, 0.0).T[:NBP])
    code = code_ref[...]
    pair = code >> 7
    lane = code & (PD - 1)
    for r in range(PAIRS):
        mine = pair == r
        for v in range(3):
            row = jnp.broadcast_to(table_ref[r, v : v + 1, :], (NBP, PD))
            found = jnp.take_along_axis(row, lane, axis=1, mode="promise_in_bounds")
            values[v] = jnp.where(mine, found, values[v])
    below = values[0] + EPS
    align_ref[:, 0, :] = (values[1] / below)[:NB]
    align_ref[:, 1, :] = (values[2] / below)[:NB]
    leaving = pltpu.make_async_copy(align_ref, align_hbm, sem_ref.at[0])
    leaving.start()
    degree = EPS + jnp.sum(values[0], axis=0, keepdims=True)
    degree_ref[...] = jnp.broadcast_to(degree, (8, PD))
    w_re = counts * re_ref[...]
    w_im = counts * im_ref[...]
    weights_ref[0] = w_re
    weights_ref[1] = w_im
    slots = received_columns(slots_ref)
    image = near_image(init_ref[...], w_re, w_im) + far_image(slots, table_ref, lists_ref)
    image = image / degree
    cur_ref[...] = image
    send_columns(image, rx_ref, send_ref)
    leaving.wait()


def next_image(recv_ref, cur_ref, weights_ref, degree_ref, table_ref, lists_ref):
    slots = received_columns(recv_ref)
    image = near_image(cur_ref[...], weights_ref[0], weights_ref[1])
    image = image + far_image(slots, table_ref, lists_ref)
    return image / degree_ref[:1, :]


def middle_kernel(
    recv_ref, cur_ref, weights_ref, degree_ref, table_ref, lists_ref, rx_ref,
    out_ref, send_ref,
):
    image = next_image(recv_ref, cur_ref, weights_ref, degree_ref, table_ref, lists_ref)
    out_ref[...] = image
    send_columns(image, rx_ref, send_ref)


def last_kernel(
    total, recv_ref, cur_ref, weights_ref, degree_ref, table_ref, lists_ref,
    out_ref, gram_ref,
):
    image = next_image(recv_ref, cur_ref, weights_ref, degree_ref, table_ref, lists_ref)
    out_ref[...] = image
    gram = lax.dot_general(
        image[:VEC], image[:VEC], NT, precision=HIGHEST, preferred_element_type=F32
    ) + lax.dot_general(
        image[VEC:], image[VEC:], NT, precision=HIGHEST, preferred_element_type=F32
    )
    gram = gram * (1.0 / total)
    wide = jnp.concatenate([gram] * 8, axis=1)
    mine = iota((VEC, PD), 1) // VEC == iota((VEC, PD), 0) % 8
    wide = jnp.where(mine, wide, 0.0)
    packed = jnp.concatenate(
        [
            jnp.sum(wide[:8], axis=0, keepdims=True),
            jnp.sum(wide[8:], axis=0, keepdims=True),
        ],
        axis=0,
    )
    gram_ref[...] = jnp.broadcast_to(packed[None], gram_ref.shape)


def finish_kernel(grams_ref, cur_ref, out_ref):
    packed = jnp.sum(grams_ref[...], axis=0)
    row = iota((VEC, PD), 0)
    lane = iota((VEC, PD), 1)
    wide = jnp.where(row < 8, packed[0:1, :], packed[1:2, :])
    wide = jnp.where(lane // VEC == row % 8, wide, 0.0)
    for shift in (64, 32, 16):
        wide = wide + pltpu.roll(wide, shift, 1)
    columns = [jnp.broadcast_to(wide[:, c : c + 1], (VEC, PD)) for c in range(VEC)]
    re = cur_ref[:VEC, :]
    im = cur_ref[VEC:, :]
    for c in range(VEC):
        pivot = columns[c][c : c + 1, :]
        scale = lax.rsqrt(pivot)
        scale = scale * (1.5 - 0.5 * pivot * scale * scale)
        column = jnp.where(row > c, columns[c] * scale, 0.0)
        for d in range(c + 1, VEC):
            columns[d] = columns[d] - column * (columns[d][c : c + 1, :] * scale)
        top_re = re[c : c + 1, :] * scale
        top_im = im[c : c + 1, :] * scale
        here = row == c
        re = jnp.where(here, top_re, re - column * top_re)
        im = jnp.where(here, top_im, im - column * top_im)
    out_ref[:VEC, :] = re
    out_ref[VEC:, :] = im


def struct(shape, dtype=F32):
    return jax.ShapeDtypeStruct(shape, dtype)


SMEM = pl.BlockSpec(memory_space=pltpu.SMEM)
VMEM = pl.BlockSpec(memory_space=pltpu.VMEM)
HBM = pl.BlockSpec(memory_space=pltpu.HBM)


def grant(mib):
    return pltpu.CompilerParams(vmem_limit_bytes=mib << 20)


def exchange(size, truncation, names, asked, packed):
    sent = pl.pallas_call(
        functools.partial(pick_kernel, size),
        out_shape=struct((PEERS, size, PD), BF16),
        in_specs=[VMEM, VMEM],
        out_specs=VMEM,
        compiler_params=grant(16),
        name="pick",
    )(asked, packed)
    received = lax.all_to_all(sent, REP, 0, 0, tiled=True)
    return pl.pallas_call(
        functools.partial(far_kernel, size),
        out_shape=(struct((PAIRS, 8, PD)), struct((PEERS, VEC, PD))),
        in_specs=[SMEM, VMEM, VMEM, VMEM],
        out_specs=(VMEM, VMEM),
        scratch_shapes=[
            pltpu.VMEM((WIDE // 2, size - HEAD + ANG, PD), F32),
            pltpu.VMEM((WIDE // 2, size - HEAD + ANG, PD), F32),
        ],
        compiler_params=grant(20),
        name="far",
    )(truncation, names, packed, received)


def shards(coefficients, truncation, neighbours, initial):
    groups = lax.axis_size(GRP)
    replicas = lax.axis_size(REP)
    devices = groups * replicas
    which, code, lists, names, requests, coefficients, initial = pl.pallas_call(
        slot_kernel,
        out_shape=(
            struct((1,), jnp.int32),
            struct((NBP, PD), jnp.int32),
            struct((PAIRS, PD)),
            struct((PEERS, PD)),
            struct((PEERS, 1, PD)),
            struct((PD, CW), BF16),
            struct((32, PD)),
        ),
        in_specs=[SMEM, HBM, HBM, HBM],
        out_specs=(SMEM,) + (VMEM,) * 6,
        compiler_params=grant(6),
        scratch_shapes=[
            pltpu.VMEM((NB, PD), jnp.int32),
            pltpu.VMEM((NBP, PD), jnp.int32),
            pltpu.VMEM((2 * PEERS, NB * PD), BF16),
            pltpu.VMEM((CAP, NB * PD), BF16),
            pltpu.SemaphoreType.DMA((3,)),
        ],
        name="slots",
    )(
        truncation,
        *(
            pltpu.with_memory_space_constraint(x, pltpu.HBM)
            for x in (neighbours, coefficients, initial)
        ),
    )
    asked = lax.all_to_all(requests, REP, 0, 0, tiled=True)
    packed, e_own, re_own, im_own = pl.pallas_call(
        local_kernel,
        out_shape=(struct((HEAD + FULL, 2 * PD), BF16),) + (struct((PD, PD)),) * 3,
        in_specs=[SMEM, VMEM, VMEM],
        scratch_shapes=[
            pltpu.VMEM((CW, PD), F32),
            pltpu.VMEM((FULL + ANG, PD), F32),
            pltpu.VMEM((FULL + ANG, PD), F32),
            pltpu.VMEM((ANG, PD, 2 * PD), F32),
        ],
        cost_estimate=pl.CostEstimate(
            flops=20_000_000_000, bytes_accessed=1_000_000, transcendentals=0
        ),
        compiler_params=grant(20),
        name="local",
    )(truncation, coefficients, initial)
    table, slots = lax.switch(
        which[0],
        [functools.partial(exchange, HEAD + size) for size in SIZES],
        truncation, names, asked, packed,
    )
    alignment, weights, degree, current, columns = pl.pallas_call(
        first_kernel,
        out_shape=(
            struct((NB, 2, PD)),
            struct((2, PD, PD)),
            struct((8, PD)),
            struct((32, PD)),
            struct((PEERS, VEC, PD)),
        ),
        in_specs=[VMEM] * 10,
        compiler_params=grant(6),
        out_specs=(HBM, VMEM, VMEM, VMEM, VMEM),
        scratch_shapes=[
            pltpu.VMEM((PD, PD), F32),
            pltpu.VMEM((NB, 2, PD), F32),
            pltpu.SemaphoreType.DMA((1,)),
        ],
        name="first",
    )(
        neighbours, code, lists, table, e_own, re_own, im_own,
        slots, initial, asked,
    )
    columns = lax.all_to_all(columns, REP, 0, 0, tiled=True)
    current, columns = pl.pallas_call(
        middle_kernel,
        out_shape=(struct((32, PD)), struct((PEERS, VEC, PD))),
        compiler_params=grant(6),
        name="middle",
    )(columns, current, weights, degree, table, lists, asked)
    columns = lax.all_to_all(columns, REP, 0, 0, tiled=True)
    current, gram = pl.pallas_call(
        functools.partial(last_kernel, float(PD * devices)),
        out_shape=(struct((32, PD)), struct((devices, 2, PD))),
        compiler_params=grant(6),
        name="last",
    )(columns, current, weights, degree, table, lists)
    grams = lax.all_to_all(gram, GRP_REP, 0, 0, tiled=True)
    vectors = pl.pallas_call(
        finish_kernel,
        out_shape=struct((32, PD)),
        compiler_params=grant(6),
        name="finish",
    )(grams, current)
    return (jnp.transpose(alignment, (1, 0, 2)), vectors)


def solution(mesh):
    split = Mesh(mesh.devices.reshape(4, 2, 4, 4), GRP_REP)
    in_specs = (P(GRP_REP, None), P(), P(None, GRP_REP), P(None, GRP_REP))
    out_specs = (P(None, None, GRP_REP), P(None, GRP_REP))
    return jax.shard_map(
        shards, mesh=split, in_specs=in_specs, out_specs=out_specs, check_vma=False
    )
```

```python
import functools

import jax
import jax.numpy as jnp
from jax import lax
from jax.experimental import pallas as pl
from jax.experimental.pallas import tpu as pltpu
from jax.sharding import Mesh
from jax.sharding import PartitionSpec as P

ANG = 64
RAD = 16
NB = 50
NBP = 56
VEC = 16
PD = 128
CAP = 64
CW = 2048
FULL = RAD * ANG
SIZES = (384, 512, 544, 576, 608, 640, 672, 704, 736, 768, 896, FULL)
HEAD = 2 * VEC
PEERS = 16
PAIRS = PEERS // 2
WIDE = 4
GROUP = 8
ALWAYS = 16
GRP = ("grp_0", "grp_1")
REP = ("rep_0", "rep_1")
GRP_REP = ("grp_0", "grp_1", "rep_0", "rep_1")
EPS = 1e-06
F32 = jnp.float32
BF16 = jnp.bfloat16
HIGHEST = lax.Precision.HIGHEST

NT = (((1,), (1,)), ((), ()))
TN = (((0,), (0,)), ((), ()))


def iota(shape, dim):
    return lax.broadcasted_iota(jnp.int32, shape, dim)


def one_hot(cond):
    return jnp.where(cond, 1.0, 0.0).astype(BF16)


def three_parts(x):
    high = x.astype(BF16)
    rest = x - high.astype(F32)
    mid = rest.astype(BF16)
    low = (rest - mid.astype(F32)).astype(BF16)
    return jnp.concatenate([high, mid, low], axis=0)


def two_parts(x):
    high = x.astype(BF16)
    rest = (x - high.astype(F32)).astype(BF16)
    return jnp.concatenate([high, rest], axis=0)


def exact_select(x, selector, dims=(((1,), (0,)), ((), ()))):
    rows = x.shape[0]
    parts = lax.dot_general(three_parts(x), selector, dims, preferred_element_type=F32)
    return parts[:rows] + (parts[rows : 2 * rows] + parts[2 * rows :])


def kept_rows(trunc_ref, rows, lanes):
    row = iota((rows, lanes), 0) % RAD
    kept = jnp.zeros((rows, lanes), jnp.int32)
    for q in range(RAD):
        kept = jnp.where(row == q, trunc_ref[q], kept)
    return kept


def place():
    index = [lax.axis_index(name) for name in GRP_REP]
    size = [lax.axis_size(name) for name in GRP_REP]
    group = index[0] * size[1] + index[1]
    member = index[2] * size[3] + index[3]
    return group * (size[2] * size[3] * PD), member


def slot_kernel(
    trunc_ref, nb_hbm, coef_hbm, init_hbm,
    which_ref, code_ref, lists_ref, names_ref, req_ref, coef_ref, init_ref,
    nb_ref, nbp_ref, a_ref, b_ref, sem_ref,
):
    bring = (
        pltpu.make_async_copy(coef_hbm, coef_ref, sem_ref.at[0]),
        pltpu.make_async_copy(init_hbm, init_ref, sem_ref.at[1]),
    )
    slots = pltpu.make_async_copy(nb_hbm, nb_ref, sem_ref.at[2])
    for copy in (slots,) + bring:
        copy.start()
    total = trunc_ref[0]
    for q in range(1, RAD):
        total = total + trunc_ref[q]
    which = jnp.int32(0)
    for size in SIZES[:-1]:
        which = which + (total > size).astype(jnp.int32)
    which_ref[0] = which
    start, me = place()
    slots.wait()
    nbp_ref[...] = jnp.full((NBP, PD), -1, jnp.int32)
    nbp_ref[:NB, :] = nb_ref[...] - start
    local = nbp_ref[...]
    owner = local >> 7
    within = local & (PD - 1)
    remote = (owner != me) & (local >= 0)
    owner = jnp.where(remote, owner, -1)
    masks = [one_hot(owner == p) for p in range(PEERS)]
    before = one_hot(iota((NBP, NBP), 0) > iota((NBP, NBP), 1))
    in_column = jnp.dot(before, jnp.concatenate(masks, axis=1), preferred_element_type=F32)
    totals = jnp.concatenate(
        [jnp.sum(m.astype(F32), axis=0, keepdims=True) for m in masks], axis=0
    )
    left = one_hot(iota((PD, PD), 0) < iota((PD, PD), 1))
    columns = jnp.dot(totals.astype(BF16), left, preferred_element_type=F32)
    rank = jnp.zeros((NBP, PD), F32)
    for p in range(PEERS):
        here = in_column[:, p * PD : (p + 1) * PD] + columns[p : p + 1, :]
        rank = jnp.where(owner == p, here, rank)
    rank = rank.astype(jnp.int32)
    code = jnp.where(remote, owner * CAP + rank, -1)
    place_in_list = jnp.where(remote, rank, -1)
    particle = iota((1, PD), 1).astype(F32) + 1.0
    peer = iota((PEERS, PD), 0)
    target = iota((CAP, PD), 0)
    for n in range(NB):
        mine = peer == owner[n : n + 1, :]
        names = within[n : n + 1, :].astype(F32)
        both = jnp.concatenate(
            [jnp.where(mine, names, 0.0), jnp.where(mine, particle, 0.0)], axis=0
        )
        a_ref[:, n * PD : (n + 1) * PD] = both.astype(BF16)
        b_ref[:, n * PD : (n + 1) * PD] = one_hot(target == place_in_list[n : n + 1, :])
    lists = lax.dot_general(a_ref[...], b_ref[...], NT, preferred_element_type=F32)
    lists = jnp.concatenate([lists, lists], axis=1)
    for p in range(PEERS):
        req_ref[p] = lists[p : p + 1, :]
    names_ref[...] = lists[PEERS:]
    first = iota((1, PD), 1) < CAP
    for r in range(PAIRS):
        even = lists[PEERS + 2 * r : PEERS + 2 * r + 1, :]
        odd = lists[PEERS + 2 * r + 1 : PEERS + 2 * r + 2, :]
        lists_ref[r : r + 1, :] = jnp.where(first, even, odd)
    code_ref[...] = code
    for copy in bring:
        copy.wait()


def wanted_row(rx_ref, r):
    even = rx_ref[2 * r]
    odd = rx_ref[2 * r + 1]
    return jnp.where(iota((1, PD), 1) < CAP, even, odd).astype(jnp.int32)


def local_kernel(
    trunc_ref, coef_ref, init_ref, out_ref, e_ref, re_ref, im_ref,
    f_ref, wide_re_ref, wide_im_ref, s_ref,
):
    init = init_ref[...]
    parts = two_parts(jnp.concatenate([init[:VEC], init[VEC:]], axis=1))
    out_ref[:HEAD, :] = parts
    for c in range(CW // PD):
        block = coef_ref[:, c * PD : (c + 1) * PD].astype(F32)
        f_ref[c * PD : (c + 1) * PD, :] = block.T
    offset = 0
    for q in range(RAD):
        here = pl.ds(offset, ANG)
        wide_re_ref[here, :] = f_ref[q * ANG : (q + 1) * ANG, :]
        wide_im_ref[here, :] = f_ref[(RAD + q) * ANG : (RAD + q + 1) * ANG, :]
        offset = offset + trunc_ref[q]
    for b in range(FULL // PD):
        rows = slice(b * PD, (b + 1) * PD)
        to = slice(HEAD + b * PD, HEAD + (b + 1) * PD)
        kept = iota((PD, PD), 0) + b * PD < offset
        out_ref[to, :PD] = jnp.where(kept, wide_re_ref[rows, :], 0.0).astype(BF16)
        out_ref[to, PD:] = jnp.where(kept, wide_im_ref[rows, :], 0.0).astype(BF16)
    own_pairs(trunc_ref, e_ref, re_ref, im_ref, f_ref, s_ref)


def pick_kernel(size, rx_ref, pack_ref, out_ref):
    rows = iota((PD, PD), 0)
    first = iota((PD, PD), 1) < CAP

    def step(r, carry):
        sides = []
        for p in range(WIDE):
            picked = rows == rx_ref[WIDE * r + p].astype(jnp.int32)
            top = one_hot(picked & first)
            bottom = one_hot(picked & jnp.logical_not(first))
            sides.append(jnp.concatenate([top, bottom], axis=0))
        side = jnp.concatenate(sides, axis=1)
        chosen = jnp.dot(pack_ref[:size, :], side, preferred_element_type=F32)
        for p in range(WIDE):
            out_ref[WIDE * r + p] = chosen[:, p * PD : (p + 1) * PD].astype(BF16)
        return carry

    lax.fori_loop(0, PEERS // WIDE, step, 0)


def own_pairs(trunc_ref, e_ref, re_ref, im_ref, xt_ref, s_ref):
    kept = kept_rows(trunc_ref, 2 * RAD, PD)
    e_ref[...] = jnp.zeros((PD, PD), F32)
    re_ref[...] = jnp.zeros((PD, PD), F32)
    im_ref[...] = jnp.zeros((PD, PD), F32)

    def sums(first):
        for b in range(PD // 8):
            sub = slice(b * 8, (b + 1) * 8)
            energy = e_ref[sub, :]
            m_re = re_ref[sub, :]
            m_im = im_ref[sub, :]
            before = max(first - 1, 0)
            re = s_ref[before, sub, :PD]
            im = s_ref[before, sub, PD:]
            for k in range(first, first + GROUP):
                if k == 0:
                    energy = energy + re * re
                    continue
                next_re = s_ref[k, sub, :PD]
                next_im = s_ref[k, sub, PD:]
                half_re = 0.5 * next_re
                half_im = 0.5 * next_im
                energy = energy + (half_re * next_re + half_im * next_im)
                if k == 1:
                    m_re = m_re + re * next_re
                    m_im = m_im - re * next_im
                else:
                    m_re = m_re + (re * half_re + im * half_im)
                    m_im = m_im + (im * half_re - re * half_im)
                re, im = next_re, next_im
            e_ref[sub, :] = energy
            re_ref[sub, :] = m_re
            im_ref[sub, :] = m_im

    for first in range(0, ANG, GROUP):
        for k in range(first, first + GROUP):
            rows = xt_ref[pl.ds(k, 2 * RAD, stride=ANG), :]
            masked = rows if k < ALWAYS else jnp.where(kept > k, rows, 0.0)
            turned = jnp.concatenate([masked[RAD:], -masked[:RAD]], axis=0)
            right = jnp.concatenate([masked, turned], axis=1).astype(BF16)
            s_ref[k] = lax.dot_general(
                rows.astype(BF16), right, TN, preferred_element_type=F32
            )
        if first > 0:
            sums(first - GROUP)
    sums(ANG - GROUP)


def far_kernel(
    size, trunc_ref, names_ref, pack_ref, recv_ref, table_ref, cur_ref,
    same_ref, cross_ref,
):
    kept = size - HEAD
    for b in range(WIDE // 2):
        same_ref[b, kept:, :] = jnp.zeros((ANG, PD), F32)
        cross_ref[b, kept:, :] = jnp.zeros((ANG, PD), F32)

    def step(r, carry):
        far_step(
            size, r, trunc_ref, names_ref, pack_ref, recv_ref, table_ref, cur_ref,
            same_ref, cross_ref,
        )
        return carry

    lax.fori_loop(0, PEERS // WIDE, step, 0)


def far_step(
    size, r, trunc_ref, names_ref, pack_ref, recv_ref, table_ref, cur_ref,
    same_ref, cross_ref,
):
    kept = size - HEAD
    first = iota((1, PD), 1) < CAP
    picks = []
    for b in range(WIDE // 2):
        even = names_ref[pl.ds(WIDE * r + 2 * b, 1), :]
        odd = names_ref[pl.ds(WIDE * r + 2 * b + 1, 1), :]
        name = jnp.where(first, even, odd).astype(jnp.int32)
        picks.append(one_hot(iota((PD, PD), 0) + 1 == name))
    pick = jnp.concatenate(picks, axis=1)
    mine_re = jnp.dot(pack_ref[HEAD:size, :PD], pick, preferred_element_type=F32)
    mine_im = jnp.dot(pack_ref[HEAD:size, PD:], pick, preferred_element_type=F32)
    for p in range(WIDE):
        parts = recv_ref[WIDE * r + p, :HEAD, :].astype(F32)
        cur_ref[WIDE * r + p] = parts[:VEC] + parts[VEC:]
    for b in range(WIDE // 2):
        even = recv_ref[WIDE * r + 2 * b, HEAD:, :].astype(F32)
        odd = recv_ref[WIDE * r + 2 * b + 1, HEAD:, :].astype(F32)
        b_re = jnp.where(first, even, pltpu.roll(odd, CAP, 1))
        b_im = jnp.where(first, pltpu.roll(even, CAP, 1), odd)
        a_re = mine_re[:, b * PD : (b + 1) * PD]
        a_im = mine_im[:, b * PD : (b + 1) * PD]
        same_ref[b, :kept, :] = a_re * b_re + a_im * b_im
        cross_ref[b, :kept, :] = a_im * b_re - a_re * b_im
    freq = iota((ANG, PD), 0)
    totals = [[jnp.zeros((ANG, PD), F32)] * 2 for _ in range(WIDE // 2)]
    offset = 0
    for q in range(RAD):
        here = pl.ds(offset, ANG)
        inside = freq[ALWAYS:] < trunc_ref[q]
        for b in range(WIDE // 2):
            for v, ref in enumerate((same_ref, cross_ref)):
                window = ref[b, here, :]
                window = jnp.concatenate(
                    [window[:ALWAYS], jnp.where(inside, window[ALWAYS:], 0.0)], axis=0
                )
                totals[b][v] = totals[b][v] + window
        offset = offset + trunc_ref[q]
    inner = (freq > 0) & (freq < ANG - 1)
    for b in range(WIDE // 2):
        s_re, s_im = totals[b]
        power = s_re * s_re + s_im * s_im
        next_re = pltpu.roll(s_re, ANG - 1, 0)
        next_im = pltpu.roll(s_im, ANG - 1, 0)
        zero_re = s_re[:1]
        energy = zero_re * zero_re + 0.5 * jnp.sum(
            jnp.where(freq == 0, 0.0, power), axis=0, keepdims=True
        )
        m_re = zero_re * s_re[1:2] + 0.5 * jnp.sum(
            jnp.where(inner, s_re * next_re + s_im * next_im, 0.0), axis=0, keepdims=True
        )
        m_im = 0.5 * jnp.sum(
            jnp.where(inner, s_im * next_re - s_re * next_im, 0.0), axis=0, keepdims=True
        ) - zero_re * s_im[1:2]
        table_ref[WIDE // 2 * r + b] = jnp.concatenate(
            [energy, m_re, m_im, jnp.zeros((5, PD), F32)], axis=0
        )


def near_image(cur, w_re, w_im):
    weights = jnp.concatenate([w_re, w_im], axis=1)
    both = jnp.dot(cur, weights, precision=HIGHEST, preferred_element_type=F32)
    re = both[:VEC, :PD] - both[VEC:, PD:]
    im = both[VEC:, :PD] + both[:VEC, PD:]
    return jnp.concatenate([re, im], axis=0)


def far_image(slots, table_ref, lists_ref):
    values = []
    picks = []
    for r in range(PAIRS):
        m_re = table_ref[r, 1:2, :]
        m_im = table_ref[r, 2:3, :]
        c_re, c_im = slots[r][:VEC], slots[r][VEC:]
        values.append(
            jnp.concatenate([m_re * c_re - m_im * c_im, m_re * c_im + m_im * c_re], axis=0)
        )
        particle = lists_ref[r : r + 1, :].astype(jnp.int32)
        picks.append(one_hot(iota((PD, PD), 0) + 1 == particle))
    return exact_select(
        jnp.concatenate(values, axis=1), jnp.concatenate(picks, axis=1), NT
    )


def send_columns(cur, rx_ref, out_ref):
    picks = [one_hot(iota((PD, PD), 0) == wanted_row(rx_ref, r)) for r in range(PAIRS)]
    columns = exact_select(cur, jnp.concatenate(picks, axis=1))
    first = iota((VEC, PD), 1) < CAP
    for r in range(PAIRS):
        re = columns[:VEC, r * PD : (r + 1) * PD]
        im = columns[VEC:, r * PD : (r + 1) * PD]
        out_ref[2 * r] = jnp.where(first, re, pltpu.roll(im, CAP, 1))
        out_ref[2 * r + 1] = jnp.where(first, pltpu.roll(re, CAP, 1), im)


def received_columns(recv_ref):
    first = iota((VEC, PD), 1) < CAP
    slots = []
    for r in range(PAIRS):
        even = recv_ref[2 * r]
        odd = recv_ref[2 * r + 1]
        re = jnp.where(first, even, pltpu.roll(odd, CAP, 1))
        im = jnp.where(first, pltpu.roll(even, CAP, 1), odd)
        slots.append(jnp.concatenate([re, im], axis=0))
    return slots


def first_kernel(
    nb_ref, code_ref, lists_ref, table_ref, e_ref, re_ref, im_ref,
    slots_ref, init_ref, rx_ref,
    align_hbm, weights_ref, degree_ref, cur_ref, send_ref,
    near_ref, align_ref, sem_ref,
):
    start, me = place()
    local = nb_ref[...] - start
    near = (local >> 7) == me
    near_ref[...] = jnp.full((PD, PD), -1.0, F32)
    near_ref[:NB, :] = jnp.where(near, local & (PD - 1), -1).astype(F32)
    rows = iota((PD, PD), 0).astype(F32)
    counts = jnp.zeros((PD, PD), F32)
    for n in range(NB):
        counts = counts + jnp.where(rows == near_ref[n : n + 1, :], 1.0, 0.0)
    named = near_ref[...].T.astype(jnp.int32)
    inside = jnp.maximum(named, 0)
    values = []
    for ref, sign in ((e_ref, 1.0), (re_ref, 1.0), (im_ref, -1.0)):
        found = jnp.take_along_axis(ref[...], inside, axis=1, mode="promise_in_bounds")
        values.append(jnp.where(named >= 0, sign * found, 0.0).T[:NBP])
    code = code_ref[...]
    pair = code >> 7
    lane = code & (PD - 1)
    for r in range(PAIRS):
        mine = pair == r
        for v in range(3):
            row = jnp.broadcast_to(table_ref[r, v : v + 1, :], (NBP, PD))
            found = jnp.take_along_axis(row, lane, axis=1, mode="promise_in_bounds")
            values[v] = jnp.where(mine, found, values[v])
    below = values[0] + EPS
    align_ref[:, 0, :] = (values[1] / below)[:NB]
    align_ref[:, 1, :] = (values[2] / below)[:NB]
    leaving = pltpu.make_async_copy(align_ref, align_hbm, sem_ref.at[0])
    leaving.start()
    degree = EPS + jnp.sum(values[0], axis=0, keepdims=True)
    degree_ref[...] = jnp.broadcast_to(degree, (8, PD))
    w_re = counts * re_ref[...]
    w_im = counts * im_ref[...]
    weights_ref[0] = w_re
    weights_ref[1] = w_im
    slots = received_columns(slots_ref)
    image = near_image(init_ref[...], w_re, w_im) + far_image(slots, table_ref, lists_ref)
    image = image / degree
    cur_ref[...] = image
    send_columns(image, rx_ref, send_ref)
    leaving.wait()


def next_image(recv_ref, cur_ref, weights_ref, degree_ref, table_ref, lists_ref):
    slots = received_columns(recv_ref)
    image = near_image(cur_ref[...], weights_ref[0], weights_ref[1])
    image = image + far_image(slots, table_ref, lists_ref)
    return image / degree_ref[:1, :]


def middle_kernel(
    recv_ref, cur_ref, weights_ref, degree_ref, table_ref, lists_ref, rx_ref,
    out_ref, send_ref,
):
    image = next_image(recv_ref, cur_ref, weights_ref, degree_ref, table_ref, lists_ref)
    out_ref[...] = image
    send_columns(image, rx_ref, send_ref)


def last_kernel(
    total, recv_ref, cur_ref, weights_ref, degree_ref, table_ref, lists_ref,
    out_ref, gram_ref,
):
    image = next_image(recv_ref, cur_ref, weights_ref, degree_ref, table_ref, lists_ref)
    out_ref[...] = image
    gram = lax.dot_general(
        image[:VEC], image[:VEC], NT, precision=HIGHEST, preferred_element_type=F32
    ) + lax.dot_general(
        image[VEC:], image[VEC:], NT, precision=HIGHEST, preferred_element_type=F32
    )
    gram = gram * (1.0 / total)
    wide = jnp.concatenate([gram] * 8, axis=1)
    mine = iota((VEC, PD), 1) // VEC == iota((VEC, PD), 0) % 8
    wide = jnp.where(mine, wide, 0.0)
    packed = jnp.concatenate(
        [
            jnp.sum(wide[:8], axis=0, keepdims=True),
            jnp.sum(wide[8:], axis=0, keepdims=True),
        ],
        axis=0,
    )
    gram_ref[...] = jnp.broadcast_to(packed[None], gram_ref.shape)


def finish_kernel(grams_ref, cur_ref, out_ref):
    packed = jnp.sum(grams_ref[...], axis=0)
    row = iota((VEC, PD), 0)
    lane = iota((VEC, PD), 1)
    wide = jnp.where(row < 8, packed[0:1, :], packed[1:2, :])
    wide = jnp.where(lane // VEC == row % 8, wide, 0.0)
    for shift in (64, 32, 16):
        wide = wide + pltpu.roll(wide, shift, 1)
    columns = [jnp.broadcast_to(wide[:, c : c + 1], (VEC, PD)) for c in range(VEC)]
    re = cur_ref[:VEC, :]
    im = cur_ref[VEC:, :]
    for c in range(VEC):
        pivot = columns[c][c : c + 1, :]
        scale = lax.rsqrt(pivot)
        scale = scale * (1.5 - 0.5 * pivot * scale * scale)
        column = jnp.where(row > c, columns[c] * scale, 0.0)
        for d in range(c + 1, VEC):
            columns[d] = columns[d] - column * (columns[d][c : c + 1, :] * scale)
        top_re = re[c : c + 1, :] * scale
        top_im = im[c : c + 1, :] * scale
        here = row == c
        re = jnp.where(here, top_re, re - column * top_re)
        im = jnp.where(here, top_im, im - column * top_im)
    out_ref[:VEC, :] = re
    out_ref[VEC:, :] = im


def struct(shape, dtype=F32):
    return jax.ShapeDtypeStruct(shape, dtype)


SMEM = pl.BlockSpec(memory_space=pltpu.SMEM)
VMEM = pl.BlockSpec(memory_space=pltpu.VMEM)
HBM = pl.BlockSpec(memory_space=pltpu.HBM)


def grant(mib):
    return pltpu.CompilerParams(vmem_limit_bytes=mib << 20)


def exchange(size, truncation, names, asked, packed):
    sent = pl.pallas_call(
        functools.partial(pick_kernel, size),
        out_shape=struct((PEERS, size, PD), BF16),
        in_specs=[VMEM, VMEM],
        out_specs=VMEM,
        compiler_params=grant(16),
        name="pick",
    )(asked, packed)
    received = lax.all_to_all(sent, REP, 0, 0, tiled=True)
    return pl.pallas_call(
        functools.partial(far_kernel, size),
        out_shape=(struct((PAIRS, 8, PD)), struct((PEERS, VEC, PD))),
        in_specs=[SMEM, VMEM, VMEM, VMEM],
        out_specs=(VMEM, VMEM),
        scratch_shapes=[
            pltpu.VMEM((WIDE // 2, size - HEAD + ANG, PD), F32),
            pltpu.VMEM((WIDE // 2, size - HEAD + ANG, PD), F32),
        ],
        compiler_params=grant(20),
        name="far",
    )(truncation, names, packed, received)


def shards(coefficients, truncation, neighbours, initial):
    groups = lax.axis_size(GRP)
    replicas = lax.axis_size(REP)
    devices = groups * replicas
    which, code, lists, names, requests, coefficients, initial = pl.pallas_call(
        slot_kernel,
        out_shape=(
            struct((1,), jnp.int32),
            struct((NBP, PD), jnp.int32),
            struct((PAIRS, PD)),
            struct((PEERS, PD)),
            struct((PEERS, 1, PD)),
            struct((PD, CW), BF16),
            struct((32, PD)),
        ),
        in_specs=[SMEM, HBM, HBM, HBM],
        out_specs=(SMEM,) + (VMEM,) * 6,
        compiler_params=grant(6),
        scratch_shapes=[
            pltpu.VMEM((NB, PD), jnp.int32),
            pltpu.VMEM((NBP, PD), jnp.int32),
            pltpu.VMEM((2 * PEERS, NB * PD), BF16),
            pltpu.VMEM((CAP, NB * PD), BF16),
            pltpu.SemaphoreType.DMA((3,)),
        ],
        name="slots",
    )(
        truncation,
        *(
            pltpu.with_memory_space_constraint(x, pltpu.HBM)
            for x in (neighbours, coefficients, initial)
        ),
    )
    asked = lax.all_to_all(requests, REP, 0, 0, tiled=True)
    packed, e_own, re_own, im_own = pl.pallas_call(
        local_kernel,
        out_shape=(struct((HEAD + FULL, 2 * PD), BF16),) + (struct((PD, PD)),) * 3,
        in_specs=[SMEM, VMEM, VMEM],
        scratch_shapes=[
            pltpu.VMEM((CW, PD), F32),
            pltpu.VMEM((FULL + ANG, PD), F32),
            pltpu.VMEM((FULL + ANG, PD), F32),
            pltpu.VMEM((ANG, PD, 2 * PD), F32),
        ],
        cost_estimate=pl.CostEstimate(
            flops=20_000_000_000, bytes_accessed=1_000_000, transcendentals=0
        ),
        compiler_params=grant(20),
        name="local",
    )(truncation, coefficients, initial)
    table, slots = lax.switch(
        which[0],
        [functools.partial(exchange, HEAD + size) for size in SIZES],
        truncation, names, asked, packed,
    )
    alignment, weights, degree, current, columns = pl.pallas_call(
        first_kernel,
        out_shape=(
            struct((NB, 2, PD)),
            struct((2, PD, PD)),
            struct((8, PD)),
            struct((32, PD)),
            struct((PEERS, VEC, PD)),
        ),
        in_specs=[VMEM] * 10,
        compiler_params=grant(6),
        out_specs=(HBM, VMEM, VMEM, VMEM, VMEM),
        scratch_shapes=[
            pltpu.VMEM((PD, PD), F32),
            pltpu.VMEM((NB, 2, PD), F32),
            pltpu.SemaphoreType.DMA((1,)),
        ],
        name="first",
    )(
        neighbours, code, lists, table, e_own, re_own, im_own,
        slots, initial, asked,
    )
    columns = lax.all_to_all(columns, REP, 0, 0, tiled=True)
    current, columns = pl.pallas_call(
        middle_kernel,
        out_shape=(struct((32, PD)), struct((PEERS, VEC, PD))),
        compiler_params=grant(6),
        name="middle",
    )(columns, current, weights, degree, table, lists, asked)
    columns = lax.all_to_all(columns, REP, 0, 0, tiled=True)
    current, gram = pl.pallas_call(
        functools.partial(last_kernel, float(PD * devices)),
        out_shape=(struct((32, PD)), struct((devices, 2, PD))),
        compiler_params=grant(6),
        name="last",
    )(columns, current, weights, degree, table, lists)
    grams = lax.all_to_all(gram, GRP_REP, 0, 0, tiled=True)
    vectors = pl.pallas_call(
        finish_kernel,
        out_shape=struct((32, PD)),
        compiler_params=grant(6),
        name="finish",
    )(grams, current)
    return (jnp.transpose(alignment, (1, 0, 2)), vectors)


def solution(mesh):
    split = Mesh(mesh.devices.reshape(4, 2, 4, 4), GRP_REP)
    in_specs = (P(GRP_REP, None), P(), P(None, GRP_REP), P(None, GRP_REP))
    out_specs = (P(None, None, GRP_REP), P(None, GRP_REP))
    return jax.shard_map(
        shards, mesh=split, in_specs=in_specs, out_specs=out_specs, check_vma=False
    )
```

```python
import functools

import jax
import jax.numpy as jnp
from jax import lax
from jax.experimental import pallas as pl
from jax.experimental.pallas import tpu as pltpu
from jax.sharding import Mesh
from jax.sharding import PartitionSpec as P

ANG = 64
RAD = 16
NB = 50
NBP = 56
VEC = 16
PD = 128
CAP = 64
CW = 2048
FULL = RAD * ANG
SIZES = (384, 512, 544, 576, 608, 640, 672, 704, 736, 768, 896, FULL)
HEAD = 2 * VEC
PEERS = 16
PAIRS = PEERS // 2
WIDE = 4
GROUP = 4
ALWAYS = 16
GRP = ("grp_0", "grp_1")
REP = ("rep_0", "rep_1")
GRP_REP = ("grp_0", "grp_1", "rep_0", "rep_1")
EPS = 1e-06
F32 = jnp.float32
BF16 = jnp.bfloat16
HIGHEST = lax.Precision.HIGHEST

NT = (((1,), (1,)), ((), ()))
TN = (((0,), (0,)), ((), ()))


def iota(shape, dim):
    return lax.broadcasted_iota(jnp.int32, shape, dim)


def one_hot(cond):
    return jnp.where(cond, 1.0, 0.0).astype(BF16)


def three_parts(x):
    high = x.astype(BF16)
    rest = x - high.astype(F32)
    mid = rest.astype(BF16)
    low = (rest - mid.astype(F32)).astype(BF16)
    return jnp.concatenate([high, mid, low], axis=0)


def two_parts(x):
    high = x.astype(BF16)
    rest = (x - high.astype(F32)).astype(BF16)
    return jnp.concatenate([high, rest], axis=0)


def exact_select(x, selector, dims=(((1,), (0,)), ((), ()))):
    rows = x.shape[0]
    parts = lax.dot_general(three_parts(x), selector, dims, preferred_element_type=F32)
    return parts[:rows] + (parts[rows : 2 * rows] + parts[2 * rows :])


def kept_rows(trunc_ref, rows, lanes):
    row = iota((rows, lanes), 0) % RAD
    kept = jnp.zeros((rows, lanes), jnp.int32)
    for q in range(RAD):
        kept = jnp.where(row == q, trunc_ref[q], kept)
    return kept


def place():
    index = [lax.axis_index(name) for name in GRP_REP]
    size = [lax.axis_size(name) for name in GRP_REP]
    group = index[0] * size[1] + index[1]
    member = index[2] * size[3] + index[3]
    return group * (size[2] * size[3] * PD), member


def slot_kernel(
    trunc_ref, nb_hbm, coef_hbm, init_hbm,
    which_ref, code_ref, lists_ref, names_ref, req_ref, coef_ref, init_ref,
    nb_ref, nbp_ref, a_ref, b_ref, sem_ref,
):
    bring = (
        pltpu.make_async_copy(coef_hbm, coef_ref, sem_ref.at[0]),
        pltpu.make_async_copy(init_hbm, init_ref, sem_ref.at[1]),
    )
    slots = pltpu.make_async_copy(nb_hbm, nb_ref, sem_ref.at[2])
    for copy in (slots,) + bring:
        copy.start()
    total = trunc_ref[0]
    for q in range(1, RAD):
        total = total + trunc_ref[q]
    which = jnp.int32(0)
    for size in SIZES[:-1]:
        which = which + (total > size).astype(jnp.int32)
    which_ref[0] = which
    start, me = place()
    slots.wait()
    nbp_ref[...] = jnp.full((NBP, PD), -1, jnp.int32)
    nbp_ref[:NB, :] = nb_ref[...] - start
    local = nbp_ref[...]
    owner = local >> 7
    within = local & (PD - 1)
    remote = (owner != me) & (local >= 0)
    owner = jnp.where(remote, owner, -1)
    masks = [one_hot(owner == p) for p in range(PEERS)]
    before = one_hot(iota((NBP, NBP), 0) > iota((NBP, NBP), 1))
    in_column = jnp.dot(before, jnp.concatenate(masks, axis=1), preferred_element_type=F32)
    totals = jnp.concatenate(
        [jnp.sum(m.astype(F32), axis=0, keepdims=True) for m in masks], axis=0
    )
    left = one_hot(iota((PD, PD), 0) < iota((PD, PD), 1))
    columns = jnp.dot(totals.astype(BF16), left, preferred_element_type=F32)
    rank = jnp.zeros((NBP, PD), F32)
    for p in range(PEERS):
        here = in_column[:, p * PD : (p + 1) * PD] + columns[p : p + 1, :]
        rank = jnp.where(owner == p, here, rank)
    rank = rank.astype(jnp.int32)
    code = jnp.where(remote, owner * CAP + rank, -1)
    place_in_list = jnp.where(remote, rank, -1)
    particle = iota((1, PD), 1).astype(F32) + 1.0
    peer = iota((PEERS, PD), 0)
    target = iota((CAP, PD), 0)
    for n in range(NB):
        mine = peer == owner[n : n + 1, :]
        names = within[n : n + 1, :].astype(F32)
        both = jnp.concatenate(
            [jnp.where(mine, names, 0.0), jnp.where(mine, particle, 0.0)], axis=0
        )
        a_ref[:, n * PD : (n + 1) * PD] = both.astype(BF16)
        b_ref[:, n * PD : (n + 1) * PD] = one_hot(target == place_in_list[n : n + 1, :])
    lists = lax.dot_general(a_ref[...], b_ref[...], NT, preferred_element_type=F32)
    lists = jnp.concatenate([lists, lists], axis=1)
    for p in range(PEERS):
        req_ref[p] = lists[p : p + 1, :]
    names_ref[...] = lists[PEERS:]
    first = iota((1, PD), 1) < CAP
    for r in range(PAIRS):
        even = lists[PEERS + 2 * r : PEERS + 2 * r + 1, :]
        odd = lists[PEERS + 2 * r + 1 : PEERS + 2 * r + 2, :]
        lists_ref[r : r + 1, :] = jnp.where(first, even, odd)
    code_ref[...] = code
    for copy in bring:
        copy.wait()


def wanted_row(rx_ref, r):
    even = rx_ref[2 * r]
    odd = rx_ref[2 * r + 1]
    return jnp.where(iota((1, PD), 1) < CAP, even, odd).astype(jnp.int32)


def local_kernel(
    trunc_ref, coef_ref, init_ref, out_ref, e_ref, re_ref, im_ref,
    f_ref, wide_re_ref, wide_im_ref, s_ref,
):
    init = init_ref[...]
    parts = two_parts(jnp.concatenate([init[:VEC], init[VEC:]], axis=1))
    out_ref[:HEAD, :] = parts
    for c in range(CW // PD):
        block = coef_ref[:, c * PD : (c + 1) * PD].astype(F32)
        f_ref[c * PD : (c + 1) * PD, :] = block.T
    offset = 0
    for q in range(RAD):
        here = pl.ds(offset, ANG)
        wide_re_ref[here, :] = f_ref[q * ANG : (q + 1) * ANG, :]
        wide_im_ref[here, :] = f_ref[(RAD + q) * ANG : (RAD + q + 1) * ANG, :]
        offset = offset + trunc_ref[q]
    for b in range(FULL // PD):
        rows = slice(b * PD, (b + 1) * PD)
        to = slice(HEAD + b * PD, HEAD + (b + 1) * PD)
        kept = iota((PD, PD), 0) + b * PD < offset
        out_ref[to, :PD] = jnp.where(kept, wide_re_ref[rows, :], 0.0).astype(BF16)
        out_ref[to, PD:] = jnp.where(kept, wide_im_ref[rows, :], 0.0).astype(BF16)
    own_pairs(trunc_ref, e_ref, re_ref, im_ref, f_ref, s_ref)


def pick_kernel(size, rx_ref, pack_ref, out_ref):
    rows = iota((PD, PD), 0)
    first = iota((PD, PD), 1) < CAP

    def step(r, carry):
        sides = []
        for p in range(WIDE):
            picked = rows == rx_ref[WIDE * r + p].astype(jnp.int32)
            top = one_hot(picked & first)
            bottom = one_hot(picked & jnp.logical_not(first))
            sides.append(jnp.concatenate([top, bottom], axis=0))
        side = jnp.concatenate(sides, axis=1)
        chosen = jnp.dot(pack_ref[:size, :], side, preferred_element_type=F32)
        for p in range(WIDE):
            out_ref[WIDE * r + p] = chosen[:, p * PD : (p + 1) * PD].astype(BF16)
        return carry

    lax.fori_loop(0, PEERS // WIDE, step, 0)


def own_pairs(trunc_ref, e_ref, re_ref, im_ref, xt_ref, s_ref):
    kept = kept_rows(trunc_ref, 2 * RAD, PD)
    e_ref[...] = jnp.zeros((PD, PD), F32)
    re_ref[...] = jnp.zeros((PD, PD), F32)
    im_ref[...] = jnp.zeros((PD, PD), F32)

    def sums(first):
        for b in range(PD // 8):
            sub = slice(b * 8, (b + 1) * 8)
            energy = e_ref[sub, :]
            m_re = re_ref[sub, :]
            m_im = im_ref[sub, :]
            before = max(first - 1, 0)
            re = s_ref[before, sub, :PD]
            im = s_ref[before, sub, PD:]
            for k in range(first, first + GROUP):
                if k == 0:
                    energy = energy + re * re
                    continue
                next_re = s_ref[k, sub, :PD]
                next_im = s_ref[k, sub, PD:]
                half_re = 0.5 * next_re
                half_im = 0.5 * next_im
                energy = energy + (half_re * next_re + half_im * next_im)
                if k == 1:
                    m_re = m_re + re * next_re
                    m_im = m_im - re * next_im
                else:
                    m_re = m_re + (re * half_re + im * half_im)
                    m_im = m_im + (im * half_re - re * half_im)
                re, im = next_re, next_im
            e_ref[sub, :] = energy
            re_ref[sub, :] = m_re
            im_ref[sub, :] = m_im

    for first in range(0, ANG, GROUP):
        for k in range(first, first + GROUP):
            rows = xt_ref[pl.ds(k, 2 * RAD, stride=ANG), :]
            masked = rows if k < ALWAYS else jnp.where(kept > k, rows, 0.0)
            turned = jnp.concatenate([masked[RAD:], -masked[:RAD]], axis=0)
            right = jnp.concatenate([masked, turned], axis=1).astype(BF16)
            s_ref[k] = lax.dot_general(
                rows.astype(BF16), right, TN, preferred_element_type=F32
            )
        if first > 0:
            sums(first - GROUP)
    sums(ANG - GROUP)


def far_kernel(
    size, trunc_ref, names_ref, pack_ref, recv_ref, table_ref, cur_ref,
    same_ref, cross_ref,
):
    kept = size - HEAD
    for b in range(WIDE // 2):
        same_ref[b, kept:, :] = jnp.zeros((ANG, PD), F32)
        cross_ref[b, kept:, :] = jnp.zeros((ANG, PD), F32)

    def step(r, carry):
        far_step(
            size, r, trunc_ref, names_ref, pack_ref, recv_ref, table_ref, cur_ref,
            same_ref, cross_ref,
        )
        return carry

    lax.fori_loop(0, PEERS // WIDE, step, 0)


def far_step(
    size, r, trunc_ref, names_ref, pack_ref, recv_ref, table_ref, cur_ref,
    same_ref, cross_ref,
):
    kept = size - HEAD
    first = iota((1, PD), 1) < CAP
    picks = []
    for b in range(WIDE // 2):
        even = names_ref[pl.ds(WIDE * r + 2 * b, 1), :]
        odd = names_ref[pl.ds(WIDE * r + 2 * b + 1, 1), :]
        name = jnp.where(first, even, odd).astype(jnp.int32)
        picks.append(one_hot(iota((PD, PD), 0) + 1 == name))
    pick = jnp.concatenate(picks, axis=1)
    mine_re = jnp.dot(pack_ref[HEAD:size, :PD], pick, preferred_element_type=F32)
    mine_im = jnp.dot(pack_ref[HEAD:size, PD:], pick, preferred_element_type=F32)
    for p in range(WIDE):
        parts = recv_ref[WIDE * r + p, :HEAD, :].astype(F32)
        cur_ref[WIDE * r + p] = parts[:VEC] + parts[VEC:]
    for b in range(WIDE // 2):
        even = recv_ref[WIDE * r + 2 * b, HEAD:, :].astype(F32)
        odd = recv_ref[WIDE * r + 2 * b + 1, HEAD:, :].astype(F32)
        b_re = jnp.where(first, even, pltpu.roll(odd, CAP, 1))
        b_im = jnp.where(first, pltpu.roll(even, CAP, 1), odd)
        a_re = mine_re[:, b * PD : (b + 1) * PD]
        a_im = mine_im[:, b * PD : (b + 1) * PD]
        same_ref[b, :kept, :] = a_re * b_re + a_im * b_im
        cross_ref[b, :kept, :] = a_im * b_re - a_re * b_im
    freq = iota((ANG, PD), 0)
    totals = [[jnp.zeros((ANG, PD), F32)] * 2 for _ in range(WIDE // 2)]
    offset = 0
    for q in range(RAD):
        here = pl.ds(offset, ANG)
        inside = freq[ALWAYS:] < trunc_ref[q]
        for b in range(WIDE // 2):
            for v, ref in enumerate((same_ref, cross_ref)):
                window = ref[b, here, :]
                window = jnp.concatenate(
                    [window[:ALWAYS], jnp.where(inside, window[ALWAYS:], 0.0)], axis=0
                )
                totals[b][v] = totals[b][v] + window
        offset = offset + trunc_ref[q]
    inner = (freq > 0) & (freq < ANG - 1)
    for b in range(WIDE // 2):
        s_re, s_im = totals[b]
        power = s_re * s_re + s_im * s_im
        next_re = pltpu.roll(s_re, ANG - 1, 0)
        next_im = pltpu.roll(s_im, ANG - 1, 0)
        zero_re = s_re[:1]
        energy = zero_re * zero_re + 0.5 * jnp.sum(
            jnp.where(freq == 0, 0.0, power), axis=0, keepdims=True
        )
        m_re = zero_re * s_re[1:2] + 0.5 * jnp.sum(
            jnp.where(inner, s_re * next_re + s_im * next_im, 0.0), axis=0, keepdims=True
        )
        m_im = 0.5 * jnp.sum(
            jnp.where(inner, s_im * next_re - s_re * next_im, 0.0), axis=0, keepdims=True
        ) - zero_re * s_im[1:2]
        table_ref[WIDE // 2 * r + b] = jnp.concatenate(
            [energy, m_re, m_im, jnp.zeros((5, PD), F32)], axis=0
        )


def near_image(cur, w_re, w_im):
    weights = jnp.concatenate([w_re, w_im], axis=1)
    both = jnp.dot(cur, weights, precision=HIGHEST, preferred_element_type=F32)
    re = both[:VEC, :PD] - both[VEC:, PD:]
    im = both[VEC:, :PD] + both[:VEC, PD:]
    return jnp.concatenate([re, im], axis=0)


def far_image(slots, table_ref, lists_ref):
    values = []
    picks = []
    for r in range(PAIRS):
        m_re = table_ref[r, 1:2, :]
        m_im = table_ref[r, 2:3, :]
        c_re, c_im = slots[r][:VEC], slots[r][VEC:]
        values.append(
            jnp.concatenate([m_re * c_re - m_im * c_im, m_re * c_im + m_im * c_re], axis=0)
        )
        particle = lists_ref[r : r + 1, :].astype(jnp.int32)
        picks.append(one_hot(iota((PD, PD), 0) + 1 == particle))
    return exact_select(
        jnp.concatenate(values, axis=1), jnp.concatenate(picks, axis=1), NT
    )


def send_columns(cur, rx_ref, out_ref):
    picks = [one_hot(iota((PD, PD), 0) == wanted_row(rx_ref, r)) for r in range(PAIRS)]
    columns = exact_select(cur, jnp.concatenate(picks, axis=1))
    first = iota((VEC, PD), 1) < CAP
    for r in range(PAIRS):
        re = columns[:VEC, r * PD : (r + 1) * PD]
        im = columns[VEC:, r * PD : (r + 1) * PD]
        out_ref[2 * r] = jnp.where(first, re, pltpu.roll(im, CAP, 1))
        out_ref[2 * r + 1] = jnp.where(first, pltpu.roll(re, CAP, 1), im)


def received_columns(recv_ref):
    first = iota((VEC, PD), 1) < CAP
    slots = []
    for r in range(PAIRS):
        even = recv_ref[2 * r]
        odd = recv_ref[2 * r + 1]
        re = jnp.where(first, even, pltpu.roll(odd, CAP, 1))
        im = jnp.where(first, pltpu.roll(even, CAP, 1), odd)
        slots.append(jnp.concatenate([re, im], axis=0))
    return slots


def first_kernel(
    nb_ref, code_ref, lists_ref, table_ref, e_ref, re_ref, im_ref,
    slots_ref, init_ref, rx_ref,
    align_hbm, weights_ref, degree_ref, cur_ref, send_ref,
    near_ref, align_ref, sem_ref,
):
    start, me = place()
    local = nb_ref[...] - start
    near = (local >> 7) == me
    near_ref[...] = jnp.full((PD, PD), -1.0, F32)
    near_ref[:NB, :] = jnp.where(near, local & (PD - 1), -1).astype(F32)
    rows = iota((PD, PD), 0).astype(F32)
    counts = jnp.zeros((PD, PD), F32)
    for n in range(NB):
        counts = counts + jnp.where(rows == near_ref[n : n + 1, :], 1.0, 0.0)
    named = near_ref[...].T.astype(jnp.int32)
    inside = jnp.maximum(named, 0)
    values = []
    for ref, sign in ((e_ref, 1.0), (re_ref, 1.0), (im_ref, -1.0)):
        found = jnp.take_along_axis(ref[...], inside, axis=1, mode="promise_in_bounds")
        values.append(jnp.where(named >= 0, sign * found, 0.0).T[:NBP])
    code = code_ref[...]
    pair = code >> 7
    lane = code & (PD - 1)
    for r in range(PAIRS):
        mine = pair == r
        for v in range(3):
            row = jnp.broadcast_to(table_ref[r, v : v + 1, :], (NBP, PD))
            found = jnp.take_along_axis(row, lane, axis=1, mode="promise_in_bounds")
            values[v] = jnp.where(mine, found, values[v])
    below = values[0] + EPS
    align_ref[:, 0, :] = (values[1] / below)[:NB]
    align_ref[:, 1, :] = (values[2] / below)[:NB]
    leaving = pltpu.make_async_copy(align_ref, align_hbm, sem_ref.at[0])
    leaving.start()
    degree = EPS + jnp.sum(values[0], axis=0, keepdims=True)
    degree_ref[...] = jnp.broadcast_to(degree, (8, PD))
    w_re = counts * re_ref[...]
    w_im = counts * im_ref[...]
    weights_ref[0] = w_re
    weights_ref[1] = w_im
    slots = received_columns(slots_ref)
    image = near_image(init_ref[...], w_re, w_im) + far_image(slots, table_ref, lists_ref)
    image = image / degree
    cur_ref[...] = image
    send_columns(image, rx_ref, send_ref)
    leaving.wait()


def next_image(recv_ref, cur_ref, weights_ref, degree_ref, table_ref, lists_ref):
    slots = received_columns(recv_ref)
    image = near_image(cur_ref[...], weights_ref[0], weights_ref[1])
    image = image + far_image(slots, table_ref, lists_ref)
    return image / degree_ref[:1, :]


def middle_kernel(
    recv_ref, cur_ref, weights_ref, degree_ref, table_ref, lists_ref, rx_ref,
    out_ref, send_ref,
):
    image = next_image(recv_ref, cur_ref, weights_ref, degree_ref, table_ref, lists_ref)
    out_ref[...] = image
    send_columns(image, rx_ref, send_ref)


def last_kernel(
    total, recv_ref, cur_ref, weights_ref, degree_ref, table_ref, lists_ref,
    out_ref, gram_ref,
):
    image = next_image(recv_ref, cur_ref, weights_ref, degree_ref, table_ref, lists_ref)
    out_ref[...] = image
    gram = lax.dot_general(
        image[:VEC], image[:VEC], NT, precision=HIGHEST, preferred_element_type=F32
    ) + lax.dot_general(
        image[VEC:], image[VEC:], NT, precision=HIGHEST, preferred_element_type=F32
    )
    gram = gram * (1.0 / total)
    wide = jnp.concatenate([gram] * 8, axis=1)
    mine = iota((VEC, PD), 1) // VEC == iota((VEC, PD), 0) % 8
    wide = jnp.where(mine, wide, 0.0)
    packed = jnp.concatenate(
        [
            jnp.sum(wide[:8], axis=0, keepdims=True),
            jnp.sum(wide[8:], axis=0, keepdims=True),
        ],
        axis=0,
    )
    gram_ref[...] = jnp.broadcast_to(packed[None], gram_ref.shape)


def finish_kernel(grams_ref, cur_ref, out_ref):
    packed = jnp.sum(grams_ref[...], axis=0)
    row = iota((VEC, PD), 0)
    lane = iota((VEC, PD), 1)
    wide = jnp.where(row < 8, packed[0:1, :], packed[1:2, :])
    wide = jnp.where(lane // VEC == row % 8, wide, 0.0)
    for shift in (64, 32, 16):
        wide = wide + pltpu.roll(wide, shift, 1)
    columns = [jnp.broadcast_to(wide[:, c : c + 1], (VEC, PD)) for c in range(VEC)]
    re = cur_ref[:VEC, :]
    im = cur_ref[VEC:, :]
    for c in range(VEC):
        pivot = columns[c][c : c + 1, :]
        scale = lax.rsqrt(pivot)
        scale = scale * (1.5 - 0.5 * pivot * scale * scale)
        column = jnp.where(row > c, columns[c] * scale, 0.0)
        for d in range(c + 1, VEC):
            columns[d] = columns[d] - column * (columns[d][c : c + 1, :] * scale)
        top_re = re[c : c + 1, :] * scale
        top_im = im[c : c + 1, :] * scale
        here = row == c
        re = jnp.where(here, top_re, re - column * top_re)
        im = jnp.where(here, top_im, im - column * top_im)
    out_ref[:VEC, :] = re
    out_ref[VEC:, :] = im


def struct(shape, dtype=F32):
    return jax.ShapeDtypeStruct(shape, dtype)


SMEM = pl.BlockSpec(memory_space=pltpu.SMEM)
VMEM = pl.BlockSpec(memory_space=pltpu.VMEM)
HBM = pl.BlockSpec(memory_space=pltpu.HBM)


def grant(mib):
    return pltpu.CompilerParams(vmem_limit_bytes=mib << 20)


def exchange(size, truncation, names, asked, packed):
    sent = pl.pallas_call(
        functools.partial(pick_kernel, size),
        out_shape=struct((PEERS, size, PD), BF16),
        in_specs=[VMEM, VMEM],
        out_specs=VMEM,
        compiler_params=grant(16),
        name="pick",
    )(asked, packed)
    received = lax.all_to_all(sent, REP, 0, 0, tiled=True)
    return pl.pallas_call(
        functools.partial(far_kernel, size),
        out_shape=(struct((PAIRS, 8, PD)), struct((PEERS, VEC, PD))),
        in_specs=[SMEM, VMEM, VMEM, VMEM],
        out_specs=(VMEM, VMEM),
        scratch_shapes=[
            pltpu.VMEM((WIDE // 2, size - HEAD + ANG, PD), F32),
            pltpu.VMEM((WIDE // 2, size - HEAD + ANG, PD), F32),
        ],
        compiler_params=grant(20),
        name="far",
    )(truncation, names, packed, received)


def shards(coefficients, truncation, neighbours, initial):
    groups = lax.axis_size(GRP)
    replicas = lax.axis_size(REP)
    devices = groups * replicas
    which, code, lists, names, requests, coefficients, initial = pl.pallas_call(
        slot_kernel,
        out_shape=(
            struct((1,), jnp.int32),
            struct((NBP, PD), jnp.int32),
            struct((PAIRS, PD)),
            struct((PEERS, PD)),
            struct((PEERS, 1, PD)),
            struct((PD, CW), BF16),
            struct((32, PD)),
        ),
        in_specs=[SMEM, HBM, HBM, HBM],
        out_specs=(SMEM,) + (VMEM,) * 6,
        compiler_params=grant(6),
        scratch_shapes=[
            pltpu.VMEM((NB, PD), jnp.int32),
            pltpu.VMEM((NBP, PD), jnp.int32),
            pltpu.VMEM((2 * PEERS, NB * PD), BF16),
            pltpu.VMEM((CAP, NB * PD), BF16),
            pltpu.SemaphoreType.DMA((3,)),
        ],
        name="slots",
    )(
        truncation,
        *(
            pltpu.with_memory_space_constraint(x, pltpu.HBM)
            for x in (neighbours, coefficients, initial)
        ),
    )
    asked = lax.all_to_all(requests, REP, 0, 0, tiled=True)
    packed, e_own, re_own, im_own = pl.pallas_call(
        local_kernel,
        out_shape=(struct((HEAD + FULL, 2 * PD), BF16),) + (struct((PD, PD)),) * 3,
        in_specs=[SMEM, VMEM, VMEM],
        scratch_shapes=[
            pltpu.VMEM((CW, PD), F32),
            pltpu.VMEM((FULL + ANG, PD), F32),
            pltpu.VMEM((FULL + ANG, PD), F32),
            pltpu.VMEM((ANG, PD, 2 * PD), F32),
        ],
        cost_estimate=pl.CostEstimate(
            flops=20_000_000_000, bytes_accessed=1_000_000, transcendentals=0
        ),
        compiler_params=grant(20),
        name="local",
    )(truncation, coefficients, initial)
    table, slots = lax.switch(
        which[0],
        [functools.partial(exchange, HEAD + size) for size in SIZES],
        truncation, names, asked, packed,
    )
    alignment, weights, degree, current, columns = pl.pallas_call(
        first_kernel,
        out_shape=(
            struct((NB, 2, PD)),
            struct((2, PD, PD)),
            struct((8, PD)),
            struct((32, PD)),
            struct((PEERS, VEC, PD)),
        ),
        in_specs=[VMEM] * 10,
        compiler_params=grant(6),
        out_specs=(HBM, VMEM, VMEM, VMEM, VMEM),
        scratch_shapes=[
            pltpu.VMEM((PD, PD), F32),
            pltpu.VMEM((NB, 2, PD), F32),
            pltpu.SemaphoreType.DMA((1,)),
        ],
        name="first",
    )(
        neighbours, code, lists, table, e_own, re_own, im_own,
        slots, initial, asked,
    )
    columns = lax.all_to_all(columns, REP, 0, 0, tiled=True)
    current, columns = pl.pallas_call(
        middle_kernel,
        out_shape=(struct((32, PD)), struct((PEERS, VEC, PD))),
        compiler_params=grant(6),
        name="middle",
    )(columns, current, weights, degree, table, lists, asked)
    columns = lax.all_to_all(columns, REP, 0, 0, tiled=True)
    current, gram = pl.pallas_call(
        functools.partial(last_kernel, float(PD * devices)),
        out_shape=(struct((32, PD)), struct((devices, 2, PD))),
        compiler_params=grant(6),
        name="last",
    )(columns, current, weights, degree, table, lists)
    grams = lax.all_to_all(gram, GRP_REP, 0, 0, tiled=True)
    vectors = pl.pallas_call(
        finish_kernel,
        out_shape=struct((32, PD)),
        compiler_params=grant(6),
        name="finish",
    )(grams, current)
    return (jnp.transpose(alignment, (1, 0, 2)), vectors)


def solution(mesh):
    split = Mesh(mesh.devices.reshape(4, 2, 4, 4), GRP_REP)
    in_specs = (P(GRP_REP, None), P(), P(None, GRP_REP), P(None, GRP_REP))
    out_specs = (P(None, None, GRP_REP), P(None, GRP_REP))
    return jax.shard_map(
        shards, mesh=split, in_specs=in_specs, out_specs=out_specs, check_vma=False
    )
```
